256 devices in a mesh: groups: 2 (over y), row: 128 (over x, z, core).
Axes of the slice: x: 4, y: 2, z: 16, core: 2. Of those that a mesh axis runs over, the one named last changes fastest.
The devices are a block of a 4x16x16 slice.
Arguments:
- pair_cols: bfloat16 [1024, 2048, 128], P(None, ('groups', 'row')), parts along dimension 1, may hold values from -410 to 410
- single: bfloat16 [2048, 384], P(('groups', 'row')), parts along dimension 0, may hold values from -6 to 6
- rotation: float32 [9, 2048], P(None, ('groups', 'row')), parts along dimension 1, may hold values from -1 to 1, as said below
- translation: float32 [3, 2048], P(None, ('groups', 'row')), parts along dimension 1, may hold values from -6 to 6
- residue_mask: int32 [2048], P('groups'), parts along dimension 0, may hold values from 0 to 1, as said below
- chain_index: int32 [2048], P('groups'), parts along dimension 0, may hold values from 0 to 3, never falling along the last dimension, each value on 1 to 512 neighbouring positions
- query_weight: bfloat16 [384, 192], replicated, may hold values from -0.3125 to 0.3125
- key_weight: bfloat16 [384, 192], replicated, may hold values from -0.3125 to 0.3125
- value_weight: bfloat16 [384, 192], replicated, may hold values from -0.3125 to 0.3125
- qpoint_weight: bfloat16 [384, 144], replicated, may hold values from -0.3125 to 0.3125
- kpoint_weight: bfloat16 [384, 144], replicated, may hold values from -0.3125 to 0.3125
- vpoint_weight: bfloat16 [384, 288], replicated, may hold values from -0.3125 to 0.3125
- pair_weight: bfloat16 [12, 128], replicated, may hold values from -0.5 to 0.5
- head_weight: float32 [12], replicated, may hold values from -3 to 3
- chain_weight: float32 [12], replicated, may hold values from -6 to 6
- output_weight: bfloat16 [2112, 384], replicated, may hold values from -0.125 to 0.125
- gain_first: float32 [384], replicated, may hold values from 0.5 to 1.5
- mlp_first: bfloat16 [384, 384], replicated, may hold values from -0.3125 to 0.3125
- mlp_second: bfloat16 [384, 384], replicated, may hold values from -0.3125 to 0.3125
- mlp_third: bfloat16 [384, 384], replicated, may hold values from -0.3125 to 0.3125
- gain_second: float32 [384], replicated, may hold values from 0.5 to 1.5
- frame_weight: bfloat16 [384, 6], replicated, may hold values from -0.3125 to 0.3125
Outputs:
- single_out: float32 [2048, 384], P(('groups', 'row')), parts along dimension 0
- rotation_out: float32 [9, 2048], P(None, ('groups', 'row')), parts along dimension 1
- translation_out: float32 [3, 2048], P(None, ('groups', 'row')), parts along dimension 1
The draws below stay inside these ranges and needn't reach their ends.
There are 2 independent parts, one for each index of `groups`. The reference program is written for one: setup_inputs(seed, part) draws one part's arguments, and reference() takes and returns one part's arrays. A program takes and returns all parts, laid end to end along the dimension named above; an argument that names none is the same for every part. Nothing has to cross between parts.
Inputs may be any that keep to these rules, and one draw needn't show every extreme that they name: `residue_mask`: 1 on a leading run of at least three quarters of 1024 positions, 0 after it. Each column is a rotation matrix, row-major.
All inputs are finite; a program needn't handle non-finite values.
Results may differ from the reference program's by a relative error of at most 0.02.
Values may be sent and summed in bfloat16 or wider, within the bound.
A program may use at most 64 MiB of HBM per device.

```python
import math
import jax
import jax.numpy as jnp
import numpy as np
from jax import lax

CS = 384
CZ = 128
H = 12
CH = 16
PQ = 4
PV = 8
RES_DEV = 8
LAYERS = 2
L = 1024
CAT = 2112
N_ROW = 128


def draw_pair_cols(key, part):
    noise_base = jnp.clip(jax.random.normal(key, (L, L, CZ), jnp.float32), -6.0, 6.0)
    return noise_base.astype(jnp.bfloat16)


def draw_rotation(key, part):
    vectors = 0.8 * jax.random.normal(key, (3, L), jnp.float32)
    inverse = 1.0 / jnp.sqrt(1.0 + jnp.sum(vectors * vectors, axis=0))
    real_part = inverse
    vector_x = vectors[0] * inverse
    vector_y = vectors[1] * inverse
    vector_z = vectors[2] * inverse
    return jnp.stack([real_part * real_part + vector_x * vector_x - vector_y * vector_y - vector_z * vector_z, 2.0 * (vector_x * vector_y - real_part * vector_z), 2.0 * (vector_x * vector_z + real_part * vector_y), 2.0 * (vector_x * vector_y + real_part * vector_z), real_part * real_part - vector_x * vector_x + vector_y * vector_y - vector_z * vector_z, 2.0 * (vector_y * vector_z - real_part * vector_x), 2.0 * (vector_x * vector_z - real_part * vector_y), 2.0 * (vector_y * vector_z + real_part * vector_x), real_part * real_part - vector_x * vector_x - vector_y * vector_y + vector_z * vector_z])


def draw_residue_mask(key, part):
    length = jax.random.randint(key, (), 3 * L // 4, L + 1)
    return (jnp.arange(L) < length).astype(jnp.int32)


def steps_of(stream_key, extent, pieces, least, largest):
    level, own = 1.0, jax.random.fold_in(stream_key, 6)
    for position, parts in pieces:
        draws = jnp.exp(jax.random.uniform(jax.random.fold_in(own, position), (parts,), jnp.float32, least / len(pieces), largest / len(pieces)))
        level = level * jnp.repeat(draws, extent[position] // parts).reshape([-1 if axis == position else 1 for axis in range(len(extent))])
    return level


def split_up(number_of, total, limit, lean):
    portions = [(1 << 20) // math.isqrt(rank ** lean) + 1 for rank in range(2, number_of + 1)]
    surplus, given = total - limit - (number_of - 1), [1] * (number_of - 1)
    while surplus > 0:
        movable = [i for i in range(number_of - 1) if given[i] < limit]
        mass, budget = sum([portions[i] for i in movable]), surplus
        for i in movable:
            extra = min(limit - given[i], max(1, budget * portions[i] // mass), surplus)
            given[i] = given[i] + extra
            surplus = surplus - extra
    return np.array([limit] + given)


def uneven_parts(own_key, amount, total, reach, lean):
    if amount == 2:
        one = jax.random.randint(own_key, (), max(1, total - reach), min(reach, total - 1) + 1)
        return jnp.stack([one, total - one])
    lengths = jnp.asarray(split_up(amount, total, reach, lean), jnp.int32)
    twos = (amount - 1) // 2
    giver, sink = lengths[1:1 + 2 * twos:2], lengths[2:2 + 2 * twos:2]
    room = jnp.minimum(giver - 1, reach - sink)
    moved = jax.random.randint(jax.random.fold_in(own_key, 1), (twos,), 0, 1 << 20) % (room + 1)
    lengths = lengths.at[1:1 + 2 * twos:2].set(giver - moved).at[2:2 + 2 * twos:2].set(sink + moved)
    return lengths[jax.random.permutation(jax.random.fold_in(own_key, 2), amount)]


def centred(stream_key, dims, deviation, bound, pieces=(), held_as=jnp.bfloat16):
    factor_of = steps_of(stream_key, dims, pieces, -0.22, 0.18) if pieces else 1.0
    values = jax.random.normal(stream_key, dims, jnp.float32) * deviation * factor_of
    return jnp.minimum(jnp.maximum(values, -bound), bound).astype(held_as)


def setup_inputs(seed: int = 0, part: int = 0) -> dict:
    key_of = jax.random.split(jax.random.key(seed), 23)
    part_keys = jax.random.split(jax.random.fold_in(key_of[22], part), 23)
    return {
        "pair_cols": draw_pair_cols(jax.random.fold_in(jax.random.fold_in(key_of[22], part), 71), part),
        "single": centred(part_keys[1], (L, CS), 1.0, 6.0, ((0, 128),)),
        "rotation": draw_rotation(jax.random.fold_in(jax.random.fold_in(key_of[22], part), 71), part),
        "translation": centred(part_keys[3], (3, L), 1.5, 6.0, ((1, 128),), jnp.float32),
        "residue_mask": draw_residue_mask(jax.random.fold_in(jax.random.fold_in(key_of[22], part), 71), part),
        "chain_index": jnp.searchsorted(jnp.cumsum(uneven_parts(part_keys[5], 4, L, L // 2, 2)), jnp.arange(L), side="right").astype(jnp.int32),
        "query_weight": centred(key_of[6], (CS, H * CH), CS ** -0.5, 0.3125),
        "key_weight": centred(key_of[7], (CS, H * CH), CS ** -0.5, 0.3125),
        "value_weight": centred(key_of[8], (CS, H * CH), CS ** -0.5, 0.3125),
        "qpoint_weight": centred(key_of[9], (CS, 3 * H * PQ), CS ** -0.5, 0.3125),
        "kpoint_weight": centred(key_of[10], (CS, 3 * H * PQ), CS ** -0.5, 0.3125),
        "vpoint_weight": centred(key_of[11], (CS, 3 * H * PV), CS ** -0.5, 0.3125),
        "pair_weight": centred(key_of[12], (H, CZ), CZ ** -0.5, 0.5),
        "head_weight": centred(key_of[13], (H,), 1.0, 3.0, (), jnp.float32),
        "chain_weight": centred(key_of[14], (H,), 1.5, 6.0, (), jnp.float32),
        "output_weight": centred(key_of[15], (CAT, CS), CAT ** -0.5, 0.125),
        "gain_first": jnp.clip(1.0 + 0.1 * jax.random.normal(key_of[16], (CS,), jnp.float32), 0.5, 1.5),
        "mlp_first": centred(key_of[17], (CS, CS), CS ** -0.5, 0.3125),
        "mlp_second": centred(key_of[18], (CS, CS), CS ** -0.5, 0.3125),
        "mlp_third": centred(key_of[19], (CS, CS), CS ** -0.5, 0.3125),
        "gain_second": jnp.clip(1.0 + 0.1 * jax.random.normal(key_of[20], (CS,), jnp.float32), 0.5, 1.5),
        "frame_weight": centred(key_of[21], (CS, 6), CS ** -0.5, 0.3125),
    }


EXACT_PRODUCT = lax.Precision.HIGHEST
LOGIT_WEIGHT = (1.0 / 3.0) ** 0.5

def to_global(points, rotation, translation):
    components = []
    for component in range(3):
        components.append(rotation[3 * component][:, None] * points[:, 0] + rotation[3 * component + 1][:, None] * points[:, 1] + rotation[3 * component + 2][:, None] * points[:, 2] + translation[component][:, None])
    return jnp.stack(components, axis=1)

def to_local(points, rotation, translation):
    shifted = points - jnp.transpose(translation)[:, :, None]
    components = []
    for component in range(3):
        components.append(rotation[component][:, None] * shifted[:, 0] + rotation[3 + component][:, None] * shifted[:, 1] + rotation[6 + component][:, None] * shifted[:, 2])
    return jnp.stack(components, axis=1)

def layer_norm(values, gain_vector):
    centered = values - lax.optimization_barrier(jnp.mean(values, axis=-1, keepdims=True))
    variance = lax.optimization_barrier(jnp.mean(centered * centered, axis=-1, keepdims=True))
    return centered * lax.rsqrt(variance + 1e-05) * gain_vector

def key_side(state_bf, rotation, translation, key_weight, value_weight, kpoint_weight, vpoint_weight):
    key_count = state_bf.shape[0]
    keys_bf = jnp.dot(state_bf, key_weight, preferred_element_type=jnp.float32).astype(jnp.bfloat16)
    values_bf = jnp.dot(state_bf, value_weight, preferred_element_type=jnp.float32).astype(jnp.bfloat16)
    key_pts = jnp.dot(state_bf, kpoint_weight, preferred_element_type=jnp.float32).reshape(key_count, 3, -1)
    value_pts = jnp.dot(state_bf, vpoint_weight, preferred_element_type=jnp.float32).reshape(key_count, 3, -1)
    return (keys_bf, values_bf, to_global(key_pts, rotation, translation), to_global(value_pts, rotation, translation))

def attend(state_bf, rotation, translation, pair_rows, chain_rows, keys_bf, values_bf, key_global, value_global, chain_index, residue_mask, query_weight, qpoint_weight, pair_weight, head_weight, chain_weight):
    row_count = state_bf.shape[0]
    heads = head_weight.shape[0]
    key_count = keys_bf.shape[0]
    pair_float = pair_rows.astype(jnp.float32)
    pair_bias = jnp.einsum('ijc,hc->ihj', pair_float, pair_weight.astype(jnp.float32), precision=EXACT_PRODUCT)
    queries = jnp.dot(state_bf, query_weight, preferred_element_type=jnp.float32).astype(jnp.bfloat16).reshape(row_count, heads, -1)
    head_dim = queries.shape[2]
    query_pts = to_global(jnp.dot(state_bf, qpoint_weight, preferred_element_type=jnp.float32).reshape(row_count, 3, -1), rotation, translation)
    query_pts = query_pts.reshape(row_count, 3, heads, -1)
    key_pts = key_global.reshape(key_count, 3, heads, -1)
    point_count = query_pts.shape[3]
    scores = jnp.einsum('ihd,jhd->ihj', queries.astype(jnp.float32), keys_bf.reshape(key_count, heads, head_dim).astype(jnp.float32), precision=EXACT_PRODUCT)
    cross_term = jnp.einsum('ikhp,jkhp->ihj', query_pts, key_pts, precision=EXACT_PRODUCT)
    query_square = lax.optimization_barrier(jnp.sum(query_pts * query_pts, axis=(1, 3)))
    key_square = lax.optimization_barrier(jnp.sum(key_pts * key_pts, axis=(1, 3)))
    distance = query_square[:, :, None] + jnp.transpose(key_square)[None] - 2.0 * cross_term
    weight_c = (2.0 / (9.0 * point_count)) ** 0.5
    point_scale = jax.nn.softplus(head_weight)
    same_chain = (chain_rows[:, None] == chain_index[None, :]).astype(jnp.float32)
    logits = LOGIT_WEIGHT * (scores * head_dim ** (-0.5) + pair_bias - (0.5 * weight_c * point_scale)[None, :, None] * distance)
    logits = logits + chain_weight[None, :, None] * same_chain[:, None, :] + ((residue_mask.astype(jnp.float32) - 1.0) * 100000.0)[None, None, :]
    attention = jax.nn.softmax(logits, axis=-1).astype(jnp.bfloat16)
    attn_float = attention.astype(jnp.float32)
    outputs = jnp.einsum('ihj,jhd->ihd', attn_float, values_bf.reshape(key_count, heads, head_dim).astype(jnp.float32), precision=EXACT_PRODUCT)
    value_pts = value_global.reshape(key_count, 3, heads, -1)
    point_glob = jnp.einsum('ihj,jkhp->ikhp', attn_float, value_pts, precision=EXACT_PRODUCT)
    point_local = to_local(point_glob.reshape(row_count, 3, -1), rotation, translation)
    point_norms = jnp.sqrt(lax.optimization_barrier(jnp.sum(point_local * point_local, axis=1)) + 1e-08)
    pair_out = jnp.einsum('ihj,ijc->ihc', attn_float, pair_float, precision=EXACT_PRODUCT)
    return jnp.concatenate([outputs.reshape(row_count, -1), point_local.reshape(row_count, -1), point_norms, pair_out.reshape(row_count, -1)], axis=1).astype(jnp.bfloat16)

def frame_compose(rotation, translation, frame_update):
    inverse = lax.rsqrt(1.0 + lax.optimization_barrier(jnp.sum(frame_update[:, :3] * frame_update[:, :3], axis=1)))
    real_part = inverse
    vector_x = frame_update[:, 0] * inverse
    vector_y = frame_update[:, 1] * inverse
    vector_z = frame_update[:, 2] * inverse
    turn_matrix = [[real_part * real_part + vector_x * vector_x - vector_y * vector_y - vector_z * vector_z, 2.0 * (vector_x * vector_y - real_part * vector_z), 2.0 * (vector_x * vector_z + real_part * vector_y)], [2.0 * (vector_x * vector_y + real_part * vector_z), real_part * real_part - vector_x * vector_x + vector_y * vector_y - vector_z * vector_z, 2.0 * (vector_y * vector_z - real_part * vector_x)], [2.0 * (vector_x * vector_z - real_part * vector_y), 2.0 * (vector_y * vector_z + real_part * vector_x), real_part * real_part - vector_x * vector_x - vector_y * vector_y + vector_z * vector_z]]
    new_rotation = jnp.stack([rotation[3 * outer] * turn_matrix[0][inner] + rotation[3 * outer + 1] * turn_matrix[1][inner] + rotation[3 * outer + 2] * turn_matrix[2][inner] for outer in range(3) for inner in range(3)])
    new_translation = jnp.stack([rotation[3 * outer] * frame_update[:, 3] + rotation[3 * outer + 1] * frame_update[:, 4] + rotation[3 * outer + 2] * frame_update[:, 5] + translation[outer] for outer in range(3)])
    return (new_rotation, new_translation)

def update(single_state, concat, rotation, translation, output_weight, gain_first, mlp_first, mlp_second, mlp_third, gain_second, frame_weight):
    single_state = single_state + jnp.dot(concat, output_weight, preferred_element_type=jnp.float32)
    normed = layer_norm(single_state, gain_first)
    hidden = jax.nn.relu(jnp.dot(normed.astype(jnp.bfloat16), mlp_first, preferred_element_type=jnp.float32)).astype(jnp.bfloat16)
    hidden = jax.nn.relu(jnp.dot(hidden, mlp_second, preferred_element_type=jnp.float32)).astype(jnp.bfloat16)
    single_state = layer_norm(normed + jnp.dot(hidden, mlp_third, preferred_element_type=jnp.float32), gain_second)
    state_bf = single_state.astype(jnp.bfloat16)
    frame_update = jnp.dot(state_bf, frame_weight, preferred_element_type=jnp.float32)
    new_rotation, new_translation = frame_compose(rotation, translation, frame_update)
    return (single_state, state_bf, new_rotation, new_translation)

def reference(pair_cols, single, rotation, translation, residue_mask, chain_index, query_weight, key_weight, value_weight, qpoint_weight, kpoint_weight, vpoint_weight, pair_weight, head_weight, chain_weight, output_weight, gain_first, mlp_first, mlp_second, mlp_third, gain_second, frame_weight):
    single_state = single.astype(jnp.float32)
    state_bf = single
    for layer_index in range(LAYERS):
        keys_bf, values_bf, key_global, value_global = key_side(state_bf, rotation, translation, key_weight, value_weight, kpoint_weight, vpoint_weight)

        def one_block(block_index):
            row_start = (block_index * RES_DEV).astype(jnp.int32)
            pair_rows = lax.dynamic_slice_in_dim(pair_cols, row_start, RES_DEV, 0)
            state_rows = lax.dynamic_slice_in_dim(state_bf, row_start, RES_DEV, 0)
            rotation_rows = lax.dynamic_slice_in_dim(rotation, row_start, RES_DEV, 1)
            translation_rows = lax.dynamic_slice_in_dim(translation, row_start, RES_DEV, 1)
            chain_rows = lax.dynamic_slice_in_dim(chain_index, row_start, RES_DEV, 0)
            return attend(state_rows, rotation_rows, translation_rows, pair_rows, chain_rows, keys_bf, values_bf, key_global, value_global, chain_index, residue_mask, query_weight, qpoint_weight, pair_weight, head_weight, chain_weight)
        concat = lax.map(one_block, jnp.arange(N_ROW, dtype=jnp.int32))
        concat = concat.reshape(L, concat.shape[2])
        single_state, state_bf, rotation, translation = update(single_state, concat, rotation, translation, output_weight, gain_first, mlp_first, mlp_second, mlp_third, gain_second, frame_weight)
    return (single_state, rotation, translation)
```

```python
import functools

import jax
import jax.numpy as jnp
from jax import lax
from jax.experimental import pallas as pl
from jax.experimental.pallas import tpu as pltpu
from jax.sharding import Mesh
from jax.sharding import PartitionSpec as P

LAYERS = 2
SPAN = 2
GROUPS_ROW = ("groups", "row_0", "row_1", "row_2")
LOGIT_WEIGHT = (1.0 / 3.0) ** 0.5
F32 = jnp.float32
BF16 = jnp.bfloat16
LANE = 128
HP = 16


def iota(shape, dim):
    return lax.broadcasted_iota(jnp.int32, shape, dim)


def dot(a, b):
    return jnp.dot(a, b, preferred_element_type=F32)


def dot_nt(a, b):
    return lax.dot_general(a, b, (((1,), (1,)), ((), ())), preferred_element_type=F32)


def split2(x):
    hi = x.astype(BF16)
    return hi, (x - hi.astype(F32)).astype(BF16)


def split3(x):
    hi = x.astype(BF16)
    rest = x - hi.astype(F32)
    mid = rest.astype(BF16)
    return hi, mid, (rest - mid.astype(F32)).astype(BF16)


def spread(x, table):
    hi, mid, lo = split3(x)
    return dot(hi, table) + dot(mid, table) + dot(lo, table)


def col(tile, lane):
    return jnp.broadcast_to(tile[:, lane : lane + 1], tile.shape)


def layer_norm(values, gain_vector):
    centered = values - jnp.mean(values, axis=-1, keepdims=True)
    variance = jnp.mean(centered * centered, axis=-1, keepdims=True)
    return centered * lax.rsqrt(variance + 1e-05) * gain_vector


def kernel(
    sizes,
    pair,
    single,
    rotation,
    translation,
    mask,
    chain,
    wq_hbm,
    wk_hbm,
    wv_hbm,
    wqp_hbm,
    wkp_hbm,
    wvp_hbm,
    pw_ref,
    hw_ref,
    cw_ref,
    wo_hbm,
    g1_ref,
    m1_hbm,
    m2_hbm,
    m3_hbm,
    g2_ref,
    fw_ref,
    out_state,
    out_frames,
    tile,
    kx,
    qx,
    xs,
    wqr,
    wkr,
    wvr,
    wqpr,
    wkpr,
    wvpr,
    wq,
    wk,
    wv,
    wo,
    m1,
    m2,
    m3,
    dec,
    expm,
    qf,
    kf,
    vh,
    vl,
    scores,
    bias,
    same,
    mh,
    me_mask,
    po,
    spb,
    ssb,
    pr,
    sr,
    w_sem,
    wo_sem,
    a2a_recv,
    a2a_send,
    x_send,
    kx_recv,
    qx_recv,
    p_send,
    s_send,
    p_recv,
    s_recv,
):
    nx, nb, cores, rows, heads = sizes
    g_count = nx * SPAN * cores
    nk = g_count * rows
    nq = nb * rows
    chan = single.shape[1]
    pq3 = wqp_hbm.shape[1]
    pqh = pq3 // 3
    pq = pqh // heads
    pv3 = wvp_hbm.shape[1]
    pvh = pv3 // 3
    pv = pvh // heads
    hd = wq_hbm.shape[1]
    dh = hd // heads
    vtail = LANE - pvh
    x = lax.axis_index("row_0")
    z = lax.axis_index("row_1")
    c = lax.axis_index("row_2")
    zb = z // SPAN
    zp = z % SPAN
    me = (x * SPAN + zp) * cores + c

    near = []
    for dx in (2, 1, 3, 0) if nx == 4 else range(nx):
        for dz in range(SPAN):
            for dc in range(cores):
                if dx or dz or dc:
                    near.append((dx, dz, dc))

    def near_id(offset):
        dx, dz, dc = offset
        return (x + dx) % nx, (zp + dz) % SPAN, (c + dc) % cores

    def dev(px, pz, pc):
        return {"row_0": px, "row_1": pz, "row_2": pc}

    def near_dev(offset):
        px, pzp, pc = near_id(offset)
        return dev(px, zb * SPAN + pzp, pc)

    def far_dev(block):
        return dev(x, block * SPAN + zp, c)

    def far_step(t):
        half = (t + 1) // 2
        sign = 1 - 2 * (t % 2)
        return (zb + nb // 2 + sign * half + nb) % nb

    barrier = pltpu.get_barrier_semaphore()
    for t in range(nb - 1):
        pl.semaphore_signal(
            barrier, inc=1, device_id=far_dev(far_step(t)), device_id_type=pl.DeviceIdType.MESH
        )
    for offset in near:
        pl.semaphore_signal(
            barrier, inc=1, device_id=near_dev(offset), device_id_type=pl.DeviceIdType.MESH
        )

    raw = [
        (wq_hbm, wqr),
        (wk_hbm, wkr),
        (wv_hbm, wvr),
        (wqp_hbm, wqpr),
        (wkp_hbm, wkpr),
        (wvp_hbm, wvpr),
        (m1_hbm, m1),
        (m2_hbm, m2),
        (m3_hbm, m3),
    ]
    raw_copies = [
        pltpu.make_async_copy(src, dst, w_sem.at[k]) for k, (src, dst) in enumerate(raw)
    ]
    for copy in raw_copies:
        copy.start()
    base_pt = hd
    base_norm = hd + pv3
    base_pair = base_norm + pvh
    wo_moves = [
        (base_pt, 0, pvh),
        (base_pt + pvh, LANE, pvh),
        (0, LANE + pvh, vtail),
        (base_pt + 2 * pvh, 2 * LANE, pvh),
        (vtail, 2 * LANE + pvh, vtail),
        (2 * vtail, 3 * LANE, hd - 2 * vtail),
        (base_norm, 4 * LANE, pvh),
        (base_pair, 5 * LANE, heads * LANE),
    ]
    wo[pvh:LANE, :] = jnp.zeros((vtail, chan), BF16)
    wo[4 * LANE + pvh : 5 * LANE, :] = jnp.zeros((vtail, chan), BF16)
    wo_copies = [
        pltpu.make_async_copy(
            wo_hbm.at[pl.ds(src, count)], wo.at[pl.ds(dst, count)], wo_sem.at[k]
        )
        for k, (src, dst, count) in enumerate(wo_moves)
    ]
    for copy in wo_copies:
        copy.start()

    lane8 = iota((rows, LANE), 1)
    take_r = (
        (iota((9, LANE), 1) % 12 == iota((9, LANE), 0)) & (iota((9, LANE), 1) < 36)
    ).astype(F32)
    take_t = (
        (iota((3, LANE), 1) % 12 == iota((3, LANE), 0) + 9) & (iota((3, LANE), 1) < 36)
    ).astype(F32)
    contract0 = (((0,), (0,)), ((), ()))
    frames = lax.dot_general(
        rotation[...], take_r, contract0, precision=lax.Precision.HIGHEST,
        preferred_element_type=F32,
    ) + lax.dot_general(
        translation[...], take_t, contract0, precision=lax.Precision.HIGHEST,
        preferred_element_type=F32,
    )

    def frame_columns(fr):
        hi = fr.astype(BF16).astype(F32)
        mid = (fr - hi).astype(BF16).astype(F32)
        lo = fr - hi - mid
        return jnp.where(lane8 < 12, hi, jnp.where(lane8 < 24, mid, lo)).astype(BF16)

    def put_message(layer, state_bf, fr):
        tail = frame_columns(fr)
        for ref in (xs.at[layer], kx.at[layer, me], qx.at[layer, zb]):
            ref[:, 0:chan] = state_bf
            ref[:, chan : chan + LANE] = tail

    def x_near(layer, offset):
        return pltpu.make_async_remote_copy(
            src_ref=xs.at[layer],
            dst_ref=kx.at[layer, me],
            send_sem=x_send.at[layer],
            recv_sem=kx_recv.at[layer],
            device_id=near_dev(offset),
            device_id_type=pl.DeviceIdType.MESH,
        )

    def x_far(layer, t):
        return pltpu.make_async_remote_copy(
            src_ref=xs.at[layer],
            dst_ref=qx.at[layer, zb],
            send_sem=x_send.at[layer],
            recv_sem=qx_recv.at[layer],
            device_id=far_dev(far_step(t)),
            device_id_type=pl.DeviceIdType.MESH,
        )

    def send_message(layer):
        for t in range(nb - 1):
            x_far(layer, t).start()
        for offset in near:
            x_near(layer, offset).start()

    put_message(0, single[...], frames)
    pl.semaphore_wait(barrier, len(near) + nb - 1)
    send_message(0)

    def a2a_step(t, carry):
        n = far_step(t)
        for offset in near:
            px, pzp, pc = near_id(offset)
            pltpu.make_async_remote_copy(
                src_ref=pair.at[px, n, pzp, pc],
                dst_ref=tile.at[n, :, pl.ds(me * rows, rows), :],
                send_sem=a2a_send,
                recv_sem=a2a_recv.at[n],
                device_id=dev(px, zb * SPAN + pzp, pc),
                device_id_type=pl.DeviceIdType.MESH,
            ).start()
        pltpu.make_async_copy(
            pair.at[x, n, zp, c], tile.at[n, :, pl.ds(me * rows, rows), :], a2a_recv.at[n]
        ).start()
        return carry

    lax.fori_loop(0, nb, a2a_step, 0)

    lane_row = iota((1, LANE), 1)

    def as_col(row):
        wide = jnp.broadcast_to(row, (HP, heads))
        pick = iota((HP, heads), 0) == iota((HP, heads), 1)
        return jnp.sum(jnp.where(pick, wide, 0.0), axis=1, keepdims=True)

    hw = hw_ref[...]
    soft = jnp.maximum(hw, 0.0) + jnp.log(1.0 + jnp.exp(-jnp.abs(hw)))
    w_col = as_col(soft * (2.0 / (9.0 * pq)) ** 0.5)
    cw_col = as_col(cw_ref[...])

    head_of = iota((HP, LANE), 0)
    lane_hp = iota((HP, LANE), 1)
    q_tail = hd - LANE
    qq0 = q_tail
    kk0 = q_tail + 2 * heads
    kk1 = kk0 + 3 * heads
    point_mask = ((lane_hp % pqh) // pq == head_of) & (lane_hp < 2 * pqh)
    tail_mask = ((lane_hp < q_tail) & ((lane_hp + LANE) // dh == head_of)) | (
        (lane_hp >= q_tail) & ((lane_hp - q_tail) % heads == head_of) & (lane_hp < kk1)
    )
    mh[:, 0:LANE] = (lane_hp // dh == head_of).astype(F32)
    mh[:, LANE : 2 * LANE] = tail_mask.astype(F32)
    for k in range(6):
        mh[:, (2 + k) * LANE : (3 + k) * LANE] = point_mask.astype(F32)
    v_mask = (lane_hp // pv == head_of) & (lane_hp < pvh)
    o_masks = [
        (lane_hp - pvh == head_of),
        ((lane_hp - pvh) // dh == head_of),
        ((lane_hp - pvh + vtail) // dh == head_of),
    ]
    for k in range(3):
        me_mask[:, k * LANE : (k + 1) * LANE] = (
            v_mask | ((lane_hp >= pvh) & o_masks[k])
        ).astype(F32)
    me_mask[:, 3 * LANE : 4 * LANE] = ((lane_hp + 2 * vtail) // dh == head_of).astype(F32)
    big_row = iota((LANE, 4 * LANE), 0) - pvh
    big_col = iota((LANE, 4 * LANE), 1)
    big_lane = big_col % LANE
    big_tile = big_col // LANE
    o_col = jnp.where(
        big_tile == 3, big_lane + 2 * vtail, big_lane - pvh + (big_tile - 1) * vtail
    )
    is_point = (big_tile < 3) & (big_lane < pvh)
    big_head = jnp.where(is_point, big_lane // pv, o_col // dh)
    has_head = is_point | (big_tile > 0)
    expm[...] = (
        (big_head == big_row) & has_head & (big_row >= 0) & (big_row < heads)
    ).astype(BF16)
    w_lane = jnp.sum(jnp.where(point_mask, w_col, 0.0), axis=0, keepdims=True)
    half_lane = -0.5 * jnp.sum(
        jnp.where((lane_hp - q_tail) % heads == head_of, w_col, 0.0), axis=0, keepdims=True
    )
    dec_row = iota((LANE, LANE), 0)
    for k in range(12):
        dec[:, k * LANE : (k + 1) * LANE] = ((dec_row % 12 == k) & (dec_row < 36)).astype(BF16)
    sel = (
        (iota((LANE, LANE), 0) < pqh)
        & (iota((LANE, LANE), 1) >= q_tail)
        & (iota((LANE, LANE), 1) < kk1)
        & ((iota((LANE, LANE), 1) - q_tail) % heads == iota((LANE, LANE), 0) // pq)
    ).astype(BF16)

    chain_v = chain[...]
    mask_v = mask[...]

    def total(values):
        return jnp.sum(
            jnp.sum(values.astype(F32), axis=1, keepdims=True), axis=0, keepdims=True
        )

    block_rows = SPAN * cores * rows
    key_local = iota((1, nk), 1)
    key_index = (
        (key_local // block_rows) * (nb * block_rows) + zb * block_rows + key_local % block_rows
    ).astype(F32)
    q_local = iota((nq, 1), 0)
    q_index = (
        x * (nb * block_rows)
        + (q_local // rows) * block_rows
        + (zp * cores + c) * rows
        + q_local % rows
    ).astype(F32)
    key_chain = jnp.zeros((1, nk), F32)
    q_chain = jnp.zeros((nq, 1), F32)
    for k in range(1, 4):
        edge = total(chain_v < k)
        key_chain = key_chain + (key_index >= edge).astype(F32)
        q_chain = q_chain + (q_index >= edge).astype(F32)
    same[...] = (q_chain == key_chain).astype(F32)
    pad_row = ((key_index < total(mask_v)).astype(F32) - 1.0) * 100000.0

    for copy in raw_copies:
        copy.wait()

    def perm(count, tile_index, width, copies):
        a = iota((count, LANE), 0)
        b = iota((count, LANE), 1)
        return ((a == tile_index * width + b % width) & (b < copies * width)).astype(BF16)

    for raw_w, raw_p, full, scale in ((wqr, wqpr, wq, 0.25), (wkr, wkpr, wk, 1.0)):
        full[:, 0:LANE] = raw_w[:, 0:LANE] * jnp.asarray(scale, BF16)
        full[:, LANE : 2 * LANE] = jnp.zeros((chan, LANE), BF16)
        full[:, LANE:hd] = raw_w[:, LANE:hd] * jnp.asarray(scale, BF16)
        for k in range(3):
            full[:, (2 + k) * LANE : (3 + k) * LANE] = dot(
                raw_p[...], perm(pq3, k, pqh, 2)
            ).astype(BF16)

    def v_pick(k):
        a = iota((hd, LANE), 0)
        b = iota((hd, LANE), 1)
        start = 2 * vtail if k == 3 else (k - 1) * vtail - pvh
        return ((a == b + start) & ((b >= pvh) | (k == 3))).astype(BF16)

    for k in range(4):
        acc = jnp.zeros((chan, LANE), F32)
        if k < 3:
            acc = acc + dot(wvpr[...], perm(pv3, k, pvh, 1))
        if k > 0:
            acc = acc + dot(wvr[...], v_pick(k))
        wv[:, k * LANE : (k + 1) * LANE] = acc.astype(BF16)

    pw16 = jnp.concatenate([pw_ref[...].astype(F32), jnp.zeros((HP - heads, LANE), F32)], axis=0)
    pw16 = pw16.astype(BF16)

    def global_points(px, py, pz, fb):
        def part(k):
            return fb[:, k * LANE : (k + 1) * LANE]

        return [
            part(3 * k) * px + part(3 * k + 1) * py + part(3 * k + 2) * pz + part(9 + k)
            for k in range(3)
        ]

    def tiles(values, start, count):
        return [values[:, (start + k) * LANE : (start + k + 1) * LANE] for k in range(count)]

    def key_phase(layer):
        message = kx[layer].reshape(nk, chan + LANE)
        fb = dot(message[:, chan:], dec[...])
        body = message[:, :chan]
        projected = dot(body, wk[...])
        lane = iota((nk, LANE), 1)
        g = global_points(*tiles(projected, 2, 3), fb)
        square = g[0] * g[0] + g[1] * g[1] + g[2] * g[2]
        kk = spread(square, sel) * half_lane
        hi = kk.astype(BF16).astype(F32)
        mid = (kk - hi).astype(BF16).astype(F32)
        lo = kk - hi - mid
        kk = jnp.where(lane < kk0 + heads, hi, jnp.where(lane < kk0 + 2 * heads, mid, lo))
        kk = jnp.where(lane < kk1, kk, 0.0)
        tail = jnp.where(
            lane < q_tail, projected[:, LANE : 2 * LANE], jnp.where(lane < kk0, 1.0, kk)
        )
        kf[:, 0:LANE] = projected[:, 0:LANE].astype(BF16)
        kf[:, LANE : 2 * LANE] = tail.astype(BF16)
        for k in range(3):
            hi = g[k].astype(BF16).astype(F32)
            pts = jnp.where(lane < pqh, hi, jnp.where(lane < 2 * pqh, g[k] - hi, 0.0)).astype(BF16)
            kf[:, (2 + k) * LANE : (3 + k) * LANE] = pts
            kf[:, (5 + k) * LANE : (6 + k) * LANE] = pts
        values = dot(body, wv[...])
        parts = tiles(values, 0, 4)
        g = global_points(parts[0], parts[1], parts[2], fb)
        for k in range(3):
            whole = jnp.where(lane < pvh, g[k], parts[k])
            hi = whole.astype(BF16)
            vh[:, k * LANE : (k + 1) * LANE] = hi
            vl[:, k * LANE : (k + 1) * LANE] = jnp.where(
                lane < pvh, whole - hi.astype(F32), 0.0
            ).astype(BF16)
        vh[:, 3 * LANE : 4 * LANE] = parts[3].astype(BF16)

    def query_phase(layer):
        message = qx[layer].reshape(nq, chan + LANE)
        fb = dot(message[:, chan:], dec[...])
        projected = dot(message[:, :chan], wq[...])
        lane = iota((nq, LANE), 1)
        g = global_points(*tiles(projected, 2, 3), fb)
        square = g[0] * g[0] + g[1] * g[1] + g[2] * g[2]
        qq = spread(square, sel) * half_lane
        hi = qq.astype(BF16).astype(F32)
        qq = jnp.where(lane < qq0 + heads, hi, qq - hi)
        tail = jnp.where(
            lane < q_tail,
            projected[:, LANE : 2 * LANE],
            jnp.where(lane < kk0, qq, jnp.where(lane < kk1, 1.0, 0.0)),
        )
        qf[:, 0:LANE] = projected[:, 0:LANE].astype(BF16).astype(F32)
        qf[:, LANE : 2 * LANE] = tail.astype(BF16).astype(F32)
        for k in range(3):
            scaled = g[k] * w_lane
            hi = scaled.astype(BF16).astype(F32)
            qf[:, (2 + k) * LANE : (3 + k) * LANE] = hi
            qf[:, (5 + k) * LANE : (6 + k) * LANE] = jnp.where(lane < pqh, scaled - hi, 0.0)

    group = 2 * rows

    def score_phase(layer):
        def step(j, carry):
            parts = []
            for r in range(group):
                row = qf[pl.ds(j * group + r, 1), :]
                parts.append((jnp.broadcast_to(row, (HP, 8 * LANE)) * mh[...]).astype(BF16))
            s = dot_nt(jnp.concatenate(parts, axis=0), kf[...])
            for r in range(group):
                match = jnp.broadcast_to(same[pl.ds(j * group + r, 1), :], (HP, nk))
                value = s[r * HP : (r + 1) * HP, :] * LOGIT_WEIGHT + match * cw_col + pad_row
                start = pl.multiple_of((j * group + r) * HP, HP)
                if layer > 0:
                    value = value + bias[pl.ds(start, HP), :]
                scores[pl.ds(start, HP), :] = value
            return carry

        lax.fori_loop(0, nq // group, step, 0)

    def p_copy(layer, n):
        return pltpu.make_async_remote_copy(
            src_ref=spb.at[layer, n],
            dst_ref=pr.at[layer, zb],
            send_sem=p_send.at[layer],
            recv_sem=p_recv.at[layer, zb],
            device_id=far_dev(n),
            device_id_type=pl.DeviceIdType.MESH,
        )

    def s_copy(layer, n):
        return pltpu.make_async_remote_copy(
            src_ref=ssb.at[layer, n],
            dst_ref=sr.at[layer, zb],
            send_sem=s_send.at[layer],
            recv_sem=s_recv.at[layer, zb],
            device_id=far_dev(n),
            device_id_type=pl.DeviceIdType.MESH,
        )

    def chunk_phase(layer):
        def chunk(t):
            n = far_step(t)
            if layer == 0:
                pltpu.make_async_copy(tile.at[n], tile.at[n], a2a_recv.at[n]).wait()
            weights = []
            inverses = []
            sums = []
            for r in range(rows):
                start = pl.multiple_of((n * rows + r) * HP, HP)
                logits = scores[pl.ds(start, HP), :]
                pair_rows = tile[n, r]
                if layer == 0:
                    own_bias = dot_nt(pw16, pair_rows) * LOGIT_WEIGHT
                    bias[pl.ds(start, HP), :] = own_bias
                    logits = logits + own_bias
                top = jnp.max(logits, axis=1, keepdims=True)
                p = jnp.exp(logits - top)
                count = jnp.sum(p, axis=1, keepdims=True)
                p = p.astype(BF16)
                inverse = 1.0 / count
                po[r * HP : (r + 1) * HP, :] = dot(p, pair_rows) * inverse
                weights.append(p)
                inverses.append(inverse)
                sums.append(top + jnp.log(count))
            p_all = jnp.concatenate(weights, axis=0)
            main = dot(p_all, vh[...])
            rest = dot(p_all, vl[...])
            for r in range(rows):
                low = r * HP
                for k in range(4):
                    value = main[low : low + HP, k * LANE : (k + 1) * LANE]
                    if k < 3:
                        value = value + rest[low : low + HP, k * LANE : (k + 1) * LANE]
                    value = value * inverses[r]
                    if k == 0:
                        value = jnp.where(lane_hp < pvh, value, sums[r])
                    value = value * me_mask[:, k * LANE : (k + 1) * LANE]
                    ssb[layer, n, r : r + 1, k * LANE : (k + 1) * LANE] = jnp.sum(
                        value, axis=0, keepdims=True
                    )
            for h in range(heads):
                spb[layer, n, h] = po[pl.ds(h, rows, stride=HP), :].astype(BF16)
            return n

        def step(t, carry):
            n = chunk(t)
            p_copy(layer, n).start()
            s_copy(layer, n).start()
            return carry

        lax.fori_loop(0, nb - 1, step, 0)
        chunk(nb - 1)

    valid = (lane8 >= pvh) & (lane8 < pvh + heads)

    def combine(layer):
        small = [ssb[layer, zb]]
        slots = [zb]
        for d in range(1, nb):
            n = (zb + d) % nb
            slots.append(n)
            pltpu.make_async_copy(
                sr.at[layer, n], sr.at[layer, n], s_recv.at[layer, n]
            ).wait()
            small.append(sr[layer, n])
        sums = [jnp.where(valid, value[:, 0:LANE], 0.0) for value in small]
        top = functools.reduce(jnp.maximum, sums)
        shares = [jnp.where(valid, jnp.exp(value - top), 0.0) for value in sums]
        whole = jnp.where(valid, functools.reduce(jnp.add, shares), 1.0)
        shares = [value / whole for value in shares]
        wide = spread(jnp.concatenate(shares, axis=0), expm[...])
        mixed = functools.reduce(
            jnp.add, [wide[d * rows : (d + 1) * rows, :] * small[d] for d in range(nb)]
        )
        for d in range(1, nb):
            pltpu.make_async_copy(
                pr.at[layer, slots[d]], pr.at[layer, slots[d]], p_recv.at[layer, slots[d]]
            ).wait()
        pairs = []
        for h in range(heads):
            acc = None
            for d in range(nb):
                part = spb[layer, zb, h] if d == 0 else pr[layer, slots[d], h]
                term = col(shares[d], pvh + h) * part.astype(F32)
                acc = term if acc is None else acc + term
            pairs.append(acc)
        return mixed, pairs

    def update(layer, state, fr, mixed, pairs):
        turn = [col(fr, k) for k in range(9)]
        shift = [col(fr, 9 + k) for k in range(3)]
        mix = tiles(mixed, 0, 4)
        moved = [mix[k] - shift[k] for k in range(3)]
        local = [
            turn[k] * moved[0] + turn[3 + k] * moved[1] + turn[6 + k] * moved[2] for k in range(3)
        ]
        inside = lane8 < pvh
        norm = jnp.sqrt(
            local[0] * local[0] + local[1] * local[1] + local[2] * local[2] + 1e-08
        )
        concat = [
            jnp.where(inside, local[0], 0.0),
            jnp.where(inside, local[1], mix[1]),
            jnp.where(inside, local[2], mix[2]),
            mix[3],
            jnp.where(inside, norm, 0.0),
        ] + pairs
        concat = jnp.concatenate(concat, axis=1).astype(BF16)
        if layer == 0:
            for copy in wo_copies:
                copy.wait()
        state = state + dot(concat, wo[...])
        normed = layer_norm(state, g1_ref[...])
        hidden = jnp.maximum(dot(normed.astype(BF16), m1[...]), 0.0).astype(BF16)
        hidden = jnp.maximum(dot(hidden, m2[...]), 0.0).astype(BF16)
        state = layer_norm(normed + dot(hidden, m3[...]), g2_ref[...])
        state_bf = state.astype(BF16)
        upd = dot(state_bf, fw_ref[...])
        u = [jnp.broadcast_to(upd[:, k : k + 1], (rows, LANE)) for k in range(6)]
        inverse = lax.rsqrt(1.0 + u[0] * u[0] + u[1] * u[1] + u[2] * u[2])
        vx, vy, vz = u[0] * inverse, u[1] * inverse, u[2] * inverse
        square = inverse * inverse
        matrix = [
            [
                square + vx * vx - vy * vy - vz * vz,
                2.0 * (vx * vy - inverse * vz),
                2.0 * (vx * vz + inverse * vy),
            ],
            [
                2.0 * (vx * vy + inverse * vz),
                square - vx * vx + vy * vy - vz * vz,
                2.0 * (vy * vz - inverse * vx),
            ],
            [
                2.0 * (vx * vz - inverse * vy),
                2.0 * (vy * vz + inverse * vx),
                square - vx * vx - vy * vy + vz * vz,
            ],
        ]
        entries = [
            turn[3 * a] * matrix[0][b]
            + turn[3 * a + 1] * matrix[1][b]
            + turn[3 * a + 2] * matrix[2][b]
            for a in range(3)
            for b in range(3)
        ] + [
            turn[3 * a] * u[3] + turn[3 * a + 1] * u[4] + turn[3 * a + 2] * u[5] + shift[a]
            for a in range(3)
        ]
        fr = jnp.zeros((rows, LANE), F32)
        for k in range(12):
            fr = jnp.where((lane8 % 12 == k) & (lane8 < 36), entries[k], fr)
        return state, state_bf, fr

    state = single[...].astype(F32)
    for layer in range(LAYERS):
        pltpu.make_async_copy(
            kx.at[layer, 0 : g_count - 1], kx.at[layer, 0 : g_count - 1], kx_recv.at[layer]
        ).wait()
        key_phase(layer)
        pltpu.make_async_copy(
            qx.at[layer, 0 : nb - 1], qx.at[layer, 0 : nb - 1], qx_recv.at[layer]
        ).wait()
        query_phase(layer)
        score_phase(layer)
        chunk_phase(layer)
        mixed, pairs = combine(layer)
        state, state_bf, frames = update(layer, state, frames, mixed, pairs)
        if layer + 1 < LAYERS:
            put_message(layer + 1, state_bf, frames)
            send_message(layer + 1)
    out_state[...] = state
    out_frames[...] = frames

    for layer in range(LAYERS):
        pltpu.make_async_copy(
            kx.at[layer, 0 : g_count - 1], kx.at[layer, 0 : g_count - 1], x_send.at[layer]
        ).wait()
        pltpu.make_async_copy(
            qx.at[layer, 0 : nb - 1], qx.at[layer, 0 : nb - 1], x_send.at[layer]
        ).wait()
        pltpu.make_async_copy(
            pr.at[layer, 0 : nb - 1], pr.at[layer, 0 : nb - 1], p_send.at[layer]
        ).wait()
        pltpu.make_async_copy(
            sr.at[layer, 0 : nb - 1], sr.at[layer, 0 : nb - 1], s_send.at[layer]
        ).wait()
    for offset in near:
        px, pzp, pc = near_id(offset)
        pltpu.make_async_copy(pair.at[px, :, pzp, pc], pair.at[px, :, pzp, pc], a2a_send).wait()


def on_device(
    pair_cols,
    single,
    rotation,
    translation,
    residue_mask,
    chain_index,
    query_weight,
    key_weight,
    value_weight,
    qpoint_weight,
    kpoint_weight,
    vpoint_weight,
    pair_weight,
    head_weight,
    chain_weight,
    output_weight,
    gain_first,
    mlp_first,
    mlp_second,
    mlp_third,
    gain_second,
    frame_weight,
):
    nx = lax.axis_size("row_0")
    nz = lax.axis_size("row_1")
    cores = lax.axis_size("row_2")
    nb = nz // SPAN
    rows, chan = single.shape
    heads = head_weight.shape[0]
    hd = query_weight.shape[1]
    g_count = nx * SPAN * cores
    nk = g_count * rows
    nq = nb * rows
    width = chan + LANE
    pair = pair_cols.reshape(nx, nb, SPAN, cores, rows, *pair_cols.shape[1:])
    vmem = pl.BlockSpec(memory_space=pltpu.VMEM)
    hbm = pl.BlockSpec(memory_space=pl.ANY)
    in_specs = [hbm] + [vmem] * 5 + [hbm] * 6 + [vmem] * 3 + [hbm, vmem] + [hbm] * 3 + [vmem] * 2
    scratch = [
        pltpu.VMEM((nb, rows, nk, LANE), BF16),
        pltpu.VMEM((LAYERS, g_count, rows, width), BF16),
        pltpu.VMEM((LAYERS, nb, rows, width), BF16),
        pltpu.VMEM((LAYERS, rows, width), BF16),
        pltpu.VMEM(query_weight.shape, BF16),
        pltpu.VMEM(key_weight.shape, BF16),
        pltpu.VMEM(value_weight.shape, BF16),
        pltpu.VMEM(qpoint_weight.shape, BF16),
        pltpu.VMEM(kpoint_weight.shape, BF16),
        pltpu.VMEM(vpoint_weight.shape, BF16),
        pltpu.VMEM((chan, 5 * LANE), BF16),
        pltpu.VMEM((chan, 5 * LANE), BF16),
        pltpu.VMEM((chan, 4 * LANE), BF16),
        pltpu.VMEM(((5 + heads) * LANE, chan), BF16),
        pltpu.VMEM(mlp_first.shape, BF16),
        pltpu.VMEM(mlp_second.shape, BF16),
        pltpu.VMEM(mlp_third.shape, BF16),
        pltpu.VMEM((LANE, 12 * LANE), BF16),
        pltpu.VMEM((LANE, 4 * LANE), BF16),
        pltpu.VMEM((nq, 8 * LANE), F32),
        pltpu.VMEM((nk, 8 * LANE), BF16),
        pltpu.VMEM((nk, 4 * LANE), BF16),
        pltpu.VMEM((nk, 3 * LANE), BF16),
        pltpu.VMEM((nq * HP, nk), F32),
        pltpu.VMEM((nq * HP, nk), F32),
        pltpu.VMEM((nq, nk), F32),
        pltpu.VMEM((HP, 8 * LANE), F32),
        pltpu.VMEM((HP, 4 * LANE), F32),
        pltpu.VMEM((rows * HP, LANE), F32),
        pltpu.VMEM((LAYERS, nb, heads, rows, LANE), BF16),
        pltpu.VMEM((LAYERS, nb, rows, 4 * LANE), F32),
        pltpu.VMEM((LAYERS, nb, heads, rows, LANE), BF16),
        pltpu.VMEM((LAYERS, nb, rows, 4 * LANE), F32),
        pltpu.SemaphoreType.DMA((9,)),
        pltpu.SemaphoreType.DMA((8,)),
        pltpu.SemaphoreType.DMA((nb,)),
        pltpu.SemaphoreType.DMA,
        pltpu.SemaphoreType.DMA((LAYERS,)),
        pltpu.SemaphoreType.DMA((LAYERS,)),
        pltpu.SemaphoreType.DMA((LAYERS,)),
        pltpu.SemaphoreType.DMA((LAYERS,)),
        pltpu.SemaphoreType.DMA((LAYERS,)),
        pltpu.SemaphoreType.DMA((LAYERS, nb)),
        pltpu.SemaphoreType.DMA((LAYERS, nb)),
    ]
    state, frames = pl.pallas_call(
        functools.partial(kernel, (nx, nb, cores, rows, heads)),
        name="structure_layers",
        out_shape=(
            jax.ShapeDtypeStruct((rows, chan), F32),
            jax.ShapeDtypeStruct((rows, LANE), F32),
        ),
        in_specs=in_specs,
        out_specs=(vmem, vmem),
        scratch_shapes=scratch,
        compiler_params=pltpu.CompilerParams(
            collective_id=0, has_side_effects=True, vmem_limit_bytes=48 * 1024 * 1024
        ),
    )(
        pair,
        single,
        rotation,
        translation,
        residue_mask.reshape(-1, LANE),
        chain_index.reshape(-1, LANE),
        query_weight,
        key_weight,
        value_weight,
        qpoint_weight,
        kpoint_weight,
        vpoint_weight,
        pair_weight,
        head_weight.reshape(1, -1),
        chain_weight.reshape(1, -1),
        output_weight,
        gain_first.reshape(1, -1),
        mlp_first,
        mlp_second,
        mlp_third,
        gain_second.reshape(1, -1),
        frame_weight,
    )
    return state, jnp.transpose(frames[:, :9]), jnp.transpose(frames[:, 9:12])


def solution(mesh):
    finer = Mesh(
        mesh.devices.reshape(mesh.shape["groups"], 4, 16, 2), ("groups", "row_0", "row_1", "row_2")
    )
    in_specs = (
        P(None, GROUPS_ROW, None),
        P(GROUPS_ROW, None),
        P(None, GROUPS_ROW),
        P(None, GROUPS_ROW),
        P("groups"),
        P("groups"),
    ) + (P(),) * 16
    out_specs = (P(GROUPS_ROW, None), P(None, GROUPS_ROW), P(None, GROUPS_ROW))
    return jax.shard_map(
        on_device, mesh=finer, in_specs=in_specs, out_specs=out_specs, check_vma=False
    )
```

```python
import functools

import jax
import jax.numpy as jnp
from jax import lax
from jax.experimental import pallas as pl
from jax.experimental.pallas import tpu as pltpu
from jax.sharding import Mesh
from jax.sharding import PartitionSpec as P

LAYERS = 2
SPAN = 2
GROUPS_ROW = ("groups", "row_0", "row_1", "row_2")
LOGIT_WEIGHT = (1.0 / 3.0) ** 0.5
F32 = jnp.float32
BF16 = jnp.bfloat16
LANE = 128
HP = 16


def iota(shape, dim):
    return lax.broadcasted_iota(jnp.int32, shape, dim)


def dot(a, b):
    return jnp.dot(a, b, preferred_element_type=F32)


def dot_nt(a, b):
    return lax.dot_general(a, b, (((1,), (1,)), ((), ())), preferred_element_type=F32)


def split2(x):
    hi = x.astype(BF16)
    return hi, (x - hi.astype(F32)).astype(BF16)


def split3(x):
    hi = x.astype(BF16)
    rest = x - hi.astype(F32)
    mid = rest.astype(BF16)
    return hi, mid, (rest - mid.astype(F32)).astype(BF16)


def spread(x, table):
    hi, mid, lo = split3(x)
    return dot(hi, table) + dot(mid, table) + dot(lo, table)


def col(tile, lane):
    return jnp.broadcast_to(tile[:, lane : lane + 1], tile.shape)


def layer_norm(values, gain_vector):
    centered = values - jnp.mean(values, axis=-1, keepdims=True)
    variance = jnp.mean(centered * centered, axis=-1, keepdims=True)
    return centered * lax.rsqrt(variance + 1e-05) * gain_vector


def kernel(
    sizes,
    pair,
    single,
    rotation,
    translation,
    mask,
    chain,
    wq_hbm,
    wk_hbm,
    wv_hbm,
    wqp_hbm,
    wkp_hbm,
    wvp_hbm,
    pw_ref,
    hw_ref,
    cw_ref,
    wo_hbm,
    g1_ref,
    m1_hbm,
    m2_hbm,
    m3_hbm,
    g2_ref,
    fw_ref,
    out_state,
    out_turn,
    out_shift,
    tile,
    kx,
    qx,
    xs,
    wqt,
    wkt,
    wvt,
    wq,
    wk,
    wv,
    wo,
    m1,
    m2,
    m3,
    dec,
    expm,
    qf,
    kf,
    vh,
    vl,
    scores,
    bias,
    same,
    mh,
    me_mask,
    po,
    sm,
    fq,
    spb,
    pr,
    w_sem,
    wo_sem,
    a2a_recv,
    a2a_send,
    x_send,
    kx_recv,
    qx_recv,
    p_send,
    p_recv,
):
    nx, nb, cores, rows, heads = sizes
    g_count = nx * SPAN * cores
    nk = g_count * rows
    nq = nb * rows
    chan = single.shape[1]
    pq3 = wqp_hbm.shape[0]
    pqh = pq3 // 3
    pq = pqh // heads
    pv3 = wvp_hbm.shape[0]
    pvh = pv3 // 3
    pv = pvh // heads
    hd = wq_hbm.shape[0]
    dh = hd // heads
    vtail = LANE - pvh
    x = lax.axis_index("row_0")
    z = lax.axis_index("row_1")
    c = lax.axis_index("row_2")
    nz = nb * SPAN
    zb = z // SPAN
    zp = z % SPAN

    def partner(core):
        return (z + 1 - 2 * ((z + core) % SPAN) + nz) % nz

    def place(core):
        return (x * SPAN + (z + core) % SPAN) * cores + c

    me = place(c)
    near = []
    for dx in (2, 1, 3, 0) if nx == 4 else range(nx):
        for dz in range(SPAN):
            for dc in range(cores):
                if dx or dz or dc:
                    near.append((dx, dz, dc))

    def near_id(offset):
        dx, dz, dc = offset
        core = (c + dc) % cores
        return (x + dx) % nx, partner(core) if dz else z, core

    def source_id(offset):
        dx, dz, dc = offset
        return (x + dx) % nx, partner(c) if dz else z, (c + dc) % cores

    def dev(px, pz, pc):
        return {"row_0": px, "row_1": pz, "row_2": pc}

    def far_dev(block):
        return dev(x, block * SPAN + zp, c)

    def far_step(t):
        half = (t + 1) // 2
        sign = 1 - 2 * (t % 2)
        return (zb + nb // 2 + sign * half + nb) % nb

    barrier = pltpu.get_barrier_semaphore()
    for t in range(nb - 1):
        pl.semaphore_signal(
            barrier, inc=1, device_id=far_dev(far_step(t)), device_id_type=pl.DeviceIdType.MESH
        )
    for offset in near:
        pl.semaphore_signal(
            barrier,
            inc=1,
            device_id=dev(*source_id(offset)),
            device_id_type=pl.DeviceIdType.MESH,
        )

    moves = [(wq_hbm, 0, wqt, 0, hd), (wk_hbm, 0, wkt, 0, hd)]
    for src, dst in ((wqp_hbm, wqt), (wkp_hbm, wkt)):
        for k in range(3):
            for copy_index in range(2):
                moves.append((src, k * pqh, dst, (2 + k) * LANE + copy_index * pqh, pqh))
    for k in range(3):
        moves.append((wvp_hbm, k * pvh, wvt, k * LANE, pvh))
    moves += [
        (wv_hbm, 0, wvt, LANE + pvh, vtail),
        (wv_hbm, vtail, wvt, 2 * LANE + pvh, vtail),
        (wv_hbm, 2 * vtail, wvt, 3 * LANE, hd - 2 * vtail),
        (m1_hbm, 0, m1, 0, chan),
        (m2_hbm, 0, m2, 0, chan),
        (m3_hbm, 0, m3, 0, chan),
    ]
    for ref in (wqt, wkt):
        ref[hd : 2 * LANE, :] = jnp.zeros((2 * LANE - hd, chan), BF16)
        for k in range(3):
            ref[(2 + k) * LANE + 2 * pqh : (3 + k) * LANE, :] = jnp.zeros(
                (LANE - 2 * pqh, chan), BF16
            )
    wvt[pvh:LANE, :] = jnp.zeros((vtail, chan), BF16)
    raw_copies = [
        pltpu.make_async_copy(
            src.at[pl.ds(start, count)], dst.at[pl.ds(into, count)], w_sem.at[k]
        )
        for k, (src, start, dst, into, count) in enumerate(moves)
    ]
    for copy in raw_copies:
        copy.start()
    base_pt = hd
    base_norm = hd + pv3
    base_pair = base_norm + pvh
    wo_moves = [
        (base_pt, 0, pvh),
        (base_pt + pvh, LANE, pvh),
        (0, LANE + pvh, vtail),
        (base_pt + 2 * pvh, 2 * LANE, pvh),
        (vtail, 2 * LANE + pvh, vtail),
        (2 * vtail, 3 * LANE, hd - 2 * vtail),
        (base_norm, 4 * LANE, pvh),
        (base_pair, 5 * LANE, heads * LANE),
    ]
    wo[pvh:LANE, :] = jnp.zeros((vtail, chan), BF16)
    wo[4 * LANE + pvh : 5 * LANE, :] = jnp.zeros((vtail, chan), BF16)
    wo_copies = [
        pltpu.make_async_copy(
            wo_hbm.at[pl.ds(src, count)], wo.at[pl.ds(dst, count)], wo_sem.at[k]
        )
        for k, (src, dst, count) in enumerate(wo_moves)
    ]
    for copy in wo_copies:
        copy.start()

    lane8 = iota((rows, LANE), 1)
    take_r = (
        (iota((9, LANE), 1) % 12 == iota((9, LANE), 0)) & (iota((9, LANE), 1) < 36)
    ).astype(F32)
    take_t = (
        (iota((3, LANE), 1) % 12 == iota((3, LANE), 0) + 9) & (iota((3, LANE), 1) < 36)
    ).astype(F32)
    contract0 = (((0,), (0,)), ((), ()))
    frames = jnp.dot(
        rotation[...], take_r, precision=lax.Precision.HIGHEST, preferred_element_type=F32
    ) + lax.dot_general(
        translation[...], take_t, contract0, precision=lax.Precision.HIGHEST,
        preferred_element_type=F32,
    )

    def frame_columns(fr):
        hi = fr.astype(BF16).astype(F32)
        mid = (fr - hi).astype(BF16).astype(F32)
        lo = fr - hi - mid
        return jnp.where(lane8 < 12, hi, jnp.where(lane8 < 24, mid, lo)).astype(BF16)

    def put_message(layer, state_bf, fr):
        tail = frame_columns(fr)
        for ref in (xs.at[layer], kx.at[layer, me], qx.at[layer, zb]):
            ref[:, 0:chan] = state_bf
            ref[:, chan : chan + LANE] = tail

    def x_near(layer, offset):
        target = near_id(offset)
        return pltpu.make_async_remote_copy(
            src_ref=xs.at[layer],
            dst_ref=kx.at[layer, place(target[2])],
            send_sem=x_send.at[layer],
            recv_sem=kx_recv.at[layer],
            device_id=dev(*target),
            device_id_type=pl.DeviceIdType.MESH,
        )

    def x_far(layer, t):
        return pltpu.make_async_remote_copy(
            src_ref=xs.at[layer],
            dst_ref=qx.at[layer, zb],
            send_sem=x_send.at[layer],
            recv_sem=qx_recv.at[layer],
            device_id=far_dev(far_step(t)),
            device_id_type=pl.DeviceIdType.MESH,
        )

    def send_message(layer):
        for t in range(nb - 1):
            x_far(layer, t).start()
        for offset in near:
            x_near(layer, offset).start()

    put_message(0, single[...], frames)
    with jax.named_scope("barrier"):
        pl.semaphore_wait(barrier, len(near) + nb - 1)
    send_message(0)

    def a2a_step(t, carry):
        n = far_step(t)
        for offset in near:
            px, pz, pc = near_id(offset)
            pltpu.make_async_remote_copy(
                src_ref=pair.at[px, n, pz % SPAN, pc],
                dst_ref=tile.at[n, :, pl.ds(place(pc) * rows, rows), :],
                send_sem=a2a_send,
                recv_sem=a2a_recv.at[n],
                device_id=dev(px, pz, pc),
                device_id_type=pl.DeviceIdType.MESH,
            ).start()
        pltpu.make_async_copy(
            pair.at[x, n, zp, c], tile.at[n, :, pl.ds(me * rows, rows), :], a2a_recv.at[n]
        ).start()
        return carry

    with jax.named_scope("exchange"):
        lax.fori_loop(0, nb, a2a_step, 0)

    lane_row = iota((1, LANE), 1)

    def as_col(row):
        wide = jnp.broadcast_to(row, (HP, heads))
        pick = iota((HP, heads), 0) == iota((HP, heads), 1)
        return jnp.sum(jnp.where(pick, wide, 0.0), axis=1, keepdims=True)

    hw = hw_ref[...]
    soft = jnp.maximum(hw, 0.0) + jnp.log(1.0 + jnp.exp(-jnp.abs(hw)))
    w_col = as_col(soft * (2.0 / (9.0 * pq)) ** 0.5)
    cw_col = as_col(cw_ref[...])

    head_of = iota((HP, LANE), 0)
    lane_hp = iota((HP, LANE), 1)
    q_tail = hd - LANE
    qq0 = q_tail
    kk0 = q_tail + 2 * heads
    kk1 = kk0 + 3 * heads
    point_mask = ((lane_hp % pqh) // pq == head_of) & (lane_hp < 2 * pqh)
    tail_mask = ((lane_hp < q_tail) & ((lane_hp + LANE) // dh == head_of)) | (
        (lane_hp >= q_tail) & ((lane_hp - q_tail) % heads == head_of) & (lane_hp < kk1)
    )
    mh[:, 0:LANE] = (lane_hp // dh == head_of).astype(F32)
    mh[:, LANE : 2 * LANE] = tail_mask.astype(F32)
    for k in range(6):
        mh[:, (2 + k) * LANE : (3 + k) * LANE] = point_mask.astype(F32)
    v_mask = (lane_hp // pv == head_of) & (lane_hp < pvh)
    o_masks = [
        ((lane_hp - pvh) % heads == head_of) & (lane_hp < pvh + 2 * heads),
        ((lane_hp - pvh) // dh == head_of),
        ((lane_hp - pvh + vtail) // dh == head_of),
    ]
    for k in range(3):
        me_mask[:, k * LANE : (k + 1) * LANE] = (
            v_mask | ((lane_hp >= pvh) & o_masks[k])
        ).astype(F32)
    me_mask[:, 3 * LANE : 4 * LANE] = ((lane_hp + 2 * vtail) // dh == head_of).astype(F32)
    big_row = iota((LANE, 4 * LANE), 0) - pvh
    big_col = iota((LANE, 4 * LANE), 1)
    big_lane = big_col % LANE
    big_tile = big_col // LANE
    o_col = jnp.where(
        big_tile == 3, big_lane + 2 * vtail, big_lane - pvh + (big_tile - 1) * vtail
    )
    is_point = (big_tile < 3) & (big_lane < pvh)
    big_head = jnp.where(is_point, big_lane // pv, o_col // dh)
    has_head = is_point | (big_tile > 0)
    expm[...] = (
        (big_head == big_row) & has_head & (big_row >= 0) & (big_row < heads)
    ).astype(BF16)
    w_lane = jnp.sum(jnp.where(point_mask, w_col, 0.0), axis=0, keepdims=True)
    half_lane = -0.5 * jnp.sum(
        jnp.where((lane_hp - q_tail) % heads == head_of, w_col, 0.0), axis=0, keepdims=True
    )
    dec_row = iota((LANE, LANE), 0)
    for k in range(12):
        dec[:, k * LANE : (k + 1) * LANE] = ((dec_row % 12 == k) & (dec_row < 36)).astype(BF16)
    sel = (
        (iota((LANE, LANE), 0) < pqh)
        & (iota((LANE, LANE), 1) >= q_tail)
        & (iota((LANE, LANE), 1) < kk1)
        & ((iota((LANE, LANE), 1) - q_tail) % heads == iota((LANE, LANE), 0) // pq)
    ).astype(BF16)

    chain_v = chain[...]
    mask_v = mask[...]

    def total(values):
        return jnp.sum(
            jnp.sum(values.astype(F32), axis=1, keepdims=True), axis=0, keepdims=True
        )

    plane_rows = cores * rows
    block_rows = SPAN * plane_rows
    key_local = iota((1, nk), 1)
    key_plane = (z - (z + c) % SPAN + (key_local // plane_rows) % SPAN + nz) % nz
    key_index = (
        ((key_local // block_rows) * nz + key_plane) * plane_rows + key_local % plane_rows
    ).astype(F32)
    q_local = iota((nq, 1), 0)
    q_index = (
        x * (nb * block_rows)
        + (q_local // rows) * block_rows
        + (zp * cores + c) * rows
        + q_local % rows
    ).astype(F32)
    key_chain = jnp.zeros((1, nk), F32)
    q_chain = jnp.zeros((nq, 1), F32)
    for k in range(1, 4):
        edge = total(chain_v < k)
        key_chain = key_chain + (key_index >= edge).astype(F32)
        q_chain = q_chain + (q_index >= edge).astype(F32)
    same[...] = (q_chain == key_chain).astype(F32)
    pad_row = ((key_index < total(mask_v)).astype(F32) - 1.0) * 100000.0

    for copy in raw_copies:
        copy.wait()
    wq[...] = jnp.transpose(wqt[...])
    wk[...] = jnp.transpose(wkt[...])
    wv[...] = jnp.transpose(wvt[...])

    pw16 = jnp.concatenate([pw_ref[...].astype(F32), jnp.zeros((HP - heads, LANE), F32)], axis=0)
    pw16 = pw16.astype(BF16)

    def global_points(px, py, pz, fb):
        def part(k):
            return fb[:, k * LANE : (k + 1) * LANE]

        return [
            part(3 * k) * px + part(3 * k + 1) * py + part(3 * k + 2) * pz + part(9 + k)
            for k in range(3)
        ]

    def tiles(values, start, count):
        return [values[:, (start + k) * LANE : (start + k + 1) * LANE] for k in range(count)]

    def key_phase(layer):
        message = kx[layer].reshape(nk, chan + LANE)
        fb = dot(message[:, chan:], dec[...])
        body = message[:, :chan]
        projected = dot(body, wk[...])
        lane = iota((nk, LANE), 1)
        g = global_points(*tiles(projected, 2, 3), fb)
        square = g[0] * g[0] + g[1] * g[1] + g[2] * g[2]
        kk = spread(square, sel) * half_lane
        hi = kk.astype(BF16).astype(F32)
        mid = (kk - hi).astype(BF16).astype(F32)
        lo = kk - hi - mid
        kk = jnp.where(lane < kk0 + heads, hi, jnp.where(lane < kk0 + 2 * heads, mid, lo))
        kk = jnp.where(lane < kk1, kk, 0.0)
        tail = jnp.where(
            lane < q_tail, projected[:, LANE : 2 * LANE], jnp.where(lane < kk0, 1.0, kk)
        )
        kf[:, 0:LANE] = projected[:, 0:LANE].astype(BF16)
        kf[:, LANE : 2 * LANE] = tail.astype(BF16)
        for k in range(3):
            hi = g[k].astype(BF16).astype(F32)
            pts = jnp.where(lane < pqh, hi, jnp.where(lane < 2 * pqh, g[k] - hi, 0.0)).astype(BF16)
            kf[:, (2 + k) * LANE : (3 + k) * LANE] = pts
            kf[:, (5 + k) * LANE : (6 + k) * LANE] = pts
        values = dot(body, wv[...])
        parts = tiles(values, 0, 4)
        g = global_points(parts[0], parts[1], parts[2], fb)
        for k in range(3):
            whole = jnp.where(lane < pvh, g[k], parts[k])
            hi = whole.astype(BF16)
            vh[:, k * LANE : (k + 1) * LANE] = hi
            vl[:, k * LANE : (k + 1) * LANE] = jnp.where(
                lane < pvh, whole - hi.astype(F32), 0.0
            ).astype(BF16)
        vh[:, 3 * LANE : 4 * LANE] = parts[3].astype(BF16)

    def query_phase(layer):
        scale = dh ** -0.5
        message = qx[layer].reshape(nq, chan + LANE)
        fb = dot(message[:, chan:], dec[...])
        fq[...] = fb
        projected = dot(message[:, :chan], wq[...])
        lane = iota((nq, LANE), 1)
        g = global_points(*tiles(projected, 2, 3), fb)
        square = g[0] * g[0] + g[1] * g[1] + g[2] * g[2]
        qq = spread(square, sel) * half_lane
        hi = qq.astype(BF16).astype(F32)
        qq = jnp.where(lane < qq0 + heads, hi, qq - hi)
        tail = jnp.where(
            lane < q_tail,
            projected[:, LANE : 2 * LANE] * scale,
            jnp.where(lane < kk0, qq, jnp.where(lane < kk1, 1.0, 0.0)),
        )
        qf[:, 0:LANE] = projected[:, 0:LANE].astype(BF16).astype(F32) * scale
        qf[:, LANE : 2 * LANE] = tail.astype(BF16).astype(F32)
        for k in range(3):
            scaled = g[k] * w_lane
            hi = scaled.astype(BF16).astype(F32)
            qf[:, (2 + k) * LANE : (3 + k) * LANE] = hi
            qf[:, (5 + k) * LANE : (6 + k) * LANE] = jnp.where(lane < pqh, scaled - hi, 0.0)

    def score_chunk(n):
        parts = []
        for r in range(rows):
            row = qf[pl.ds(n * rows + r, 1), :]
            parts.append((jnp.broadcast_to(row, (HP, 8 * LANE)) * mh[...]).astype(BF16))
        s = dot_nt(jnp.concatenate(parts, axis=0), kf[...]) * LOGIT_WEIGHT
        extra = []
        for r in range(rows):
            match = jnp.broadcast_to(same[pl.ds(n * rows + r, 1), :], (HP, nk))
            extra.append(match * cw_col + pad_row)
        return s + jnp.concatenate(extra, axis=0)

    def chunk_rows(n):
        return pl.ds(pl.multiple_of(n * rows * HP, rows * HP), rows * HP)

    def score_phase():
        def step(n, carry):
            scores[chunk_rows(n), :] = score_chunk(n)
            return carry

        lax.fori_loop(0, nb, step, 0)

    def p_copy(layer, n):
        return pltpu.make_async_remote_copy(
            src_ref=spb.at[layer, n],
            dst_ref=pr.at[layer, zb],
            send_sem=p_send.at[layer],
            recv_sem=p_recv.at[layer, zb],
            device_id=far_dev(n),
            device_id_type=pl.DeviceIdType.MESH,
        )

    lane_all = iota((rows * HP, LANE), 1)

    def chunk_phase(layer):
        def chunk(t):
            n = far_step(t)
            if layer == 0:
                logits = scores[chunk_rows(n), :]
                with jax.named_scope("tile_wait"):
                    pltpu.make_async_copy(tile.at[n], tile.at[n], a2a_recv.at[n]).wait()
                pair_rows = [tile[n, r] for r in range(rows)]
                own = jnp.concatenate([dot_nt(pw16, v) for v in pair_rows], axis=0) * LOGIT_WEIGHT
                logits = logits + own
            else:
                pair_rows = [tile[n, r] for r in range(rows)]
                logits = score_chunk(n) + bias[chunk_rows(n), :]
            top = jnp.max(logits, axis=1, keepdims=True)
            p = jnp.exp(logits - top)
            count = jnp.sum(p, axis=1, keepdims=True)
            p = p.astype(BF16)
            inverse = 1.0 / count
            log_sum = top + jnp.log(count)
            mixed = jnp.concatenate(
                [dot(p[r * HP : (r + 1) * HP, :], pair_rows[r]) for r in range(rows)], axis=0
            )
            main = dot(p, vh[...])
            rest = dot(p, vl[...])
            turn = fq[pl.ds(n * rows, rows), :]
            po[...] = mixed * inverse
            if layer == 0:
                bias[chunk_rows(n), :] = own
            for k in range(4):
                value = main[:, k * LANE : (k + 1) * LANE]
                if k < 3:
                    value = value + rest[:, k * LANE : (k + 1) * LANE]
                value = value * inverse
                if k == 0:
                    value = jnp.where(lane_all < pvh, value, log_sum)
                for r in range(rows):
                    sm[r : r + 1, k * LANE : (k + 1) * LANE] = jnp.sum(
                        value[r * HP : (r + 1) * HP, :]
                        * me_mask[:, k * LANE : (k + 1) * LANE],
                        axis=0,
                        keepdims=True,
                    )
            part = tiles(sm[...], 0, 4)
            frame = tiles(turn, 0, 12)
            moved = [part[k] - frame[9 + k] for k in range(3)]
            inside = lane8 < pvh
            for k in range(3):
                local = frame[k] * moved[0] + frame[3 + k] * moved[1] + frame[6 + k] * moved[2]
                if k == 0:
                    hi = part[0].astype(BF16).astype(F32)
                    other = jnp.where(lane8 < pvh + heads, hi, part[0] - hi)
                else:
                    other = part[k]
                spb[layer, n, heads + k] = jnp.where(inside, local, other).astype(BF16)
            spb[layer, n, heads + 3] = part[3].astype(BF16)
            for h in range(heads):
                spb[layer, n, h] = po[pl.ds(h, rows, stride=HP), :].astype(BF16)
            return n

        def step(t, carry):
            p_copy(layer, chunk(t)).start()
            return carry

        lax.fori_loop(0, nb - 1, step, 0)
        chunk(nb - 1)

    def combine(layer):
        slots = [(zb + d) % nb for d in range(nb)]
        with jax.named_scope("part_wait"):
            for n in slots[1:]:
                pltpu.make_async_copy(pr.at[layer, n], pr.at[layer, n], p_recv.at[layer, n]).wait()

        def piece(d, k):
            ref = spb if d == 0 else pr
            return ref[layer, slots[d], k].astype(F32)

        first = jnp.concatenate([piece(d, heads) for d in range(nb)], axis=0)
        sums = first + pltpu.roll(first, LANE - heads, 1)
        valid_all = (iota((nb * rows, LANE), 1) >= pvh) & (
            iota((nb * rows, LANE), 1) < pvh + heads
        )
        sums = jnp.where(valid_all, sums, 0.0)
        valid = (lane8 >= pvh) & (lane8 < pvh + heads)
        sums = [sums[d * rows : (d + 1) * rows, :] for d in range(nb)]
        top = functools.reduce(jnp.maximum, sums)
        shares = [jnp.where(valid, jnp.exp(value - top), 0.0) for value in sums]
        whole = jnp.where(valid, functools.reduce(jnp.add, shares), 1.0)
        shares = [value / whole for value in shares]
        wide = spread(jnp.concatenate(shares, axis=0), expm[...])
        mixed = []
        for k in range(4):
            acc = None
            for d in range(nb):
                term = wide[d * rows : (d + 1) * rows, k * LANE : (k + 1) * LANE] * piece(
                    d, heads + k
                )
                acc = term if acc is None else acc + term
            mixed.append(acc)
        pairs = []
        for h in range(heads):
            acc = None
            for d in range(nb):
                term = col(shares[d], pvh + h) * piece(d, h)
                acc = term if acc is None else acc + term
            pairs.append(acc)
        return mixed, pairs

    def gain_row(ref):
        return jnp.concatenate([ref[k : k + 1, :] for k in range(chan // LANE)], axis=1)

    def update(layer, state, fr, mixed, pairs):
        turn = [col(fr, k) for k in range(9)]
        shift = [col(fr, 9 + k) for k in range(3)]
        inside = lane8 < pvh
        norm = jnp.sqrt(
            mixed[0] * mixed[0] + mixed[1] * mixed[1] + mixed[2] * mixed[2] + 1e-08
        )
        concat = mixed + [jnp.where(inside, norm, 0.0)] + pairs
        concat = jnp.concatenate(concat, axis=1).astype(BF16)
        if layer == 0:
            for copy in wo_copies:
                copy.wait()
        state = state + dot(concat, wo[...])
        normed = layer_norm(state, gain_row(g1_ref))
        hidden = jnp.maximum(dot(normed.astype(BF16), m1[...]), 0.0).astype(BF16)
        hidden = jnp.maximum(dot(hidden, m2[...]), 0.0).astype(BF16)
        state = layer_norm(normed + dot(hidden, m3[...]), gain_row(g2_ref))
        state_bf = state.astype(BF16)
        upd = dot_nt(state_bf, fw_ref[...])
        u = [jnp.broadcast_to(upd[:, k : k + 1], (rows, LANE)) for k in range(6)]
        inverse = lax.rsqrt(1.0 + u[0] * u[0] + u[1] * u[1] + u[2] * u[2])
        vx, vy, vz = u[0] * inverse, u[1] * inverse, u[2] * inverse
        square = inverse * inverse
        matrix = [
            [
                square + vx * vx - vy * vy - vz * vz,
                2.0 * (vx * vy - inverse * vz),
                2.0 * (vx * vz + inverse * vy),
            ],
            [
                2.0 * (vx * vy + inverse * vz),
                square - vx * vx + vy * vy - vz * vz,
                2.0 * (vy * vz - inverse * vx),
            ],
            [
                2.0 * (vx * vz - inverse * vy),
                2.0 * (vy * vz + inverse * vx),
                square - vx * vx - vy * vy + vz * vz,
            ],
        ]
        entries = [
            turn[3 * a] * matrix[0][b]
            + turn[3 * a + 1] * matrix[1][b]
            + turn[3 * a + 2] * matrix[2][b]
            for a in range(3)
            for b in range(3)
        ] + [
            turn[3 * a] * u[3] + turn[3 * a + 1] * u[4] + turn[3 * a + 2] * u[5] + shift[a]
            for a in range(3)
        ]
        fr = jnp.zeros((rows, LANE), F32)
        for k in range(12):
            fr = jnp.where((lane8 % 12 == k) & (lane8 < 36), entries[k], fr)
        return state, state_bf, fr

    state = single[...].astype(F32)
    for layer in range(LAYERS):
        with jax.named_scope(f"key_wait_{layer}"):
            pltpu.make_async_copy(
                kx.at[layer, 0 : g_count - 1], kx.at[layer, 0 : g_count - 1], kx_recv.at[layer]
            ).wait()
        with jax.named_scope(f"key_{layer}"):
            key_phase(layer)
        with jax.named_scope(f"query_wait_{layer}"):
            pltpu.make_async_copy(
                qx.at[layer, 0 : nb - 1], qx.at[layer, 0 : nb - 1], qx_recv.at[layer]
            ).wait()
        with jax.named_scope(f"query_{layer}"):
            query_phase(layer)
        if layer == 0:
            with jax.named_scope(f"score_{layer}"):
                score_phase()
        with jax.named_scope(f"chunk_{layer}"):
            chunk_phase(layer)
        with jax.named_scope(f"combine_{layer}"):
            mixed, pairs = combine(layer)
        with jax.named_scope(f"update_{layer}"):
            state, state_bf, frames = update(layer, state, frames, mixed, pairs)
        if layer + 1 < LAYERS:
            with jax.named_scope(f"send_{layer}"):
                put_message(layer + 1, state_bf, frames)
                send_message(layer + 1)
    out_state[...] = state
    out_turn[...] = frames[:, 0:9]
    pick = (iota((3, LANE), 1) == iota((3, LANE), 0) + 9).astype(F32)
    out_shift[...] = lax.dot_general(
        pick, frames, (((1,), (1,)), ((), ())), precision=lax.Precision.HIGHEST,
        preferred_element_type=F32,
    )

    for layer in range(LAYERS):
        pltpu.make_async_copy(
            kx.at[layer, 0 : g_count - 1], kx.at[layer, 0 : g_count - 1], x_send.at[layer]
        ).wait()
        pltpu.make_async_copy(
            qx.at[layer, 0 : nb - 1], qx.at[layer, 0 : nb - 1], x_send.at[layer]
        ).wait()
        pltpu.make_async_copy(
            pr.at[layer, 0 : nb - 1], pr.at[layer, 0 : nb - 1], p_send.at[layer]
        ).wait()
    for offset in near:
        pltpu.make_async_copy(pair.at[0, :, 0, 0], pair.at[0, :, 0, 0], a2a_send).wait()


def on_device(
    pair_cols,
    single,
    rotation,
    translation,
    residue_mask,
    chain_index,
    query_weight,
    key_weight,
    value_weight,
    qpoint_weight,
    kpoint_weight,
    vpoint_weight,
    pair_weight,
    head_weight,
    chain_weight,
    output_weight,
    gain_first,
    mlp_first,
    mlp_second,
    mlp_third,
    gain_second,
    frame_weight,
):
    nx = lax.axis_size("row_0")
    nz = lax.axis_size("row_1")
    cores = lax.axis_size("row_2")
    nb = nz // SPAN
    rows, chan = single.shape
    heads = head_weight.shape[0]
    hd = query_weight.shape[1]
    g_count = nx * SPAN * cores
    nk = g_count * rows
    nq = nb * rows
    width = chan + LANE
    pair = pair_cols.reshape(nx, nb, SPAN, cores, rows, *pair_cols.shape[1:])
    vmem = pl.BlockSpec(memory_space=pltpu.VMEM)
    hbm = pl.BlockSpec(memory_space=pl.ANY)
    in_specs = [hbm] + [vmem] * 5 + [hbm] * 6 + [vmem] * 3 + [hbm, vmem] + [hbm] * 3 + [vmem] * 2
    scratch = [
        pltpu.VMEM((nb, rows, nk, LANE), BF16),
        pltpu.VMEM((LAYERS, g_count, rows, width), BF16),
        pltpu.VMEM((LAYERS, nb, rows, width), BF16),
        pltpu.VMEM((LAYERS, rows, width), BF16),
        pltpu.VMEM((5 * LANE, chan), BF16),
        pltpu.VMEM((5 * LANE, chan), BF16),
        pltpu.VMEM((4 * LANE, chan), BF16),
        pltpu.VMEM((chan, 5 * LANE), BF16),
        pltpu.VMEM((chan, 5 * LANE), BF16),
        pltpu.VMEM((chan, 4 * LANE), BF16),
        pltpu.VMEM(((5 + heads) * LANE, chan), BF16),
        pltpu.VMEM(mlp_first.shape, BF16),
        pltpu.VMEM(mlp_second.shape, BF16),
        pltpu.VMEM(mlp_third.shape, BF16),
        pltpu.VMEM((LANE, 12 * LANE), BF16),
        pltpu.VMEM((LANE, 4 * LANE), BF16),
        pltpu.VMEM((nq, 8 * LANE), F32),
        pltpu.VMEM((nk, 8 * LANE), BF16),
        pltpu.VMEM((nk, 4 * LANE), BF16),
        pltpu.VMEM((nk, 3 * LANE), BF16),
        pltpu.VMEM((nq * HP, nk), F32),
        pltpu.VMEM((nq * HP, nk), F32),
        pltpu.VMEM((nq, nk), F32),
        pltpu.VMEM((HP, 8 * LANE), F32),
        pltpu.VMEM((HP, 4 * LANE), F32),
        pltpu.VMEM((rows * HP, LANE), F32),
        pltpu.VMEM((rows, 4 * LANE), F32),
        pltpu.VMEM((nq, 12 * LANE), F32),
        pltpu.VMEM((LAYERS, nb, heads + 4, rows, LANE), BF16),
        pltpu.VMEM((LAYERS, nb, heads + 4, rows, LANE), BF16),
        pltpu.SemaphoreType.DMA((23,)),
        pltpu.SemaphoreType.DMA((8,)),
        pltpu.SemaphoreType.DMA((nb,)),
        pltpu.SemaphoreType.DMA,
        pltpu.SemaphoreType.DMA((LAYERS,)),
        pltpu.SemaphoreType.DMA((LAYERS,)),
        pltpu.SemaphoreType.DMA((LAYERS,)),
        pltpu.SemaphoreType.DMA((LAYERS,)),
        pltpu.SemaphoreType.DMA((LAYERS, nb)),
    ]
    state, turned, moved = pl.pallas_call(
        functools.partial(kernel, (nx, nb, cores, rows, heads)),
        name="structure_layers",
        out_shape=(
            jax.ShapeDtypeStruct((rows, chan), F32),
            jax.ShapeDtypeStruct((rows, 9), F32),
            jax.ShapeDtypeStruct((3, rows), F32),
        ),
        in_specs=in_specs,
        out_specs=(vmem, vmem, vmem),
        scratch_shapes=scratch,
        compiler_params=pltpu.CompilerParams(
            collective_id=0, has_side_effects=True, vmem_limit_bytes=62 * 1024 * 1024
        ),
    )(
        pair,
        single,
        jnp.transpose(rotation),
        translation,
        residue_mask.reshape(-1, LANE),
        chain_index.reshape(-1, LANE),
        jnp.transpose(query_weight),
        jnp.transpose(key_weight),
        jnp.transpose(value_weight),
        jnp.transpose(qpoint_weight),
        jnp.transpose(kpoint_weight),
        jnp.transpose(vpoint_weight),
        pair_weight,
        head_weight.reshape(1, -1),
        chain_weight.reshape(1, -1),
        output_weight,
        gain_first.reshape(-1, LANE),
        mlp_first,
        mlp_second,
        mlp_third,
        gain_second.reshape(-1, LANE),
        jnp.transpose(frame_weight),
    )
    return state, jnp.transpose(turned), moved


def solution(mesh):
    finer = Mesh(
        mesh.devices.reshape(mesh.shape["groups"], 4, 16, 2), ("groups", "row_0", "row_1", "row_2")
    )
    in_specs = (
        P(None, GROUPS_ROW, None),
        P(GROUPS_ROW, None),
        P(None, GROUPS_ROW),
        P(None, GROUPS_ROW),
        P("groups"),
        P("groups"),
    ) + (P(),) * 16
    out_specs = (P(GROUPS_ROW, None), P(None, GROUPS_ROW), P(None, GROUPS_ROW))
    return jax.shard_map(
        on_device, mesh=finer, in_specs=in_specs, out_specs=out_specs, check_vma=False
    )
```

```python
import functools

import jax
import jax.numpy as jnp
from jax import lax
from jax.experimental import pallas as pl
from jax.experimental.pallas import tpu as pltpu
from jax.sharding import Mesh
from jax.sharding import PartitionSpec as P

LAYERS = 2
SPAN = 2
GROUPS_ROW = ("groups", "row_0", "row_1", "row_2")
LOGIT_WEIGHT = (1.0 / 3.0) ** 0.5
F32 = jnp.float32
BF16 = jnp.bfloat16
LANE = 128
HP = 16


def iota(shape, dim):
    return lax.broadcasted_iota(jnp.int32, shape, dim)


def dot(a, b):
    return jnp.dot(a, b, preferred_element_type=F32)


def dot_nt(a, b):
    return lax.dot_general(a, b, (((1,), (1,)), ((), ())), preferred_element_type=F32)


def split2(x):
    hi = x.astype(BF16)
    return hi, (x - hi.astype(F32)).astype(BF16)


def split3(x):
    hi = x.astype(BF16)
    rest = x - hi.astype(F32)
    mid = rest.astype(BF16)
    return hi, mid, (rest - mid.astype(F32)).astype(BF16)


def spread(x, table):
    hi, mid, lo = split3(x)
    return dot(hi, table) + dot(mid, table) + dot(lo, table)


def col(tile, lane):
    return jnp.broadcast_to(tile[:, lane : lane + 1], tile.shape)


def layer_norm(values, gain_vector):
    centered = values - jnp.mean(values, axis=-1, keepdims=True)
    variance = jnp.mean(centered * centered, axis=-1, keepdims=True)
    return centered * lax.rsqrt(variance + 1e-05) * gain_vector


def kernel(
    sizes,
    pair,
    single_hbm,
    rotation_hbm,
    translation_hbm,
    mask_hbm,
    chain_hbm,
    wq_hbm,
    wk_hbm,
    wv_hbm,
    wqp_hbm,
    wkp_hbm,
    wvp_hbm,
    pw_hbm,
    hw_hbm,
    cw_hbm,
    wo_hbm,
    g1_hbm,
    m1_hbm,
    m2_hbm,
    m3_hbm,
    g2_hbm,
    fw_hbm,
    out_state,
    out_turn,
    out_shift,
    single,
    rotation,
    translation,
    mask,
    chain,
    pw_ref,
    hw_ref,
    cw_ref,
    g1_ref,
    g2_ref,
    fw_ref,
    tile,
    kx,
    qx,
    xs,
    wqt,
    wkt,
    wvt,
    wq,
    wk,
    wv,
    wo,
    m1,
    m2,
    m3,
    dec,
    expm,
    qf,
    kf,
    vh,
    vl,
    scores,
    bias,
    same,
    mh,
    me_mask,
    po,
    sm,
    fq,
    spb,
    pr,
    state_buf,
    turn_buf,
    shift_buf,
    last_sem,
    small_sem,
    w_sem,
    wo_sem,
    a2a_recv,
    a2a_send,
    x_send,
    kx_recv,
    qx_recv,
    p_send,
    p_recv,
):
    nx, nb, cores, rows, heads = sizes
    g_count = nx * SPAN * cores
    nk = g_count * rows
    nq = nb * rows
    chan = single.shape[1]
    pq3 = wqp_hbm.shape[0]
    pqh = pq3 // 3
    pq = pqh // heads
    pv3 = wvp_hbm.shape[0]
    pvh = pv3 // 3
    pv = pvh // heads
    hd = wq_hbm.shape[0]
    dh = hd // heads
    vtail = LANE - pvh
    x = lax.axis_index("row_0")
    z = lax.axis_index("row_1")
    c = lax.axis_index("row_2")
    nz = nb * SPAN
    zb = z // SPAN
    zp = z % SPAN

    def partner(core):
        return (z + 1 - 2 * ((z + core) % SPAN) + nz) % nz

    def place(core):
        return (x * SPAN + (z + core) % SPAN) * cores + c

    me = place(c)
    near = []
    for dx in (2, 1, 3, 0) if nx == 4 else range(nx):
        for dz in range(SPAN):
            for dc in range(cores):
                if dx or dz or dc:
                    near.append((dx, dz, dc))

    def near_id(offset):
        dx, dz, dc = offset
        core = (c + dc) % cores
        return (x + dx) % nx, partner(core) if dz else z, core

    def source_id(offset):
        dx, dz, dc = offset
        return (x + dx) % nx, partner(c) if dz else z, (c + dc) % cores

    def dev(px, pz, pc):
        return {"row_0": px, "row_1": pz, "row_2": pc}

    def far_dev(block):
        return dev(x, block * SPAN + zp, c)

    def far_step(t):
        half = (t + 1) // 2
        sign = 1 - 2 * (t % 2)
        return (zb + nb // 2 + sign * half + nb) % nb

    barrier = pltpu.get_barrier_semaphore()
    for t in range(nb - 1):
        pl.semaphore_signal(
            barrier, inc=1, device_id=far_dev(far_step(t)), device_id_type=pl.DeviceIdType.MESH
        )
    for offset in near:
        pl.semaphore_signal(
            barrier,
            inc=1,
            device_id=dev(*source_id(offset)),
            device_id_type=pl.DeviceIdType.MESH,
        )
    small = [
        (single_hbm, single),
        (rotation_hbm, rotation),
        (translation_hbm, translation),
        (mask_hbm, mask),
        (chain_hbm, chain),
        (pw_hbm, pw_ref),
        (hw_hbm, hw_ref),
        (cw_hbm, cw_ref),
        (g1_hbm, g1_ref),
        (g2_hbm, g2_ref),
        (fw_hbm, fw_ref),
    ]
    small_copies = [
        pltpu.make_async_copy(src, dst, small_sem.at[k]) for k, (src, dst) in enumerate(small)
    ]
    for copy in small_copies:
        copy.start()

    across = [offset for offset in near if offset[1]]
    within = [offset for offset in near if not offset[1]]

    def exchange(t, offsets):
        n = far_step(t)
        for offset in offsets:
            px, pz, pc = near_id(offset)
            pltpu.make_async_remote_copy(
                src_ref=pair.at[px, n, pz % SPAN, pc],
                dst_ref=tile.at[n, :, pl.ds(place(pc) * rows, rows), :],
                send_sem=a2a_send,
                recv_sem=a2a_recv.at[n],
                device_id=dev(px, pz, pc),
                device_id_type=pl.DeviceIdType.MESH,
            ).start()

    def exchange_across(t, carry):
        exchange(t, across)
        return carry

    def exchange_within(t, carry):
        n = far_step(t)
        exchange(t, within)
        pltpu.make_async_copy(
            pair.at[x, n, zp, c], tile.at[n, :, pl.ds(me * rows, rows), :], a2a_recv.at[n]
        ).start()
        return carry

    first = min(2, nb)

    with jax.named_scope("barrier"):
        pl.semaphore_wait(barrier, len(near) + nb - 1)
    exchange_across(0, 0)
    exchange_within(0, 0)

    lane8 = iota((rows, LANE), 1)
    for copy in small_copies[:3]:
        copy.wait()
    take_r = (
        (iota((9, LANE), 1) % 12 == iota((9, LANE), 0)) & (iota((9, LANE), 1) < 36)
    ).astype(F32)
    take_t = (
        (iota((3, LANE), 1) % 12 == iota((3, LANE), 0) + 9) & (iota((3, LANE), 1) < 36)
    ).astype(F32)
    contract0 = (((0,), (0,)), ((), ()))
    frames = jnp.dot(
        rotation[...], take_r, precision=lax.Precision.HIGHEST, preferred_element_type=F32
    ) + lax.dot_general(
        translation[...], take_t, contract0, precision=lax.Precision.HIGHEST,
        preferred_element_type=F32,
    )

    def frame_columns(fr):
        hi = fr.astype(BF16).astype(F32)
        mid = (fr - hi).astype(BF16).astype(F32)
        lo = fr - hi - mid
        return jnp.where(lane8 < 12, hi, jnp.where(lane8 < 24, mid, lo)).astype(BF16)

    def put_message(layer, state_bf, fr):
        tail = frame_columns(fr)
        for ref in (xs.at[layer], kx.at[layer, me], qx.at[layer, zb]):
            ref[:, 0:chan] = state_bf
            ref[:, chan : chan + LANE] = tail

    def x_near(layer, offset):
        target = near_id(offset)
        return pltpu.make_async_remote_copy(
            src_ref=xs.at[layer],
            dst_ref=kx.at[layer, place(target[2])],
            send_sem=x_send.at[layer],
            recv_sem=kx_recv.at[layer],
            device_id=dev(*target),
            device_id_type=pl.DeviceIdType.MESH,
        )

    def far_copy(layer, block):
        return pltpu.make_async_remote_copy(
            src_ref=xs.at[layer],
            dst_ref=qx.at[layer, zb],
            send_sem=x_send.at[layer],
            recv_sem=qx_recv.at[layer],
            device_id=far_dev(block),
            device_id_type=pl.DeviceIdType.MESH,
        )

    def send_message(layer):
        for t in range(nb - 1):
            far_copy(layer, far_step(t)).start()
        for offset in near:
            x_near(layer, offset).start()

    put_message(0, single[...], frames)
    send_message(0)
    with jax.named_scope("exchange"):
        for t in range(1, first):
            exchange_across(t, 0)
            exchange_within(t, 0)
        lax.fori_loop(first, nb, exchange_across, 0)
        lax.fori_loop(first, nb, exchange_within, 0)
    moves = [(wq_hbm, 0, wqt, 0, hd), (wk_hbm, 0, wkt, 0, hd)]
    for src, dst in ((wqp_hbm, wqt), (wkp_hbm, wkt)):
        for k in range(3):
            for copy_index in range(2):
                moves.append((src, k * pqh, dst, (2 + k) * LANE + copy_index * pqh, pqh))
    for k in range(3):
        moves.append((wvp_hbm, k * pvh, wvt, k * LANE, pvh))
    moves += [
        (wv_hbm, 0, wvt, LANE + pvh, vtail),
        (wv_hbm, vtail, wvt, 2 * LANE + pvh, vtail),
        (wv_hbm, 2 * vtail, wvt, 3 * LANE, hd - 2 * vtail),
        (m1_hbm, 0, m1, 0, chan),
        (m2_hbm, 0, m2, 0, chan),
        (m3_hbm, 0, m3, 0, chan),
    ]
    for ref in (wqt, wkt):
        ref[hd : 2 * LANE, :] = jnp.zeros((2 * LANE - hd, chan), BF16)
        for k in range(3):
            ref[(2 + k) * LANE + 2 * pqh : (3 + k) * LANE, :] = jnp.zeros(
                (LANE - 2 * pqh, chan), BF16
            )
    wvt[pvh:LANE, :] = jnp.zeros((vtail, chan), BF16)
    raw_copies = [
        pltpu.make_async_copy(
            src.at[pl.ds(start, count)], dst.at[pl.ds(into, count)], w_sem.at[k]
        )
        for k, (src, start, dst, into, count) in enumerate(moves)
    ]
    for copy in raw_copies:
        copy.start()
    base_pt = hd
    base_norm = hd + pv3
    base_pair = base_norm + pvh
    wo_moves = [
        (base_pt, 0, pvh),
        (base_pt + pvh, LANE, pvh),
        (0, LANE + pvh, vtail),
        (base_pt + 2 * pvh, 2 * LANE, pvh),
        (vtail, 2 * LANE + pvh, vtail),
        (2 * vtail, 3 * LANE, hd - 2 * vtail),
        (base_norm, 4 * LANE, pvh),
        (base_pair, 5 * LANE, heads * LANE),
    ]
    wo[pvh:LANE, :] = jnp.zeros((vtail, chan), BF16)
    wo[4 * LANE + pvh : 5 * LANE, :] = jnp.zeros((vtail, chan), BF16)
    wo_copies = [
        pltpu.make_async_copy(
            wo_hbm.at[pl.ds(src, count)], wo.at[pl.ds(dst, count)], wo_sem.at[k]
        )
        for k, (src, dst, count) in enumerate(wo_moves)
    ]
    for copy in wo_copies:
        copy.start()


    for copy in small_copies[3:]:
        copy.wait()
    lane_row = iota((1, LANE), 1)

    def as_col(row):
        wide = jnp.broadcast_to(row, (HP, heads))
        pick = iota((HP, heads), 0) == iota((HP, heads), 1)
        return jnp.sum(jnp.where(pick, wide, 0.0), axis=1, keepdims=True)

    hw = hw_ref[...]
    soft = jnp.maximum(hw, 0.0) + jnp.log(1.0 + jnp.exp(-jnp.abs(hw)))
    w_col = as_col(soft * (2.0 / (9.0 * pq)) ** 0.5)
    cw_col = as_col(cw_ref[...])

    head_of = iota((HP, LANE), 0)
    lane_hp = iota((HP, LANE), 1)
    q_tail = hd - LANE
    qq0 = q_tail
    kk0 = q_tail + 2 * heads
    kk1 = kk0 + 3 * heads
    point_mask = ((lane_hp % pqh) // pq == head_of) & (lane_hp < 2 * pqh)
    tail_mask = ((lane_hp < q_tail) & ((lane_hp + LANE) // dh == head_of)) | (
        (lane_hp >= q_tail) & ((lane_hp - q_tail) % heads == head_of) & (lane_hp < kk1)
    )
    mh[:, 0:LANE] = (lane_hp // dh == head_of).astype(F32)
    mh[:, LANE : 2 * LANE] = tail_mask.astype(F32)
    for k in range(6):
        mh[:, (2 + k) * LANE : (3 + k) * LANE] = point_mask.astype(F32)
    v_mask = (lane_hp // pv == head_of) & (lane_hp < pvh)
    o_masks = [
        ((lane_hp - pvh) % heads == head_of) & (lane_hp < pvh + 2 * heads),
        ((lane_hp - pvh) // dh == head_of),
        ((lane_hp - pvh + vtail) // dh == head_of),
    ]
    for k in range(3):
        me_mask[:, k * LANE : (k + 1) * LANE] = (
            v_mask | ((lane_hp >= pvh) & o_masks[k])
        ).astype(F32)
    me_mask[:, 3 * LANE : 4 * LANE] = ((lane_hp + 2 * vtail) // dh == head_of).astype(F32)
    big_row = iota((LANE, 4 * LANE), 0) - pvh
    big_col = iota((LANE, 4 * LANE), 1)
    big_lane = big_col % LANE
    big_tile = big_col // LANE
    o_col = jnp.where(
        big_tile == 3, big_lane + 2 * vtail, big_lane - pvh + (big_tile - 1) * vtail
    )
    is_point = (big_tile < 3) & (big_lane < pvh)
    big_head = jnp.where(is_point, big_lane // pv, o_col // dh)
    has_head = is_point | (big_tile > 0)
    expm[...] = (
        (big_head == big_row) & has_head & (big_row >= 0) & (big_row < heads)
    ).astype(BF16)
    w_lane = jnp.sum(jnp.where(point_mask, w_col, 0.0), axis=0, keepdims=True)
    half_lane = -0.5 * jnp.sum(
        jnp.where((lane_hp - q_tail) % heads == head_of, w_col, 0.0), axis=0, keepdims=True
    )
    dec_row = iota((LANE, LANE), 0)
    for k in range(12):
        dec[:, k * LANE : (k + 1) * LANE] = ((dec_row % 12 == k) & (dec_row < 36)).astype(BF16)
    sel = (
        (iota((LANE, LANE), 0) < pqh)
        & (iota((LANE, LANE), 1) >= q_tail)
        & (iota((LANE, LANE), 1) < kk1)
        & ((iota((LANE, LANE), 1) - q_tail) % heads == iota((LANE, LANE), 0) // pq)
    ).astype(BF16)

    chain_v = chain[...]
    mask_v = mask[...]

    def total(values):
        return jnp.sum(
            jnp.sum(values.astype(F32), axis=1, keepdims=True), axis=0, keepdims=True
        )

    plane_rows = cores * rows
    block_rows = SPAN * plane_rows
    key_local = iota((1, nk), 1)
    key_plane = (z - (z + c) % SPAN + (key_local // plane_rows) % SPAN + nz) % nz
    key_index = (
        ((key_local // block_rows) * nz + key_plane) * plane_rows + key_local % plane_rows
    ).astype(F32)
    q_local = iota((nq, 1), 0)
    q_index = (
        x * (nb * block_rows)
        + (q_local // rows) * block_rows
        + (zp * cores + c) * rows
        + q_local % rows
    ).astype(F32)
    key_chain = jnp.zeros((1, nk), F32)
    q_chain = jnp.zeros((nq, 1), F32)
    for k in range(1, 4):
        edge = total(chain_v < k)
        key_chain = key_chain + (key_index >= edge).astype(F32)
        q_chain = q_chain + (q_index >= edge).astype(F32)
    same[...] = (q_chain == key_chain).astype(F32)
    pad_row = ((key_index < total(mask_v)).astype(F32) - 1.0) * 100000.0

    for copy in raw_copies:
        copy.wait()
    wq[...] = jnp.transpose(wqt[...])
    wk[...] = jnp.transpose(wkt[...])
    wv[...] = jnp.transpose(wvt[...])

    pw16 = jnp.concatenate([pw_ref[...].astype(F32), jnp.zeros((HP - heads, LANE), F32)], axis=0)
    pw16 = pw16.astype(BF16)

    def global_points(px, py, pz, fb):
        def part(k):
            return fb[:, k * LANE : (k + 1) * LANE]

        return [
            part(3 * k) * px + part(3 * k + 1) * py + part(3 * k + 2) * pz + part(9 + k)
            for k in range(3)
        ]

    def tiles(values, start, count):
        return [values[:, (start + k) * LANE : (start + k + 1) * LANE] for k in range(count)]

    def key_phase(layer):
        message = kx[layer].reshape(nk, chan + LANE)
        fb = dot(message[:, chan:], dec[...])
        body = message[:, :chan]
        projected = dot(body, wk[...])
        lane = iota((nk, LANE), 1)
        g = global_points(*tiles(projected, 2, 3), fb)
        square = g[0] * g[0] + g[1] * g[1] + g[2] * g[2]
        kk = spread(square, sel) * half_lane
        hi = kk.astype(BF16).astype(F32)
        mid = (kk - hi).astype(BF16).astype(F32)
        lo = kk - hi - mid
        kk = jnp.where(lane < kk0 + heads, hi, jnp.where(lane < kk0 + 2 * heads, mid, lo))
        kk = jnp.where(lane < kk1, kk, 0.0)
        tail = jnp.where(
            lane < q_tail, projected[:, LANE : 2 * LANE], jnp.where(lane < kk0, 1.0, kk)
        )
        kf[:, 0:LANE] = projected[:, 0:LANE].astype(BF16)
        kf[:, LANE : 2 * LANE] = tail.astype(BF16)
        for k in range(3):
            hi = g[k].astype(BF16).astype(F32)
            pts = jnp.where(lane < pqh, hi, jnp.where(lane < 2 * pqh, g[k] - hi, 0.0)).astype(BF16)
            kf[:, (2 + k) * LANE : (3 + k) * LANE] = pts
            kf[:, (5 + k) * LANE : (6 + k) * LANE] = pts
        values = dot(body, wv[...])
        parts = tiles(values, 0, 4)
        g = global_points(parts[0], parts[1], parts[2], fb)
        for k in range(3):
            whole = jnp.where(lane < pvh, g[k], parts[k])
            hi = whole.astype(BF16)
            vh[:, k * LANE : (k + 1) * LANE] = hi
            vl[:, k * LANE : (k + 1) * LANE] = jnp.where(
                lane < pvh, whole - hi.astype(F32), 0.0
            ).astype(BF16)
        vh[:, 3 * LANE : 4 * LANE] = parts[3].astype(BF16)

    def query_phase(layer):
        scale = dh ** -0.5
        message = qx[layer].reshape(nq, chan + LANE)
        fb = dot(message[:, chan:], dec[...])
        fq[...] = fb
        projected = dot(message[:, :chan], wq[...])
        lane = iota((nq, LANE), 1)
        g = global_points(*tiles(projected, 2, 3), fb)
        square = g[0] * g[0] + g[1] * g[1] + g[2] * g[2]
        qq = spread(square, sel) * half_lane
        hi = qq.astype(BF16).astype(F32)
        qq = jnp.where(lane < qq0 + heads, hi, qq - hi)
        tail = jnp.where(
            lane < q_tail,
            projected[:, LANE : 2 * LANE] * scale,
            jnp.where(lane < kk0, qq, jnp.where(lane < kk1, 1.0, 0.0)),
        )
        qf[:, 0:LANE] = projected[:, 0:LANE].astype(BF16).astype(F32) * scale
        qf[:, LANE : 2 * LANE] = tail.astype(BF16).astype(F32)
        for k in range(3):
            scaled = g[k] * w_lane
            hi = scaled.astype(BF16).astype(F32)
            qf[:, (2 + k) * LANE : (3 + k) * LANE] = hi
            qf[:, (5 + k) * LANE : (6 + k) * LANE] = jnp.where(lane < pqh, scaled - hi, 0.0)

    def score_chunk(n):
        parts = []
        for r in range(rows):
            row = qf[pl.ds(n * rows + r, 1), :]
            parts.append((jnp.broadcast_to(row, (HP, 8 * LANE)) * mh[...]).astype(BF16))
        s = dot_nt(jnp.concatenate(parts, axis=0), kf[...]) * LOGIT_WEIGHT
        extra = []
        for r in range(rows):
            match = jnp.broadcast_to(same[pl.ds(n * rows + r, 1), :], (HP, nk))
            extra.append(match * cw_col + pad_row)
        return s + jnp.concatenate(extra, axis=0)

    def chunk_rows(n):
        return pl.ds(pl.multiple_of(n * rows * HP, rows * HP), rows * HP)

    def score_phase():
        def step(n, carry):
            scores[chunk_rows(n), :] = score_chunk(n)
            return carry

        lax.fori_loop(0, nb, step, 0)

    def p_copy(layer, n):
        return pltpu.make_async_remote_copy(
            src_ref=spb.at[layer, n],
            dst_ref=pr.at[layer, zb],
            send_sem=p_send.at[layer],
            recv_sem=p_recv.at[layer, zb],
            device_id=far_dev(n),
            device_id_type=pl.DeviceIdType.MESH,
        )

    lane_all = iota((rows * HP, LANE), 1)

    def chunk_phase(layer):
        def chunk(t):
            n = far_step(t)
            if layer == 0:
                logits = scores[chunk_rows(n), :]
                with jax.named_scope("tile_wait"):
                    pltpu.make_async_copy(tile.at[n], tile.at[n], a2a_recv.at[n]).wait()
                pair_rows = [tile[n, r] for r in range(rows)]
                own = jnp.concatenate([dot_nt(pw16, v) for v in pair_rows], axis=0) * LOGIT_WEIGHT
                logits = logits + own
            else:
                pair_rows = [tile[n, r] for r in range(rows)]
                logits = score_chunk(n) + bias[chunk_rows(n), :]
            top = jnp.max(logits, axis=1, keepdims=True)
            p = jnp.exp(logits - top)
            count = jnp.sum(p, axis=1, keepdims=True)
            p = p.astype(BF16)
            inverse = 1.0 / count
            log_sum = top + jnp.log(count)
            mixed = jnp.concatenate(
                [dot(p[r * HP : (r + 1) * HP, :], pair_rows[r]) for r in range(rows)], axis=0
            )
            main = dot(p, vh[...])
            rest = dot(p, vl[...])
            turn = fq[pl.ds(n * rows, rows), :]
            po[...] = mixed * inverse
            if layer == 0:
                bias[chunk_rows(n), :] = own
            for k in range(4):
                value = main[:, k * LANE : (k + 1) * LANE]
                if k < 3:
                    value = value + rest[:, k * LANE : (k + 1) * LANE]
                value = value * inverse
                if k == 0:
                    value = jnp.where(lane_all < pvh, value, log_sum)
                for r in range(rows):
                    sm[r : r + 1, k * LANE : (k + 1) * LANE] = jnp.sum(
                        value[r * HP : (r + 1) * HP, :]
                        * me_mask[:, k * LANE : (k + 1) * LANE],
                        axis=0,
                        keepdims=True,
                    )
            part = tiles(sm[...], 0, 4)
            frame = tiles(turn, 0, 12)
            moved = [part[k] - frame[9 + k] for k in range(3)]
            inside = lane8 < pvh
            for k in range(3):
                local = frame[k] * moved[0] + frame[3 + k] * moved[1] + frame[6 + k] * moved[2]
                if k == 0:
                    hi = part[0].astype(BF16).astype(F32)
                    other = jnp.where(lane8 < pvh + heads, hi, part[0] - hi)
                else:
                    other = part[k]
                spb[layer, n, heads + k] = jnp.where(inside, local, other).astype(BF16)
            spb[layer, n, heads + 3] = part[3].astype(BF16)
            for h in range(heads):
                spb[layer, n, h] = po[pl.ds(h, rows, stride=HP), :].astype(BF16)
            return n

        def step(t, carry):
            p_copy(layer, chunk(t)).start()
            return carry

        lax.fori_loop(0, nb - 1, step, 0)
        chunk(nb - 1)

    def combine(layer):
        slots = [(zb + d) % nb for d in range(nb)]
        with jax.named_scope("part_wait"):
            for n in slots[1:]:
                pltpu.make_async_copy(pr.at[layer, n], pr.at[layer, n], p_recv.at[layer, n]).wait()

        def piece(d, k):
            ref = spb if d == 0 else pr
            return ref[layer, slots[d], k].astype(F32)

        first = jnp.concatenate([piece(d, heads) for d in range(nb)], axis=0)
        sums = first + pltpu.roll(first, LANE - heads, 1)
        valid_all = (iota((nb * rows, LANE), 1) >= pvh) & (
            iota((nb * rows, LANE), 1) < pvh + heads
        )
        sums = jnp.where(valid_all, sums, 0.0)
        valid = (lane8 >= pvh) & (lane8 < pvh + heads)
        sums = [sums[d * rows : (d + 1) * rows, :] for d in range(nb)]
        top = functools.reduce(jnp.maximum, sums)
        shares = [jnp.where(valid, jnp.exp(value - top), 0.0) for value in sums]
        whole = jnp.where(valid, functools.reduce(jnp.add, shares), 1.0)
        shares = [value / whole for value in shares]
        wide = spread(jnp.concatenate(shares, axis=0), expm[...])
        mixed = []
        for k in range(4):
            acc = None
            for d in range(nb):
                term = wide[d * rows : (d + 1) * rows, k * LANE : (k + 1) * LANE] * piece(
                    d, heads + k
                )
                acc = term if acc is None else acc + term
            mixed.append(acc)
        pairs = []
        for h in range(heads):
            acc = None
            for d in range(nb):
                term = col(shares[d], pvh + h) * piece(d, h)
                acc = term if acc is None else acc + term
            pairs.append(acc)
        return mixed, pairs

    def gain_row(ref):
        return jnp.concatenate([ref[k : k + 1, :] for k in range(chan // LANE)], axis=1)

    def update(layer, state, fr, mixed, pairs):
        turn = [col(fr, k) for k in range(9)]
        shift = [col(fr, 9 + k) for k in range(3)]
        inside = lane8 < pvh
        norm = jnp.sqrt(
            mixed[0] * mixed[0] + mixed[1] * mixed[1] + mixed[2] * mixed[2] + 1e-08
        )
        concat = mixed + [jnp.where(inside, norm, 0.0)] + pairs
        concat = jnp.concatenate(concat, axis=1).astype(BF16)
        if layer == 0:
            for copy in wo_copies:
                copy.wait()
        state = state + dot(concat, wo[...])
        normed = layer_norm(state, gain_row(g1_ref))
        hidden = jnp.maximum(dot(normed.astype(BF16), m1[...]), 0.0).astype(BF16)
        hidden = jnp.maximum(dot(hidden, m2[...]), 0.0).astype(BF16)
        state = layer_norm(normed + dot(hidden, m3[...]), gain_row(g2_ref))
        if layer == LAYERS - 1:
            state_buf[...] = state
            last_copies[0].start()
        state_bf = state.astype(BF16)
        upd = dot_nt(state_bf, fw_ref[...])
        u = [jnp.broadcast_to(upd[:, k : k + 1], (rows, LANE)) for k in range(6)]
        inverse = lax.rsqrt(1.0 + u[0] * u[0] + u[1] * u[1] + u[2] * u[2])
        vx, vy, vz = u[0] * inverse, u[1] * inverse, u[2] * inverse
        square = inverse * inverse
        matrix = [
            [
                square + vx * vx - vy * vy - vz * vz,
                2.0 * (vx * vy - inverse * vz),
                2.0 * (vx * vz + inverse * vy),
            ],
            [
                2.0 * (vx * vy + inverse * vz),
                square - vx * vx + vy * vy - vz * vz,
                2.0 * (vy * vz - inverse * vx),
            ],
            [
                2.0 * (vx * vz - inverse * vy),
                2.0 * (vy * vz + inverse * vx),
                square - vx * vx - vy * vy + vz * vz,
            ],
        ]
        entries = [
            turn[3 * a] * matrix[0][b]
            + turn[3 * a + 1] * matrix[1][b]
            + turn[3 * a + 2] * matrix[2][b]
            for a in range(3)
            for b in range(3)
        ] + [
            turn[3 * a] * u[3] + turn[3 * a + 1] * u[4] + turn[3 * a + 2] * u[5] + shift[a]
            for a in range(3)
        ]
        fr = jnp.zeros((rows, LANE), F32)
        for k in range(12):
            fr = jnp.where((lane8 % 12 == k) & (lane8 < 36), entries[k], fr)
        return state, state_bf, fr

    last_copies = [
        pltpu.make_async_copy(src, dst, last_sem.at[k])
        for k, (src, dst) in enumerate(
            ((state_buf, out_state), (turn_buf, out_turn), (shift_buf, out_shift))
        )
    ]
    state = single[...].astype(F32)
    for layer in range(LAYERS):
        with jax.named_scope(f"key_wait_{layer}"):
            pltpu.make_async_copy(
                kx.at[layer, 0 : g_count - 1], kx.at[layer, 0 : g_count - 1], kx_recv.at[layer]
            ).wait()
        with jax.named_scope(f"key_{layer}"):
            key_phase(layer)
        with jax.named_scope(f"query_wait_{layer}"):
            pltpu.make_async_copy(
                qx.at[layer, 0 : nb - 1], qx.at[layer, 0 : nb - 1], qx_recv.at[layer]
            ).wait()
        with jax.named_scope(f"query_{layer}"):
            query_phase(layer)
        if layer == 0:
            with jax.named_scope(f"score_{layer}"):
                score_phase()
        with jax.named_scope(f"chunk_{layer}"):
            chunk_phase(layer)
        with jax.named_scope(f"combine_{layer}"):
            mixed, pairs = combine(layer)
        with jax.named_scope(f"update_{layer}"):
            state, state_bf, frames = update(layer, state, frames, mixed, pairs)
        if layer + 1 < LAYERS:
            with jax.named_scope(f"send_{layer}"):
                put_message(layer + 1, state_bf, frames)
                send_message(layer + 1)
    turn_buf[...] = frames[:, 0:9]
    pick = (iota((3, LANE), 1) == iota((3, LANE), 0) + 9).astype(F32)
    shift_buf[...] = lax.dot_general(
        pick, frames, (((1,), (1,)), ((), ())), precision=lax.Precision.HIGHEST,
        preferred_element_type=F32,
    )
    last_copies[1].start()
    last_copies[2].start()
    for layer in range(LAYERS):
        pltpu.make_async_copy(
            kx.at[layer, 0 : g_count - 1], kx.at[layer, 0 : g_count - 1], x_send.at[layer]
        ).wait()
        pltpu.make_async_copy(
            qx.at[layer, 0 : nb - 1], qx.at[layer, 0 : nb - 1], x_send.at[layer]
        ).wait()
        pltpu.make_async_copy(
            pr.at[layer, 0 : nb - 1], pr.at[layer, 0 : nb - 1], p_send.at[layer]
        ).wait()
    for offset in near:
        pltpu.make_async_copy(pair.at[0, :, 0, 0], pair.at[0, :, 0, 0], a2a_send).wait()
    for copy in last_copies:
        copy.wait()


def hand_over(a, b, c, a_out, b_out, c_out, sem):
    copies = [
        pltpu.make_async_copy(src, dst, sem.at[k])
        for k, (src, dst) in enumerate(((a, a_out), (b, b_out), (c, c_out)))
    ]
    for copy in copies:
        copy.start()
    for copy in copies:
        copy.wait()


def on_device(
    pair_cols,
    single,
    rotation,
    translation,
    residue_mask,
    chain_index,
    query_weight,
    key_weight,
    value_weight,
    qpoint_weight,
    kpoint_weight,
    vpoint_weight,
    pair_weight,
    head_weight,
    chain_weight,
    output_weight,
    gain_first,
    mlp_first,
    mlp_second,
    mlp_third,
    gain_second,
    frame_weight,
):
    nx = lax.axis_size("row_0")
    nz = lax.axis_size("row_1")
    cores = lax.axis_size("row_2")
    nb = nz // SPAN
    rows, chan = single.shape
    heads = head_weight.shape[0]
    hd = query_weight.shape[1]
    g_count = nx * SPAN * cores
    nk = g_count * rows
    nq = nb * rows
    width = chan + LANE
    pair = pair_cols.reshape(nx, nb, SPAN, cores, rows, *pair_cols.shape[1:])
    hbm = pl.BlockSpec(memory_space=pl.ANY)
    small = [
        single,
        jnp.transpose(rotation),
        translation,
        residue_mask.reshape(-1, LANE),
        chain_index.reshape(-1, LANE),
        pair_weight,
        head_weight.reshape(1, -1),
        chain_weight.reshape(1, -1),
        gain_first.reshape(-1, LANE),
        gain_second.reshape(-1, LANE),
        jnp.transpose(frame_weight),
    ]
    scratch = [pltpu.VMEM(v.shape, v.dtype) for v in small] + [
        pltpu.VMEM((nb, rows, nk, LANE), BF16),
        pltpu.VMEM((LAYERS, g_count, rows, width), BF16),
        pltpu.VMEM((LAYERS, nb, rows, width), BF16),
        pltpu.VMEM((LAYERS, rows, width), BF16),
        pltpu.VMEM((5 * LANE, chan), BF16),
        pltpu.VMEM((5 * LANE, chan), BF16),
        pltpu.VMEM((4 * LANE, chan), BF16),
        pltpu.VMEM((chan, 5 * LANE), BF16),
        pltpu.VMEM((chan, 5 * LANE), BF16),
        pltpu.VMEM((chan, 4 * LANE), BF16),
        pltpu.VMEM(((5 + heads) * LANE, chan), BF16),
        pltpu.VMEM(mlp_first.shape, BF16),
        pltpu.VMEM(mlp_second.shape, BF16),
        pltpu.VMEM(mlp_third.shape, BF16),
        pltpu.VMEM((LANE, 12 * LANE), BF16),
        pltpu.VMEM((LANE, 4 * LANE), BF16),
        pltpu.VMEM((nq, 8 * LANE), F32),
        pltpu.VMEM((nk, 8 * LANE), BF16),
        pltpu.VMEM((nk, 4 * LANE), BF16),
        pltpu.VMEM((nk, 3 * LANE), BF16),
        pltpu.VMEM((nq * HP, nk), F32),
        pltpu.VMEM((nq * HP, nk), F32),
        pltpu.VMEM((nq, nk), F32),
        pltpu.VMEM((HP, 8 * LANE), F32),
        pltpu.VMEM((HP, 4 * LANE), F32),
        pltpu.VMEM((rows * HP, LANE), F32),
        pltpu.VMEM((rows, 4 * LANE), F32),
        pltpu.VMEM((nq, 12 * LANE), F32),
        pltpu.VMEM((LAYERS, nb, heads + 4, rows, LANE), BF16),
        pltpu.VMEM((LAYERS, nb, heads + 4, rows, LANE), BF16),
        pltpu.VMEM((rows, chan), F32),
        pltpu.VMEM((rows, 9), F32),
        pltpu.VMEM((3, rows), F32),
        pltpu.SemaphoreType.DMA((3,)),
        pltpu.SemaphoreType.DMA((11,)),
        pltpu.SemaphoreType.DMA((23,)),
        pltpu.SemaphoreType.DMA((8,)),
        pltpu.SemaphoreType.DMA((nb,)),
        pltpu.SemaphoreType.DMA,
        pltpu.SemaphoreType.DMA((LAYERS,)),
        pltpu.SemaphoreType.DMA((LAYERS,)),
        pltpu.SemaphoreType.DMA((LAYERS,)),
        pltpu.SemaphoreType.DMA((LAYERS,)),
        pltpu.SemaphoreType.DMA((LAYERS, nb)),
    ]
    state, turned, moved = pl.pallas_call(
        functools.partial(kernel, (nx, nb, cores, rows, heads)),
        name="structure_layers",
        out_shape=(
            jax.ShapeDtypeStruct((rows, chan), F32),
            jax.ShapeDtypeStruct((rows, 9), F32),
            jax.ShapeDtypeStruct((3, rows), F32),
        ),
        in_specs=[hbm] * 22,
        out_specs=(hbm, hbm, hbm),
        scratch_shapes=scratch,
        compiler_params=pltpu.CompilerParams(
            collective_id=0, has_side_effects=True, vmem_limit_bytes=62 * 1024 * 1024
        ),
    )(
        pair,
        *small[:5],
        jnp.transpose(query_weight),
        jnp.transpose(key_weight),
        jnp.transpose(value_weight),
        jnp.transpose(qpoint_weight),
        jnp.transpose(kpoint_weight),
        jnp.transpose(vpoint_weight),
        *small[5:8],
        output_weight,
        small[8],
        mlp_first,
        mlp_second,
        mlp_third,
        small[9],
        small[10],
    )
    state, turned, moved = pl.pallas_call(
        hand_over,
        name="hand_over",
        out_shape=tuple(jax.ShapeDtypeStruct(v.shape, v.dtype) for v in (state, turned, moved)),
        in_specs=[hbm] * 3,
        out_specs=(hbm,) * 3,
        scratch_shapes=[pltpu.SemaphoreType.DMA((3,))],
        compiler_params=pltpu.CompilerParams(vmem_limit_bytes=62 * 1024 * 1024),
    )(state, turned, moved)
    return state, jnp.transpose(turned), moved


def solution(mesh):
    finer = Mesh(
        mesh.devices.reshape(mesh.shape["groups"], 4, 16, 2), ("groups", "row_0", "row_1", "row_2")
    )
    in_specs = (
        P(None, GROUPS_ROW, None),
        P(GROUPS_ROW, None),
        P(None, GROUPS_ROW),
        P(None, GROUPS_ROW),
        P("groups"),
        P("groups"),
    ) + (P(),) * 16
    out_specs = (P(GROUPS_ROW, None), P(None, GROUPS_ROW), P(None, GROUPS_ROW))
    return jax.shard_map(
        on_device, mesh=finer, in_specs=in_specs, out_specs=out_specs, check_vma=False
    )
```

```python
import functools

import jax
import jax.numpy as jnp
from jax import lax
from jax.experimental import pallas as pl
from jax.experimental.pallas import tpu as pltpu
from jax.sharding import Mesh
from jax.sharding import PartitionSpec as P

LAYERS = 2
SPAN = 2
GROUPS_ROW = ("groups", "row_0", "row_1", "row_2")
LOGIT_WEIGHT = (1.0 / 3.0) ** 0.5
F32 = jnp.float32
BF16 = jnp.bfloat16
LANE = 128
HP = 16


def iota(shape, dim):
    return lax.broadcasted_iota(jnp.int32, shape, dim)


def dot(a, b):
    return jnp.dot(a, b, preferred_element_type=F32)


def dot_nt(a, b):
    return lax.dot_general(a, b, (((1,), (1,)), ((), ())), preferred_element_type=F32)


def split2(x):
    hi = x.astype(BF16)
    return hi, (x - hi.astype(F32)).astype(BF16)


def split3(x):
    hi = x.astype(BF16)
    rest = x - hi.astype(F32)
    mid = rest.astype(BF16)
    return hi, mid, (rest - mid.astype(F32)).astype(BF16)


def spread(x, table):
    hi, mid, lo = split3(x)
    return dot(hi, table) + dot(mid, table) + dot(lo, table)


def col(tile, lane):
    return jnp.broadcast_to(tile[:, lane : lane + 1], tile.shape)


def layer_norm(values, gain_vector):
    centered = values - jnp.mean(values, axis=-1, keepdims=True)
    variance = jnp.mean(centered * centered, axis=-1, keepdims=True)
    return centered * lax.rsqrt(variance + 1e-05) * gain_vector


def kernel(
    sizes,
    pair,
    single_hbm,
    rotation_hbm,
    translation_hbm,
    mask_hbm,
    chain_hbm,
    wq_hbm,
    wk_hbm,
    wv_hbm,
    wqp_hbm,
    wkp_hbm,
    wvp_hbm,
    pw_hbm,
    hw_hbm,
    cw_hbm,
    wo_hbm,
    g1_hbm,
    m1_hbm,
    m2_hbm,
    m3_hbm,
    g2_hbm,
    fw_hbm,
    out_state,
    out_turn,
    out_shift,
    single,
    rotation,
    translation,
    mask,
    chain,
    pw_ref,
    hw_ref,
    cw_ref,
    g1_ref,
    g2_ref,
    fw_ref,
    tile,
    kx,
    qx,
    xs,
    wqt,
    wkt,
    wvt,
    wq,
    wk,
    wv,
    wo,
    m1,
    m2,
    m3,
    dec,
    expm,
    qf,
    kf,
    vh,
    vl,
    scores,
    bias,
    same,
    mh,
    me_mask,
    po,
    sm,
    fq,
    spb,
    pr,
    state_buf,
    turn_buf,
    shift_buf,
    last_sem,
    small_sem,
    w_sem,
    wo_sem,
    a2a_recv,
    a2a_send,
    x_send,
    kx_recv,
    qx_recv,
    p_send,
    p_recv,
):
    nx, nb, cores, rows, heads = sizes
    g_count = nx * SPAN * cores
    nk = g_count * rows
    nq = nb * rows
    chan = single.shape[1]
    pq3 = wqp_hbm.shape[0]
    pqh = pq3 // 3
    pq = pqh // heads
    pv3 = wvp_hbm.shape[0]
    pvh = pv3 // 3
    pv = pvh // heads
    hd = wq_hbm.shape[0]
    dh = hd // heads
    vtail = LANE - pvh
    x = lax.axis_index("row_0")
    z = lax.axis_index("row_1")
    c = lax.axis_index("row_2")
    nz = nb * SPAN
    zb = z // SPAN
    zp = z % SPAN

    def partner(core):
        return (z + 1 - 2 * ((z + core) % SPAN) + nz) % nz

    def place(core):
        return (x * SPAN + (z + core) % SPAN) * cores + c

    me = place(c)
    near = []
    for dx in (2, 1, 3, 0) if nx == 4 else range(nx):
        for dz in range(SPAN):
            for dc in range(cores):
                if dx or dz or dc:
                    near.append((dx, dz, dc))

    def near_id(offset):
        dx, dz, dc = offset
        core = (c + dc) % cores
        return (x + dx) % nx, partner(core) if dz else z, core

    def source_id(offset):
        dx, dz, dc = offset
        return (x + dx) % nx, partner(c) if dz else z, (c + dc) % cores

    def dev(px, pz, pc):
        return {"row_0": px, "row_1": pz, "row_2": pc}

    def far_dev(block):
        return dev(x, block * SPAN + zp, c)

    def far_step(t, block=None):
        half = (t + 1) // 2
        sign = 1 - 2 * (t % 2)
        return ((zb if block is None else block) + nb // 2 + sign * half + nb) % nb

    barrier = pltpu.get_barrier_semaphore()
    for t in range(nb - 1):
        pl.semaphore_signal(
            barrier, inc=1, device_id=far_dev(far_step(t)), device_id_type=pl.DeviceIdType.MESH
        )
    for offset in near:
        pl.semaphore_signal(
            barrier,
            inc=1,
            device_id=dev(*source_id(offset)),
            device_id_type=pl.DeviceIdType.MESH,
        )
    small = [
        (single_hbm, single),
        (rotation_hbm, rotation),
        (translation_hbm, translation),
        (mask_hbm, mask),
        (chain_hbm, chain),
        (pw_hbm, pw_ref),
        (hw_hbm, hw_ref),
        (cw_hbm, cw_ref),
        (g1_hbm, g1_ref),
        (g2_hbm, g2_ref),
        (fw_hbm, fw_ref),
    ]
    small_copies = [
        pltpu.make_async_copy(src, dst, small_sem.at[k]) for k, (src, dst) in enumerate(small)
    ]
    for copy in small_copies:
        copy.start()

    across = [offset for offset in near if offset[1]]
    within = [offset for offset in near if not offset[1]]

    def exchange(t, offsets):
        for offset in offsets:
            px, pz, pc = near_id(offset)
            n = far_step(t, pz // SPAN)
            pltpu.make_async_remote_copy(
                src_ref=pair.at[px, n, pz % SPAN, pc],
                dst_ref=tile.at[n, :, pl.ds(place(pc) * rows, rows), :],
                send_sem=a2a_send,
                recv_sem=a2a_recv.at[n],
                device_id=dev(px, pz, pc),
                device_id_type=pl.DeviceIdType.MESH,
            ).start()

    def exchange_across(t):
        if t < nb:
            exchange(t, across)

    def exchange_within(t, carry):
        exchange(t, within)
        n = far_step(t)
        pltpu.make_async_copy(
            pair.at[x, n, zp, c], tile.at[n, :, pl.ds(me * rows, rows), :], a2a_recv.at[n]
        ).start()
        return carry

    with jax.named_scope("barrier"):
        pl.semaphore_wait(barrier, len(near) + nb - 1)
    exchange_within(0, 0)
    exchange_across(0)

    lane8 = iota((rows, LANE), 1)
    for copy in small_copies[:3]:
        copy.wait()
    take_r = (
        (iota((9, LANE), 1) % 12 == iota((9, LANE), 0)) & (iota((9, LANE), 1) < 36)
    ).astype(F32)
    take_t = (
        (iota((3, LANE), 1) % 12 == iota((3, LANE), 0) + 9) & (iota((3, LANE), 1) < 36)
    ).astype(F32)
    contract0 = (((0,), (0,)), ((), ()))
    frames = jnp.dot(
        rotation[...], take_r, precision=lax.Precision.HIGHEST, preferred_element_type=F32
    ) + lax.dot_general(
        translation[...], take_t, contract0, precision=lax.Precision.HIGHEST,
        preferred_element_type=F32,
    )

    def frame_columns(fr):
        hi = fr.astype(BF16).astype(F32)
        mid = (fr - hi).astype(BF16).astype(F32)
        lo = fr - hi - mid
        return jnp.where(lane8 < 12, hi, jnp.where(lane8 < 24, mid, lo)).astype(BF16)

    def put_message(layer, state_bf, fr):
        tail = frame_columns(fr)
        for ref in (xs.at[layer], kx.at[layer, me], qx.at[layer, zb]):
            ref[:, 0:chan] = state_bf
            ref[:, chan : chan + LANE] = tail

    def x_near(layer, offset):
        target = near_id(offset)
        return pltpu.make_async_remote_copy(
            src_ref=xs.at[layer],
            dst_ref=kx.at[layer, place(target[2])],
            send_sem=x_send.at[layer],
            recv_sem=kx_recv.at[layer],
            device_id=dev(*target),
            device_id_type=pl.DeviceIdType.MESH,
        )

    def far_copy(layer, block):
        return pltpu.make_async_remote_copy(
            src_ref=xs.at[layer],
            dst_ref=qx.at[layer, zb],
            send_sem=x_send.at[layer],
            recv_sem=qx_recv.at[layer],
            device_id=far_dev(block),
            device_id_type=pl.DeviceIdType.MESH,
        )

    def send_message(layer):
        for t in range(nb - 1):
            far_copy(layer, far_step(t)).start()
        for offset in near:
            x_near(layer, offset).start()

    put_message(0, single[...], frames)
    send_message(0)
    with jax.named_scope("exchange"):
        lax.fori_loop(1, nb, exchange_within, 0)
        exchange_across(1)
    moves = [(wq_hbm, 0, wqt, 0, hd), (wk_hbm, 0, wkt, 0, hd)]
    for src, dst in ((wqp_hbm, wqt), (wkp_hbm, wkt)):
        for k in range(3):
            for copy_index in range(2):
                moves.append((src, k * pqh, dst, (2 + k) * LANE + copy_index * pqh, pqh))
    for k in range(3):
        moves.append((wvp_hbm, k * pvh, wvt, k * LANE, pvh))
    moves += [
        (wv_hbm, 0, wvt, LANE + pvh, vtail),
        (wv_hbm, vtail, wvt, 2 * LANE + pvh, vtail),
        (wv_hbm, 2 * vtail, wvt, 3 * LANE, hd - 2 * vtail),
        (m1_hbm, 0, m1, 0, chan),
        (m2_hbm, 0, m2, 0, chan),
        (m3_hbm, 0, m3, 0, chan),
    ]
    for ref in (wqt, wkt):
        ref[hd : 2 * LANE, :] = jnp.zeros((2 * LANE - hd, chan), BF16)
        for k in range(3):
            ref[(2 + k) * LANE + 2 * pqh : (3 + k) * LANE, :] = jnp.zeros(
                (LANE - 2 * pqh, chan), BF16
            )
    wvt[pvh:LANE, :] = jnp.zeros((vtail, chan), BF16)
    raw_copies = [
        pltpu.make_async_copy(
            src.at[pl.ds(start, count)], dst.at[pl.ds(into, count)], w_sem.at[k]
        )
        for k, (src, start, dst, into, count) in enumerate(moves)
    ]
    for copy in raw_copies:
        copy.start()
    base_pt = hd
    base_norm = hd + pv3
    base_pair = base_norm + pvh
    wo_moves = [
        (base_pt, 0, pvh),
        (base_pt + pvh, LANE, pvh),
        (0, LANE + pvh, vtail),
        (base_pt + 2 * pvh, 2 * LANE, pvh),
        (vtail, 2 * LANE + pvh, vtail),
        (2 * vtail, 3 * LANE, hd - 2 * vtail),
        (base_norm, 4 * LANE, pvh),
        (base_pair, 5 * LANE, heads * LANE),
    ]
    wo[pvh:LANE, :] = jnp.zeros((vtail, chan), BF16)
    wo[4 * LANE + pvh : 5 * LANE, :] = jnp.zeros((vtail, chan), BF16)
    wo_copies = [
        pltpu.make_async_copy(
            wo_hbm.at[pl.ds(src, count)], wo.at[pl.ds(dst, count)], wo_sem.at[k]
        )
        for k, (src, dst, count) in enumerate(wo_moves)
    ]
    for copy in wo_copies:
        copy.start()


    for copy in small_copies[3:]:
        copy.wait()
    lane_row = iota((1, LANE), 1)

    def as_col(row):
        wide = jnp.broadcast_to(row, (HP, heads))
        pick = iota((HP, heads), 0) == iota((HP, heads), 1)
        return jnp.sum(jnp.where(pick, wide, 0.0), axis=1, keepdims=True)

    hw = hw_ref[...]
    soft = jnp.maximum(hw, 0.0) + jnp.log(1.0 + jnp.exp(-jnp.abs(hw)))
    w_col = as_col(soft * (2.0 / (9.0 * pq)) ** 0.5)
    cw_col = as_col(cw_ref[...])

    head_of = iota((HP, LANE), 0)
    lane_hp = iota((HP, LANE), 1)
    q_tail = hd - LANE
    qq0 = q_tail
    kk0 = q_tail + 2 * heads
    kk1 = kk0 + 3 * heads
    point_mask = ((lane_hp % pqh) // pq == head_of) & (lane_hp < 2 * pqh)
    tail_mask = ((lane_hp < q_tail) & ((lane_hp + LANE) // dh == head_of)) | (
        (lane_hp >= q_tail) & ((lane_hp - q_tail) % heads == head_of) & (lane_hp < kk1)
    )
    mh[:, 0:LANE] = (lane_hp // dh == head_of).astype(F32)
    mh[:, LANE : 2 * LANE] = tail_mask.astype(F32)
    for k in range(6):
        mh[:, (2 + k) * LANE : (3 + k) * LANE] = point_mask.astype(F32)
    v_mask = (lane_hp // pv == head_of) & (lane_hp < pvh)
    o_masks = [
        ((lane_hp - pvh) % heads == head_of) & (lane_hp < pvh + 2 * heads),
        ((lane_hp - pvh) // dh == head_of),
        ((lane_hp - pvh + vtail) // dh == head_of),
    ]
    for k in range(3):
        me_mask[:, k * LANE : (k + 1) * LANE] = (
            v_mask | ((lane_hp >= pvh) & o_masks[k])
        ).astype(F32)
    me_mask[:, 3 * LANE : 4 * LANE] = ((lane_hp + 2 * vtail) // dh == head_of).astype(F32)
    big_row = iota((LANE, 4 * LANE), 0) - pvh
    big_col = iota((LANE, 4 * LANE), 1)
    big_lane = big_col % LANE
    big_tile = big_col // LANE
    o_col = jnp.where(
        big_tile == 3, big_lane + 2 * vtail, big_lane - pvh + (big_tile - 1) * vtail
    )
    is_point = (big_tile < 3) & (big_lane < pvh)
    big_head = jnp.where(is_point, big_lane // pv, o_col // dh)
    has_head = is_point | (big_tile > 0)
    expm[...] = (
        (big_head == big_row) & has_head & (big_row >= 0) & (big_row < heads)
    ).astype(BF16)
    w_lane = jnp.sum(jnp.where(point_mask, w_col, 0.0), axis=0, keepdims=True)
    half_lane = -0.5 * jnp.sum(
        jnp.where((lane_hp - q_tail) % heads == head_of, w_col, 0.0), axis=0, keepdims=True
    )
    dec_row = iota((LANE, LANE), 0)
    for k in range(12):
        dec[:, k * LANE : (k + 1) * LANE] = ((dec_row % 12 == k) & (dec_row < 36)).astype(BF16)
    sel = (
        (iota((LANE, LANE), 0) < pqh)
        & (iota((LANE, LANE), 1) >= q_tail)
        & (iota((LANE, LANE), 1) < kk1)
        & ((iota((LANE, LANE), 1) - q_tail) % heads == iota((LANE, LANE), 0) // pq)
    ).astype(BF16)

    chain_v = chain[...]
    mask_v = mask[...]

    def total(values):
        return jnp.sum(
            jnp.sum(values.astype(F32), axis=1, keepdims=True), axis=0, keepdims=True
        )

    plane_rows = cores * rows
    block_rows = SPAN * plane_rows
    key_local = iota((1, nk), 1)
    key_plane = (z - (z + c) % SPAN + (key_local // plane_rows) % SPAN + nz) % nz
    key_index = (
        ((key_local // block_rows) * nz + key_plane) * plane_rows + key_local % plane_rows
    ).astype(F32)
    q_local = iota((nq, 1), 0)
    q_index = (
        x * (nb * block_rows)
        + (q_local // rows) * block_rows
        + (zp * cores + c) * rows
        + q_local % rows
    ).astype(F32)
    key_chain = jnp.zeros((1, nk), F32)
    q_chain = jnp.zeros((nq, 1), F32)
    for k in range(1, 4):
        edge = total(chain_v < k)
        key_chain = key_chain + (key_index >= edge).astype(F32)
        q_chain = q_chain + (q_index >= edge).astype(F32)
    same[...] = (q_chain == key_chain).astype(F32)
    pad_row = ((key_index < total(mask_v)).astype(F32) - 1.0) * 100000.0

    for copy in raw_copies:
        copy.wait()
    wq[...] = jnp.transpose(wqt[...])
    wk[...] = jnp.transpose(wkt[...])
    wv[...] = jnp.transpose(wvt[...])

    pw16 = jnp.concatenate([pw_ref[...].astype(F32), jnp.zeros((HP - heads, LANE), F32)], axis=0)
    pw16 = pw16.astype(BF16)

    def global_points(px, py, pz, fb):
        def part(k):
            return fb[:, k * LANE : (k + 1) * LANE]

        return [
            part(3 * k) * px + part(3 * k + 1) * py + part(3 * k + 2) * pz + part(9 + k)
            for k in range(3)
        ]

    def tiles(values, start, count):
        return [values[:, (start + k) * LANE : (start + k + 1) * LANE] for k in range(count)]

    def key_phase(layer):
        message = kx[layer].reshape(nk, chan + LANE)
        fb = dot(message[:, chan:], dec[...])
        body = message[:, :chan]
        projected = dot(body, wk[...])
        lane = iota((nk, LANE), 1)
        g = global_points(*tiles(projected, 2, 3), fb)
        square = g[0] * g[0] + g[1] * g[1] + g[2] * g[2]
        kk = spread(square, sel) * half_lane
        hi = kk.astype(BF16).astype(F32)
        mid = (kk - hi).astype(BF16).astype(F32)
        lo = kk - hi - mid
        kk = jnp.where(lane < kk0 + heads, hi, jnp.where(lane < kk0 + 2 * heads, mid, lo))
        kk = jnp.where(lane < kk1, kk, 0.0)
        tail = jnp.where(
            lane < q_tail, projected[:, LANE : 2 * LANE], jnp.where(lane < kk0, 1.0, kk)
        )
        kf[:, 0:LANE] = projected[:, 0:LANE].astype(BF16)
        kf[:, LANE : 2 * LANE] = tail.astype(BF16)
        for k in range(3):
            hi = g[k].astype(BF16).astype(F32)
            pts = jnp.where(lane < pqh, hi, jnp.where(lane < 2 * pqh, g[k] - hi, 0.0)).astype(BF16)
            kf[:, (2 + k) * LANE : (3 + k) * LANE] = pts
            kf[:, (5 + k) * LANE : (6 + k) * LANE] = pts
        values = dot(body, wv[...])
        parts = tiles(values, 0, 4)
        g = global_points(parts[0], parts[1], parts[2], fb)
        for k in range(3):
            whole = jnp.where(lane < pvh, g[k], parts[k])
            hi = whole.astype(BF16)
            vh[:, k * LANE : (k + 1) * LANE] = hi
            vl[:, k * LANE : (k + 1) * LANE] = jnp.where(
                lane < pvh, whole - hi.astype(F32), 0.0
            ).astype(BF16)
        vh[:, 3 * LANE : 4 * LANE] = parts[3].astype(BF16)

    def query_phase(layer):
        scale = dh ** -0.5
        message = qx[layer].reshape(nq, chan + LANE)
        fb = dot(message[:, chan:], dec[...])
        fq[...] = fb
        projected = dot(message[:, :chan], wq[...])
        lane = iota((nq, LANE), 1)
        g = global_points(*tiles(projected, 2, 3), fb)
        square = g[0] * g[0] + g[1] * g[1] + g[2] * g[2]
        qq = spread(square, sel) * half_lane
        hi = qq.astype(BF16).astype(F32)
        qq = jnp.where(lane < qq0 + heads, hi, qq - hi)
        tail = jnp.where(
            lane < q_tail,
            projected[:, LANE : 2 * LANE] * scale,
            jnp.where(lane < kk0, qq, jnp.where(lane < kk1, 1.0, 0.0)),
        )
        qf[:, 0:LANE] = projected[:, 0:LANE].astype(BF16).astype(F32) * scale
        qf[:, LANE : 2 * LANE] = tail.astype(BF16).astype(F32)
        for k in range(3):
            scaled = g[k] * w_lane
            hi = scaled.astype(BF16).astype(F32)
            qf[:, (2 + k) * LANE : (3 + k) * LANE] = hi
            qf[:, (5 + k) * LANE : (6 + k) * LANE] = jnp.where(lane < pqh, scaled - hi, 0.0)

    def score_chunk(n):
        parts = []
        for r in range(rows):
            row = qf[pl.ds(n * rows + r, 1), :]
            parts.append((jnp.broadcast_to(row, (HP, 8 * LANE)) * mh[...]).astype(BF16))
        s = dot_nt(jnp.concatenate(parts, axis=0), kf[...]) * LOGIT_WEIGHT
        extra = []
        for r in range(rows):
            match = jnp.broadcast_to(same[pl.ds(n * rows + r, 1), :], (HP, nk))
            extra.append(match * cw_col + pad_row)
        return s + jnp.concatenate(extra, axis=0)

    def chunk_rows(n):
        return pl.ds(pl.multiple_of(n * rows * HP, rows * HP), rows * HP)

    def score_phase():
        def step(n, carry):
            scores[chunk_rows(n), :] = score_chunk(n)
            return carry

        lax.fori_loop(0, nb, step, 0)

    def p_copy(layer, n):
        return pltpu.make_async_remote_copy(
            src_ref=spb.at[layer, n],
            dst_ref=pr.at[layer, zb],
            send_sem=p_send.at[layer],
            recv_sem=p_recv.at[layer, zb],
            device_id=far_dev(n),
            device_id_type=pl.DeviceIdType.MESH,
        )

    lane_all = iota((rows * HP, LANE), 1)

    def chunk_phase(layer):
        def chunk(t):
            n = far_step(t)
            if layer == 0:

                @pl.when((t >= 2) & (t + 4 < nb))
                def _():
                    exchange(t + 4, across)

                logits = scores[chunk_rows(n), :]
                with jax.named_scope("tile_wait"):
                    pltpu.make_async_copy(tile.at[n], tile.at[n], a2a_recv.at[n]).wait()
                pair_rows = [tile[n, r] for r in range(rows)]
                own = jnp.concatenate([dot_nt(pw16, v) for v in pair_rows], axis=0) * LOGIT_WEIGHT
                logits = logits + own
            else:
                pair_rows = [tile[n, r] for r in range(rows)]
                logits = score_chunk(n) + bias[chunk_rows(n), :]
            top = jnp.max(logits, axis=1, keepdims=True)
            p = jnp.exp(logits - top)
            count = jnp.sum(p, axis=1, keepdims=True)
            p = p.astype(BF16)
            inverse = 1.0 / count
            log_sum = top + jnp.log(count)
            mixed = jnp.concatenate(
                [dot(p[r * HP : (r + 1) * HP, :], pair_rows[r]) for r in range(rows)], axis=0
            )
            main = dot(p, vh[...])
            rest = dot(p, vl[...])
            turn = fq[pl.ds(n * rows, rows), :]
            po[...] = mixed * inverse
            if layer == 0:
                bias[chunk_rows(n), :] = own
            for k in range(4):
                value = main[:, k * LANE : (k + 1) * LANE]
                if k < 3:
                    value = value + rest[:, k * LANE : (k + 1) * LANE]
                value = value * inverse
                if k == 0:
                    value = jnp.where(lane_all < pvh, value, log_sum)
                for r in range(rows):
                    sm[r : r + 1, k * LANE : (k + 1) * LANE] = jnp.sum(
                        value[r * HP : (r + 1) * HP, :]
                        * me_mask[:, k * LANE : (k + 1) * LANE],
                        axis=0,
                        keepdims=True,
                    )
            part = tiles(sm[...], 0, 4)
            frame = tiles(turn, 0, 12)
            moved = [part[k] - frame[9 + k] for k in range(3)]
            inside = lane8 < pvh
            for k in range(3):
                local = frame[k] * moved[0] + frame[3 + k] * moved[1] + frame[6 + k] * moved[2]
                if k == 0:
                    hi = part[0].astype(BF16).astype(F32)
                    other = jnp.where(lane8 < pvh + heads, hi, part[0] - hi)
                else:
                    other = part[k]
                spb[layer, n, heads + k] = jnp.where(inside, local, other).astype(BF16)
            spb[layer, n, heads + 3] = part[3].astype(BF16)
            for h in range(heads):
                spb[layer, n, h] = po[pl.ds(h, rows, stride=HP), :].astype(BF16)
            return n

        def step(t, carry):
            p_copy(layer, chunk(t)).start()
            return carry

        lax.fori_loop(0, nb - 1, step, 0)
        chunk(nb - 1)

    def combine(layer):
        slots = [(zb + d) % nb for d in range(nb)]
        with jax.named_scope("part_wait"):
            for n in slots[1:]:
                pltpu.make_async_copy(pr.at[layer, n], pr.at[layer, n], p_recv.at[layer, n]).wait()

        def piece(d, k):
            ref = spb if d == 0 else pr
            return ref[layer, slots[d], k].astype(F32)

        first = jnp.concatenate([piece(d, heads) for d in range(nb)], axis=0)
        sums = first + pltpu.roll(first, LANE - heads, 1)
        valid_all = (iota((nb * rows, LANE), 1) >= pvh) & (
            iota((nb * rows, LANE), 1) < pvh + heads
        )
        sums = jnp.where(valid_all, sums, 0.0)
        valid = (lane8 >= pvh) & (lane8 < pvh + heads)
        sums = [sums[d * rows : (d + 1) * rows, :] for d in range(nb)]
        top = functools.reduce(jnp.maximum, sums)
        shares = [jnp.where(valid, jnp.exp(value - top), 0.0) for value in sums]
        whole = jnp.where(valid, functools.reduce(jnp.add, shares), 1.0)
        shares = [value / whole for value in shares]
        wide = spread(jnp.concatenate(shares, axis=0), expm[...])
        mixed = []
        for k in range(4):
            acc = None
            for d in range(nb):
                term = wide[d * rows : (d + 1) * rows, k * LANE : (k + 1) * LANE] * piece(
                    d, heads + k
                )
                acc = term if acc is None else acc + term
            mixed.append(acc)
        pairs = []
        for h in range(heads):
            acc = None
            for d in range(nb):
                term = col(shares[d], pvh + h) * piece(d, h)
                acc = term if acc is None else acc + term
            pairs.append(acc)
        return mixed, pairs

    def gain_row(ref):
        return jnp.concatenate([ref[k : k + 1, :] for k in range(chan // LANE)], axis=1)

    def update(layer, state, fr, mixed, pairs):
        turn = [col(fr, k) for k in range(9)]
        shift = [col(fr, 9 + k) for k in range(3)]
        inside = lane8 < pvh
        norm = jnp.sqrt(
            mixed[0] * mixed[0] + mixed[1] * mixed[1] + mixed[2] * mixed[2] + 1e-08
        )
        concat = mixed + [jnp.where(inside, norm, 0.0)] + pairs
        concat = jnp.concatenate(concat, axis=1).astype(BF16)
        if layer == 0:
            for copy in wo_copies:
                copy.wait()
        state = state + dot(concat, wo[...])
        normed = layer_norm(state, gain_row(g1_ref))
        hidden = jnp.maximum(dot(normed.astype(BF16), m1[...]), 0.0).astype(BF16)
        hidden = jnp.maximum(dot(hidden, m2[...]), 0.0).astype(BF16)
        state = layer_norm(normed + dot(hidden, m3[...]), gain_row(g2_ref))
        if layer == LAYERS - 1:
            state_buf[...] = state
            last_copies[0].start()
        state_bf = state.astype(BF16)
        upd = dot_nt(state_bf, fw_ref[...])
        u = [jnp.broadcast_to(upd[:, k : k + 1], (rows, LANE)) for k in range(6)]
        inverse = lax.rsqrt(1.0 + u[0] * u[0] + u[1] * u[1] + u[2] * u[2])
        vx, vy, vz = u[0] * inverse, u[1] * inverse, u[2] * inverse
        square = inverse * inverse
        matrix = [
            [
                square + vx * vx - vy * vy - vz * vz,
                2.0 * (vx * vy - inverse * vz),
                2.0 * (vx * vz + inverse * vy),
            ],
            [
                2.0 * (vx * vy + inverse * vz),
                square - vx * vx + vy * vy - vz * vz,
                2.0 * (vy * vz - inverse * vx),
            ],
            [
                2.0 * (vx * vz - inverse * vy),
                2.0 * (vy * vz + inverse * vx),
                square - vx * vx - vy * vy + vz * vz,
            ],
        ]
        entries = [
            turn[3 * a] * matrix[0][b]
            + turn[3 * a + 1] * matrix[1][b]
            + turn[3 * a + 2] * matrix[2][b]
            for a in range(3)
            for b in range(3)
        ] + [
            turn[3 * a] * u[3] + turn[3 * a + 1] * u[4] + turn[3 * a + 2] * u[5] + shift[a]
            for a in range(3)
        ]
        fr = jnp.zeros((rows, LANE), F32)
        for k in range(12):
            fr = jnp.where((lane8 % 12 == k) & (lane8 < 36), entries[k], fr)
        return state, state_bf, fr

    last_copies = [
        pltpu.make_async_copy(src, dst, last_sem.at[k])
        for k, (src, dst) in enumerate(
            ((state_buf, out_state), (turn_buf, out_turn), (shift_buf, out_shift))
        )
    ]
    state = single[...].astype(F32)
    for layer in range(LAYERS):
        if layer == 0:
            exchange_across(2)
        with jax.named_scope(f"key_wait_{layer}"):
            pltpu.make_async_copy(
                kx.at[layer, 0 : g_count - 1], kx.at[layer, 0 : g_count - 1], kx_recv.at[layer]
            ).wait()
        if layer == 0:
            exchange_across(3)
        with jax.named_scope(f"key_{layer}"):
            key_phase(layer)
        with jax.named_scope(f"query_wait_{layer}"):
            pltpu.make_async_copy(
                qx.at[layer, 0 : nb - 1], qx.at[layer, 0 : nb - 1], qx_recv.at[layer]
            ).wait()
        with jax.named_scope(f"query_{layer}"):
            query_phase(layer)
        if layer == 0:
            exchange_across(4)
            with jax.named_scope(f"score_{layer}"):
                score_phase()
            exchange_across(5)
        with jax.named_scope(f"chunk_{layer}"):
            chunk_phase(layer)
        with jax.named_scope(f"combine_{layer}"):
            mixed, pairs = combine(layer)
        with jax.named_scope(f"update_{layer}"):
            state, state_bf, frames = update(layer, state, frames, mixed, pairs)
        if layer + 1 < LAYERS:
            with jax.named_scope(f"send_{layer}"):
                put_message(layer + 1, state_bf, frames)
                send_message(layer + 1)
    turn_buf[...] = frames[:, 0:9]
    pick = (iota((3, LANE), 1) == iota((3, LANE), 0) + 9).astype(F32)
    shift_buf[...] = lax.dot_general(
        pick, frames, (((1,), (1,)), ((), ())), precision=lax.Precision.HIGHEST,
        preferred_element_type=F32,
    )
    last_copies[1].start()
    last_copies[2].start()
    for layer in range(LAYERS):
        pltpu.make_async_copy(
            kx.at[layer, 0 : g_count - 1], kx.at[layer, 0 : g_count - 1], x_send.at[layer]
        ).wait()
        pltpu.make_async_copy(
            qx.at[layer, 0 : nb - 1], qx.at[layer, 0 : nb - 1], x_send.at[layer]
        ).wait()
        pltpu.make_async_copy(
            pr.at[layer, 0 : nb - 1], pr.at[layer, 0 : nb - 1], p_send.at[layer]
        ).wait()
    for offset in near:
        pltpu.make_async_copy(pair.at[0, :, 0, 0], pair.at[0, :, 0, 0], a2a_send).wait()
    for copy in last_copies:
        copy.wait()


def hand_over(a, b, c, a_out, b_out, c_out, sem):
    copies = [
        pltpu.make_async_copy(src, dst, sem.at[k])
        for k, (src, dst) in enumerate(((a, a_out), (b, b_out), (c, c_out)))
    ]
    for copy in copies:
        copy.start()
    for copy in copies:
        copy.wait()


def on_device(
    pair_cols,
    single,
    rotation,
    translation,
    residue_mask,
    chain_index,
    query_weight,
    key_weight,
    value_weight,
    qpoint_weight,
    kpoint_weight,
    vpoint_weight,
    pair_weight,
    head_weight,
    chain_weight,
    output_weight,
    gain_first,
    mlp_first,
    mlp_second,
    mlp_third,
    gain_second,
    frame_weight,
):
    nx = lax.axis_size("row_0")
    nz = lax.axis_size("row_1")
    cores = lax.axis_size("row_2")
    nb = nz // SPAN
    rows, chan = single.shape
    heads = head_weight.shape[0]
    hd = query_weight.shape[1]
    g_count = nx * SPAN * cores
    nk = g_count * rows
    nq = nb * rows
    width = chan + LANE
    pair = pair_cols.reshape(nx, nb, SPAN, cores, rows, *pair_cols.shape[1:])
    hbm = pl.BlockSpec(memory_space=pl.ANY)
    small = [
        single,
        jnp.transpose(rotation),
        translation,
        residue_mask.reshape(-1, LANE),
        chain_index.reshape(-1, LANE),
        pair_weight,
        head_weight.reshape(1, -1),
        chain_weight.reshape(1, -1),
        gain_first.reshape(-1, LANE),
        gain_second.reshape(-1, LANE),
        jnp.transpose(frame_weight),
    ]
    scratch = [pltpu.VMEM(v.shape, v.dtype) for v in small] + [
        pltpu.VMEM((nb, rows, nk, LANE), BF16),
        pltpu.VMEM((LAYERS, g_count, rows, width), BF16),
        pltpu.VMEM((LAYERS, nb, rows, width), BF16),
        pltpu.VMEM((LAYERS, rows, width), BF16),
        pltpu.VMEM((5 * LANE, chan), BF16),
        pltpu.VMEM((5 * LANE, chan), BF16),
        pltpu.VMEM((4 * LANE, chan), BF16),
        pltpu.VMEM((chan, 5 * LANE), BF16),
        pltpu.VMEM((chan, 5 * LANE), BF16),
        pltpu.VMEM((chan, 4 * LANE), BF16),
        pltpu.VMEM(((5 + heads) * LANE, chan), BF16),
        pltpu.VMEM(mlp_first.shape, BF16),
        pltpu.VMEM(mlp_second.shape, BF16),
        pltpu.VMEM(mlp_third.shape, BF16),
        pltpu.VMEM((LANE, 12 * LANE), BF16),
        pltpu.VMEM((LANE, 4 * LANE), BF16),
        pltpu.VMEM((nq, 8 * LANE), F32),
        pltpu.VMEM((nk, 8 * LANE), BF16),
        pltpu.VMEM((nk, 4 * LANE), BF16),
        pltpu.VMEM((nk, 3 * LANE), BF16),
        pltpu.VMEM((nq * HP, nk), F32),
        pltpu.VMEM((nq * HP, nk), F32),
        pltpu.VMEM((nq, nk), F32),
        pltpu.VMEM((HP, 8 * LANE), F32),
        pltpu.VMEM((HP, 4 * LANE), F32),
        pltpu.VMEM((rows * HP, LANE), F32),
        pltpu.VMEM((rows, 4 * LANE), F32),
        pltpu.VMEM((nq, 12 * LANE), F32),
        pltpu.VMEM((LAYERS, nb, heads + 4, rows, LANE), BF16),
        pltpu.VMEM((LAYERS, nb, heads + 4, rows, LANE), BF16),
        pltpu.VMEM((rows, chan), F32),
        pltpu.VMEM((rows, 9), F32),
        pltpu.VMEM((3, rows), F32),
        pltpu.SemaphoreType.DMA((3,)),
        pltpu.SemaphoreType.DMA((11,)),
        pltpu.SemaphoreType.DMA((23,)),
        pltpu.SemaphoreType.DMA((8,)),
        pltpu.SemaphoreType.DMA((nb,)),
        pltpu.SemaphoreType.DMA,
        pltpu.SemaphoreType.DMA((LAYERS,)),
        pltpu.SemaphoreType.DMA((LAYERS,)),
        pltpu.SemaphoreType.DMA((LAYERS,)),
        pltpu.SemaphoreType.DMA((LAYERS,)),
        pltpu.SemaphoreType.DMA((LAYERS, nb)),
    ]
    state, turned, moved = pl.pallas_call(
        functools.partial(kernel, (nx, nb, cores, rows, heads)),
        name="structure_layers",
        out_shape=(
            jax.ShapeDtypeStruct((rows, chan), F32),
            jax.ShapeDtypeStruct((rows, 9), F32),
            jax.ShapeDtypeStruct((3, rows), F32),
        ),
        in_specs=[hbm] * 22,
        out_specs=(hbm, hbm, hbm),
        scratch_shapes=scratch,
        compiler_params=pltpu.CompilerParams(
            collective_id=0, has_side_effects=True, vmem_limit_bytes=62 * 1024 * 1024
        ),
    )(
        pair,
        *small[:5],
        jnp.transpose(query_weight),
        jnp.transpose(key_weight),
        jnp.transpose(value_weight),
        jnp.transpose(qpoint_weight),
        jnp.transpose(kpoint_weight),
        jnp.transpose(vpoint_weight),
        *small[5:8],
        output_weight,
        small[8],
        mlp_first,
        mlp_second,
        mlp_third,
        small[9],
        small[10],
    )
    state, turned, moved = pl.pallas_call(
        hand_over,
        name="hand_over",
        out_shape=tuple(jax.ShapeDtypeStruct(v.shape, v.dtype) for v in (state, turned, moved)),
        in_specs=[hbm] * 3,
        out_specs=(hbm,) * 3,
        scratch_shapes=[pltpu.SemaphoreType.DMA((3,))],
        compiler_params=pltpu.CompilerParams(vmem_limit_bytes=62 * 1024 * 1024),
    )(state, turned, moved)
    return state, jnp.transpose(turned), moved


def solution(mesh):
    finer = Mesh(
        mesh.devices.reshape(mesh.shape["groups"], 4, 16, 2), ("groups", "row_0", "row_1", "row_2")
    )
    in_specs = (
        P(None, GROUPS_ROW, None),
        P(GROUPS_ROW, None),
        P(None, GROUPS_ROW),
        P(None, GROUPS_ROW),
        P("groups"),
        P("groups"),
    ) + (P(),) * 16
    out_specs = (P(GROUPS_ROW, None), P(None, GROUPS_ROW), P(None, GROUPS_ROW))
    return jax.shard_map(
        on_device, mesh=finer, in_specs=in_specs, out_specs=out_specs, check_vma=False
    )
```

```python
import functools

import jax
import jax.numpy as jnp
from jax import lax
from jax.experimental import pallas as pl
from jax.experimental.pallas import tpu as pltpu
from jax.sharding import Mesh
from jax.sharding import PartitionSpec as P

LAYERS = 2
SPAN = 2
GROUPS_ROW = ("groups", "row_0", "row_1", "row_2")
LOGIT_WEIGHT = (1.0 / 3.0) ** 0.5
F32 = jnp.float32
BF16 = jnp.bfloat16
LANE = 128
HP = 16


def iota(shape, dim):
    return lax.broadcasted_iota(jnp.int32, shape, dim)


def dot(a, b):
    return jnp.dot(a, b, preferred_element_type=F32)


def dot_nt(a, b):
    return lax.dot_general(a, b, (((1,), (1,)), ((), ())), preferred_element_type=F32)


def split2(x):
    hi = x.astype(BF16)
    return hi, (x - hi.astype(F32)).astype(BF16)


def split3(x):
    hi = x.astype(BF16)
    rest = x - hi.astype(F32)
    mid = rest.astype(BF16)
    return hi, mid, (rest - mid.astype(F32)).astype(BF16)


def spread(x, table):
    hi, mid, lo = split3(x)
    return dot(hi, table) + dot(mid, table) + dot(lo, table)


def col(tile, lane):
    return jnp.broadcast_to(tile[:, lane : lane + 1], tile.shape)


def layer_norm(values, gain_vector):
    centered = values - jnp.mean(values, axis=-1, keepdims=True)
    variance = jnp.mean(centered * centered, axis=-1, keepdims=True)
    return centered * lax.rsqrt(variance + 1e-05) * gain_vector


def kernel(
    sizes,
    pair,
    single_hbm,
    rotation_hbm,
    translation_hbm,
    mask_hbm,
    chain_hbm,
    wq_hbm,
    wk_hbm,
    wv_hbm,
    wqp_hbm,
    wkp_hbm,
    wvp_hbm,
    pw_hbm,
    hw_hbm,
    cw_hbm,
    wo_hbm,
    g1_hbm,
    m1_hbm,
    m2_hbm,
    m3_hbm,
    g2_hbm,
    fw_hbm,
    out_state,
    out_turn,
    out_shift,
    single,
    rotation,
    translation,
    mask,
    chain,
    pw_ref,
    hw_ref,
    cw_ref,
    g1_ref,
    g2_ref,
    fw_ref,
    tile,
    kx,
    qx,
    xs,
    wqt,
    wkt,
    wvt,
    wq,
    wk,
    wv,
    wo,
    m1,
    m2,
    m3,
    dec,
    expm,
    qf,
    kf,
    vh,
    vl,
    scores,
    bias,
    same,
    mh,
    me_mask,
    po,
    sm,
    fq,
    spb,
    pr,
    state_buf,
    turn_buf,
    shift_buf,
    last_sem,
    small_sem,
    w_sem,
    wo_sem,
    a2a_recv,
    a2a_send,
    x_send,
    kx_recv,
    qx_recv,
    p_send,
    p_recv,
):
    nx, nb, cores, rows, heads = sizes
    g_count = nx * SPAN * cores
    nk = g_count * rows
    nq = nb * rows
    chan = single.shape[1]
    pq3 = wqp_hbm.shape[0]
    pqh = pq3 // 3
    pq = pqh // heads
    pv3 = wvp_hbm.shape[0]
    pvh = pv3 // 3
    pv = pvh // heads
    hd = wq_hbm.shape[0]
    dh = hd // heads
    vtail = LANE - pvh
    x = lax.axis_index("row_0")
    z = lax.axis_index("row_1")
    c = lax.axis_index("row_2")
    nz = nb * SPAN
    zb = z // SPAN
    zp = z % SPAN

    def partner(core):
        return (z + 1 - 2 * ((z + core) % SPAN) + nz) % nz

    def place(core):
        return (x * SPAN + (z + core) % SPAN) * cores + c

    me = place(c)
    near = []
    for dx in (2, 1, 3, 0) if nx == 4 else range(nx):
        for dz in range(SPAN):
            for dc in range(cores):
                if dx or dz or dc:
                    near.append((dx, dz, dc))

    def near_id(offset):
        dx, dz, dc = offset
        core = (c + dc) % cores
        return (x + dx) % nx, partner(core) if dz else z, core

    def source_id(offset):
        dx, dz, dc = offset
        return (x + dx) % nx, partner(c) if dz else z, (c + dc) % cores

    def dev(px, pz, pc):
        return {"row_0": px, "row_1": pz, "row_2": pc}

    def far_dev(block):
        return dev(x, block * SPAN + zp, c)

    def far_step(t, block=None):
        half = (t + 1) // 2
        sign = 1 - 2 * (t % 2)
        return ((zb if block is None else block) + nb // 2 + sign * half + nb) % nb

    barrier = pltpu.get_barrier_semaphore()
    for t in range(nb - 1):
        pl.semaphore_signal(
            barrier, inc=1, device_id=far_dev(far_step(t)), device_id_type=pl.DeviceIdType.MESH
        )
    for offset in near:
        pl.semaphore_signal(
            barrier,
            inc=1,
            device_id=dev(*source_id(offset)),
            device_id_type=pl.DeviceIdType.MESH,
        )
    small = [
        (single_hbm, single),
        (rotation_hbm, rotation),
        (translation_hbm, translation),
        (mask_hbm, mask),
        (chain_hbm, chain),
        (pw_hbm, pw_ref),
        (hw_hbm, hw_ref),
        (cw_hbm, cw_ref),
        (g1_hbm, g1_ref),
        (g2_hbm, g2_ref),
        (fw_hbm, fw_ref),
    ]
    small_copies = [
        pltpu.make_async_copy(src, dst, small_sem.at[k]) for k, (src, dst) in enumerate(small)
    ]
    for copy in small_copies:
        copy.start()

    across = [offset for offset in near if offset[1]]
    within = [offset for offset in near if not offset[1]]

    def exchange(t, offsets):
        for offset in offsets:
            px, pz, pc = near_id(offset)
            n = far_step(t, pz // SPAN)
            pltpu.make_async_remote_copy(
                src_ref=pair.at[px, n, pz % SPAN, pc],
                dst_ref=tile.at[n, :, pl.ds(place(pc) * rows, rows), :],
                send_sem=a2a_send,
                recv_sem=a2a_recv.at[n],
                device_id=dev(px, pz, pc),
                device_id_type=pl.DeviceIdType.MESH,
            ).start()

    def exchange_across(t):
        if t < nb:
            exchange(t, across)

    def exchange_within(t, carry):
        exchange(t, within)
        n = far_step(t)
        pltpu.make_async_copy(
            pair.at[x, n, zp, c], tile.at[n, :, pl.ds(me * rows, rows), :], a2a_recv.at[n]
        ).start()
        return carry

    with jax.named_scope("barrier"):
        pl.semaphore_wait(barrier, len(near) + nb - 1)
    exchange_within(0, 0)
    exchange_across(0)

    lane8 = iota((rows, LANE), 1)
    for copy in small_copies[:3]:
        copy.wait()
    take_r = (
        (iota((9, LANE), 1) % 12 == iota((9, LANE), 0)) & (iota((9, LANE), 1) < 36)
    ).astype(F32)
    take_t = (
        (iota((3, LANE), 1) % 12 == iota((3, LANE), 0) + 9) & (iota((3, LANE), 1) < 36)
    ).astype(F32)
    contract0 = (((0,), (0,)), ((), ()))
    frames = jnp.dot(
        rotation[...], take_r, precision=lax.Precision.HIGHEST, preferred_element_type=F32
    ) + lax.dot_general(
        translation[...], take_t, contract0, precision=lax.Precision.HIGHEST,
        preferred_element_type=F32,
    )

    def frame_columns(fr):
        hi = fr.astype(BF16).astype(F32)
        mid = (fr - hi).astype(BF16).astype(F32)
        lo = fr - hi - mid
        return jnp.where(lane8 < 12, hi, jnp.where(lane8 < 24, mid, lo)).astype(BF16)

    def put_message(layer, state_bf, fr):
        tail = frame_columns(fr)
        for ref in (xs.at[layer], kx.at[layer, me], qx.at[layer, zb]):
            ref[:, 0:chan] = state_bf
            ref[:, chan : chan + LANE] = tail

    def x_near(layer, offset):
        target = near_id(offset)
        return pltpu.make_async_remote_copy(
            src_ref=xs.at[layer],
            dst_ref=kx.at[layer, place(target[2])],
            send_sem=x_send.at[layer],
            recv_sem=kx_recv.at[layer],
            device_id=dev(*target),
            device_id_type=pl.DeviceIdType.MESH,
        )

    def far_copy(layer, block):
        return pltpu.make_async_remote_copy(
            src_ref=xs.at[layer],
            dst_ref=qx.at[layer, zb],
            send_sem=x_send.at[layer],
            recv_sem=qx_recv.at[layer],
            device_id=far_dev(block),
            device_id_type=pl.DeviceIdType.MESH,
        )

    def send_message(layer):
        for t in range(nb - 1):
            far_copy(layer, far_step(t)).start()
        for offset in near:
            x_near(layer, offset).start()

    put_message(0, single[...], frames)
    send_message(0)
    with jax.named_scope("exchange"):
        lax.fori_loop(1, nb, exchange_within, 0)
        exchange_across(1)
    moves = [(wq_hbm, 0, wqt, 0, hd), (wk_hbm, 0, wkt, 0, hd)]
    for src, dst in ((wqp_hbm, wqt), (wkp_hbm, wkt)):
        for k in range(3):
            for copy_index in range(2):
                moves.append((src, k * pqh, dst, (2 + k) * LANE + copy_index * pqh, pqh))
    for k in range(3):
        moves.append((wvp_hbm, k * pvh, wvt, k * LANE, pvh))
    moves += [
        (wv_hbm, 0, wvt, LANE + pvh, vtail),
        (wv_hbm, vtail, wvt, 2 * LANE + pvh, vtail),
        (wv_hbm, 2 * vtail, wvt, 3 * LANE, hd - 2 * vtail),
        (m1_hbm, 0, m1, 0, chan),
        (m2_hbm, 0, m2, 0, chan),
        (m3_hbm, 0, m3, 0, chan),
    ]
    for ref in (wqt, wkt):
        ref[hd : 2 * LANE, :] = jnp.zeros((2 * LANE - hd, chan), BF16)
        for k in range(3):
            ref[(2 + k) * LANE + 2 * pqh : (3 + k) * LANE, :] = jnp.zeros(
                (LANE - 2 * pqh, chan), BF16
            )
    wvt[pvh:LANE, :] = jnp.zeros((vtail, chan), BF16)
    raw_copies = [
        pltpu.make_async_copy(
            src.at[pl.ds(start, count)], dst.at[pl.ds(into, count)], w_sem.at[k]
        )
        for k, (src, start, dst, into, count) in enumerate(moves)
    ]
    for copy in raw_copies:
        copy.start()
    base_pt = hd
    base_norm = hd + pv3
    base_pair = base_norm + pvh
    wo_moves = [
        (base_pt, 0, pvh),
        (base_pt + pvh, LANE, pvh),
        (0, LANE + pvh, vtail),
        (base_pt + 2 * pvh, 2 * LANE, pvh),
        (vtail, 2 * LANE + pvh, vtail),
        (2 * vtail, 3 * LANE, hd - 2 * vtail),
        (base_norm, 4 * LANE, pvh),
        (base_pair, 5 * LANE, heads * LANE),
    ]
    wo[pvh:LANE, :] = jnp.zeros((vtail, chan), BF16)
    wo[4 * LANE + pvh : 5 * LANE, :] = jnp.zeros((vtail, chan), BF16)
    wo_copies = [
        pltpu.make_async_copy(
            wo_hbm.at[pl.ds(src, count)], wo.at[pl.ds(dst, count)], wo_sem.at[k]
        )
        for k, (src, dst, count) in enumerate(wo_moves)
    ]
    for copy in wo_copies:
        copy.start()


    for copy in small_copies[3:]:
        copy.wait()
    lane_row = iota((1, LANE), 1)

    def as_col(row):
        wide = jnp.broadcast_to(row, (HP, heads))
        pick = iota((HP, heads), 0) == iota((HP, heads), 1)
        return jnp.sum(jnp.where(pick, wide, 0.0), axis=1, keepdims=True)

    hw = hw_ref[...]
    soft = jnp.maximum(hw, 0.0) + jnp.log(1.0 + jnp.exp(-jnp.abs(hw)))
    w_col = as_col(soft * (2.0 / (9.0 * pq)) ** 0.5)
    cw_col = as_col(cw_ref[...])

    head_of = iota((HP, LANE), 0)
    lane_hp = iota((HP, LANE), 1)
    q_tail = hd - LANE
    qq0 = q_tail
    kk0 = q_tail + 2 * heads
    kk1 = kk0 + 3 * heads
    point_mask = ((lane_hp % pqh) // pq == head_of) & (lane_hp < 2 * pqh)
    tail_mask = ((lane_hp < q_tail) & ((lane_hp + LANE) // dh == head_of)) | (
        (lane_hp >= q_tail) & ((lane_hp - q_tail) % heads == head_of) & (lane_hp < kk1)
    )
    mh[:, 0:LANE] = (lane_hp // dh == head_of).astype(F32)
    mh[:, LANE : 2 * LANE] = tail_mask.astype(F32)
    for k in range(6):
        mh[:, (2 + k) * LANE : (3 + k) * LANE] = point_mask.astype(F32)
    v_mask = (lane_hp // pv == head_of) & (lane_hp < pvh)
    o_masks = [
        ((lane_hp - pvh) % heads == head_of) & (lane_hp < pvh + 2 * heads),
        ((lane_hp - pvh) // dh == head_of),
        ((lane_hp - pvh + vtail) // dh == head_of),
    ]
    for k in range(3):
        me_mask[:, k * LANE : (k + 1) * LANE] = (
            v_mask | ((lane_hp >= pvh) & o_masks[k])
        ).astype(F32)
    me_mask[:, 3 * LANE : 4 * LANE] = ((lane_hp + 2 * vtail) // dh == head_of).astype(F32)
    big_row = iota((LANE, 4 * LANE), 0) - pvh
    big_col = iota((LANE, 4 * LANE), 1)
    big_lane = big_col % LANE
    big_tile = big_col // LANE
    o_col = jnp.where(
        big_tile == 3, big_lane + 2 * vtail, big_lane - pvh + (big_tile - 1) * vtail
    )
    is_point = (big_tile < 3) & (big_lane < pvh)
    big_head = jnp.where(is_point, big_lane // pv, o_col // dh)
    has_head = is_point | (big_tile > 0)
    expm[...] = (
        (big_head == big_row) & has_head & (big_row >= 0) & (big_row < heads)
    ).astype(BF16)
    w_lane = jnp.sum(jnp.where(point_mask, w_col, 0.0), axis=0, keepdims=True)
    half_lane = -0.5 * jnp.sum(
        jnp.where((lane_hp - q_tail) % heads == head_of, w_col, 0.0), axis=0, keepdims=True
    )
    dec_row = iota((LANE, LANE), 0)
    for k in range(12):
        dec[:, k * LANE : (k + 1) * LANE] = ((dec_row % 12 == k) & (dec_row < 36)).astype(BF16)
    sel = (
        (iota((LANE, LANE), 0) < pqh)
        & (iota((LANE, LANE), 1) >= q_tail)
        & (iota((LANE, LANE), 1) < kk1)
        & ((iota((LANE, LANE), 1) - q_tail) % heads == iota((LANE, LANE), 0) // pq)
    ).astype(BF16)

    chain_v = chain[...]
    mask_v = mask[...]

    def total(values):
        return jnp.sum(
            jnp.sum(values.astype(F32), axis=1, keepdims=True), axis=0, keepdims=True
        )

    plane_rows = cores * rows
    block_rows = SPAN * plane_rows
    key_local = iota((1, nk), 1)
    key_plane = (z - (z + c) % SPAN + (key_local // plane_rows) % SPAN + nz) % nz
    key_index = (
        ((key_local // block_rows) * nz + key_plane) * plane_rows + key_local % plane_rows
    ).astype(F32)
    q_local = iota((nq, 1), 0)
    q_index = (
        x * (nb * block_rows)
        + (q_local // rows) * block_rows
        + (zp * cores + c) * rows
        + q_local % rows
    ).astype(F32)
    key_chain = jnp.zeros((1, nk), F32)
    q_chain = jnp.zeros((nq, 1), F32)
    for k in range(1, 4):
        edge = total(chain_v < k)
        key_chain = key_chain + (key_index >= edge).astype(F32)
        q_chain = q_chain + (q_index >= edge).astype(F32)
    same[...] = (q_chain == key_chain).astype(F32)
    pad_row = ((key_index < total(mask_v)).astype(F32) - 1.0) * 100000.0

    for copy in raw_copies:
        copy.wait()
    wq[...] = jnp.transpose(wqt[...])
    wk[...] = jnp.transpose(wkt[...])
    wv[...] = jnp.transpose(wvt[...])

    pw16 = jnp.concatenate([pw_ref[...].astype(F32), jnp.zeros((HP - heads, LANE), F32)], axis=0)
    pw16 = pw16.astype(BF16)

    def global_points(px, py, pz, fb):
        def part(k):
            return fb[:, k * LANE : (k + 1) * LANE]

        return [
            part(3 * k) * px + part(3 * k + 1) * py + part(3 * k + 2) * pz + part(9 + k)
            for k in range(3)
        ]

    def tiles(values, start, count):
        return [values[:, (start + k) * LANE : (start + k + 1) * LANE] for k in range(count)]

    def key_phase(layer):
        message = kx[layer].reshape(nk, chan + LANE)
        fb = dot(message[:, chan:], dec[...])
        body = message[:, :chan]
        projected = dot(body, wk[...])
        lane = iota((nk, LANE), 1)
        g = global_points(*tiles(projected, 2, 3), fb)
        square = g[0] * g[0] + g[1] * g[1] + g[2] * g[2]
        kk = spread(square, sel) * half_lane
        hi = kk.astype(BF16).astype(F32)
        mid = (kk - hi).astype(BF16).astype(F32)
        lo = kk - hi - mid
        kk = jnp.where(lane < kk0 + heads, hi, jnp.where(lane < kk0 + 2 * heads, mid, lo))
        kk = jnp.where(lane < kk1, kk, 0.0)
        tail = jnp.where(
            lane < q_tail, projected[:, LANE : 2 * LANE], jnp.where(lane < kk0, 1.0, kk)
        )
        kf[:, 0:LANE] = projected[:, 0:LANE].astype(BF16)
        kf[:, LANE : 2 * LANE] = tail.astype(BF16)
        for k in range(3):
            hi = g[k].astype(BF16).astype(F32)
            pts = jnp.where(lane < pqh, hi, jnp.where(lane < 2 * pqh, g[k] - hi, 0.0)).astype(BF16)
            kf[:, (2 + k) * LANE : (3 + k) * LANE] = pts
            kf[:, (5 + k) * LANE : (6 + k) * LANE] = pts
        values = dot(body, wv[...])
        parts = tiles(values, 0, 4)
        g = global_points(parts[0], parts[1], parts[2], fb)
        for k in range(3):
            whole = jnp.where(lane < pvh, g[k], parts[k])
            hi = whole.astype(BF16)
            vh[:, k * LANE : (k + 1) * LANE] = hi
            vl[:, k * LANE : (k + 1) * LANE] = jnp.where(
                lane < pvh, whole - hi.astype(F32), 0.0
            ).astype(BF16)
        vh[:, 3 * LANE : 4 * LANE] = parts[3].astype(BF16)

    def query_phase(layer):
        scale = dh ** -0.5
        message = qx[layer].reshape(nq, chan + LANE)
        fb = dot(message[:, chan:], dec[...])
        fq[...] = fb
        projected = dot(message[:, :chan], wq[...])
        lane = iota((nq, LANE), 1)
        g = global_points(*tiles(projected, 2, 3), fb)
        square = g[0] * g[0] + g[1] * g[1] + g[2] * g[2]
        qq = spread(square, sel) * half_lane
        hi = qq.astype(BF16).astype(F32)
        qq = jnp.where(lane < qq0 + heads, hi, qq - hi)
        tail = jnp.where(
            lane < q_tail,
            projected[:, LANE : 2 * LANE] * scale,
            jnp.where(lane < kk0, qq, jnp.where(lane < kk1, 1.0, 0.0)),
        )
        qf[:, 0:LANE] = projected[:, 0:LANE].astype(BF16).astype(F32) * scale
        qf[:, LANE : 2 * LANE] = tail.astype(BF16).astype(F32)
        for k in range(3):
            scaled = g[k] * w_lane
            hi = scaled.astype(BF16).astype(F32)
            qf[:, (2 + k) * LANE : (3 + k) * LANE] = hi
            qf[:, (5 + k) * LANE : (6 + k) * LANE] = jnp.where(lane < pqh, scaled - hi, 0.0)

    def score_chunk(n):
        parts = []
        for r in range(rows):
            row = qf[pl.ds(n * rows + r, 1), :]
            parts.append((jnp.broadcast_to(row, (HP, 8 * LANE)) * mh[...]).astype(BF16))
        s = dot_nt(jnp.concatenate(parts, axis=0), kf[...]) * LOGIT_WEIGHT
        extra = []
        for r in range(rows):
            match = jnp.broadcast_to(same[pl.ds(n * rows + r, 1), :], (HP, nk))
            extra.append(match * cw_col + pad_row)
        return s + jnp.concatenate(extra, axis=0)

    def chunk_rows(n):
        return pl.ds(pl.multiple_of(n * rows * HP, rows * HP), rows * HP)

    def score_phase():
        def step(n, carry):
            scores[chunk_rows(n), :] = score_chunk(n)
            return carry

        lax.fori_loop(0, nb, step, 0)

    def p_copy(layer, n):
        return pltpu.make_async_remote_copy(
            src_ref=spb.at[layer, n],
            dst_ref=pr.at[layer, zb],
            send_sem=p_send.at[layer],
            recv_sem=p_recv.at[layer, zb],
            device_id=far_dev(n),
            device_id_type=pl.DeviceIdType.MESH,
        )

    lane_all = iota((rows * HP, LANE), 1)

    def chunk_phase(layer):
        def chunk(t):
            n = far_step(t)
            if layer == 0:

                @pl.when((t == 1) & (t + 6 < nb))
                def _():
                    exchange(t + 6, across)

                logits = scores[chunk_rows(n), :]
                with jax.named_scope("tile_wait"):
                    pltpu.make_async_copy(tile.at[n], tile.at[n], a2a_recv.at[n]).wait()
                pair_rows = [tile[n, r] for r in range(rows)]
                own = jnp.concatenate([dot_nt(pw16, v) for v in pair_rows], axis=0) * LOGIT_WEIGHT
                logits = logits + own
            else:
                pair_rows = [tile[n, r] for r in range(rows)]
                logits = score_chunk(n) + bias[chunk_rows(n), :]
            top = jnp.max(logits, axis=1, keepdims=True)
            p = jnp.exp(logits - top)
            count = jnp.sum(p, axis=1, keepdims=True)
            p = p.astype(BF16)
            inverse = 1.0 / count
            log_sum = top + jnp.log(count)
            mixed = jnp.concatenate(
                [dot(p[r * HP : (r + 1) * HP, :], pair_rows[r]) for r in range(rows)], axis=0
            )
            main = dot(p, vh[...])
            rest = dot(p, vl[...])
            turn = fq[pl.ds(n * rows, rows), :]
            po[...] = mixed * inverse
            if layer == 0:
                bias[chunk_rows(n), :] = own
            for k in range(4):
                value = main[:, k * LANE : (k + 1) * LANE]
                if k < 3:
                    value = value + rest[:, k * LANE : (k + 1) * LANE]
                value = value * inverse
                if k == 0:
                    value = jnp.where(lane_all < pvh, value, log_sum)
                for r in range(rows):
                    sm[r : r + 1, k * LANE : (k + 1) * LANE] = jnp.sum(
                        value[r * HP : (r + 1) * HP, :]
                        * me_mask[:, k * LANE : (k + 1) * LANE],
                        axis=0,
                        keepdims=True,
                    )
            part = tiles(sm[...], 0, 4)
            frame = tiles(turn, 0, 12)
            moved = [part[k] - frame[9 + k] for k in range(3)]
            inside = lane8 < pvh
            for k in range(3):
                local = frame[k] * moved[0] + frame[3 + k] * moved[1] + frame[6 + k] * moved[2]
                if k == 0:
                    hi = part[0].astype(BF16).astype(F32)
                    other = jnp.where(lane8 < pvh + heads, hi, part[0] - hi)
                else:
                    other = part[k]
                spb[layer, n, heads + k] = jnp.where(inside, local, other).astype(BF16)
            spb[layer, n, heads + 3] = part[3].astype(BF16)
            for h in range(heads):
                spb[layer, n, h] = po[pl.ds(h, rows, stride=HP), :].astype(BF16)
            return n

        def step(t, carry):
            p_copy(layer, chunk(t)).start()
            return carry

        lax.fori_loop(0, nb - 1, step, 0)
        chunk(nb - 1)

    def combine(layer):
        slots = [(zb + d) % nb for d in range(nb)]
        with jax.named_scope("part_wait"):
            for n in slots[1:]:
                pltpu.make_async_copy(pr.at[layer, n], pr.at[layer, n], p_recv.at[layer, n]).wait()

        def piece(d, k):
            ref = spb if d == 0 else pr
            return ref[layer, slots[d], k].astype(F32)

        first = jnp.concatenate([piece(d, heads) for d in range(nb)], axis=0)
        sums = first + pltpu.roll(first, LANE - heads, 1)
        valid_all = (iota((nb * rows, LANE), 1) >= pvh) & (
            iota((nb * rows, LANE), 1) < pvh + heads
        )
        sums = jnp.where(valid_all, sums, 0.0)
        valid = (lane8 >= pvh) & (lane8 < pvh + heads)
        sums = [sums[d * rows : (d + 1) * rows, :] for d in range(nb)]
        top = functools.reduce(jnp.maximum, sums)
        shares = [jnp.where(valid, jnp.exp(value - top), 0.0) for value in sums]
        whole = jnp.where(valid, functools.reduce(jnp.add, shares), 1.0)
        shares = [value / whole for value in shares]
        wide = spread(jnp.concatenate(shares, axis=0), expm[...])
        mixed = []
        for k in range(4):
            acc = None
            for d in range(nb):
                term = wide[d * rows : (d + 1) * rows, k * LANE : (k + 1) * LANE] * piece(
                    d, heads + k
                )
                acc = term if acc is None else acc + term
            mixed.append(acc)
        pairs = []
        for h in range(heads):
            acc = None
            for d in range(nb):
                term = col(shares[d], pvh + h) * piece(d, h)
                acc = term if acc is None else acc + term
            pairs.append(acc)
        return mixed, pairs

    def gain_row(ref):
        return jnp.concatenate([ref[k : k + 1, :] for k in range(chan // LANE)], axis=1)

    def update(layer, state, fr, mixed, pairs):
        turn = [col(fr, k) for k in range(9)]
        shift = [col(fr, 9 + k) for k in range(3)]
        inside = lane8 < pvh
        norm = jnp.sqrt(
            mixed[0] * mixed[0] + mixed[1] * mixed[1] + mixed[2] * mixed[2] + 1e-08
        )
        concat = mixed + [jnp.where(inside, norm, 0.0)] + pairs
        concat = jnp.concatenate(concat, axis=1).astype(BF16)
        if layer == 0:
            for copy in wo_copies:
                copy.wait()
        state = state + dot(concat, wo[...])
        normed = layer_norm(state, gain_row(g1_ref))
        hidden = jnp.maximum(dot(normed.astype(BF16), m1[...]), 0.0).astype(BF16)
        hidden = jnp.maximum(dot(hidden, m2[...]), 0.0).astype(BF16)
        state = layer_norm(normed + dot(hidden, m3[...]), gain_row(g2_ref))
        if layer == LAYERS - 1:
            state_buf[...] = state
            last_copies[0].start()
        state_bf = state.astype(BF16)
        upd = dot_nt(state_bf, fw_ref[...])
        u = [jnp.broadcast_to(upd[:, k : k + 1], (rows, LANE)) for k in range(6)]
        inverse = lax.rsqrt(1.0 + u[0] * u[0] + u[1] * u[1] + u[2] * u[2])
        vx, vy, vz = u[0] * inverse, u[1] * inverse, u[2] * inverse
        square = inverse * inverse
        matrix = [
            [
                square + vx * vx - vy * vy - vz * vz,
                2.0 * (vx * vy - inverse * vz),
                2.0 * (vx * vz + inverse * vy),
            ],
            [
                2.0 * (vx * vy + inverse * vz),
                square - vx * vx + vy * vy - vz * vz,
                2.0 * (vy * vz - inverse * vx),
            ],
            [
                2.0 * (vx * vz - inverse * vy),
                2.0 * (vy * vz + inverse * vx),
                square - vx * vx - vy * vy + vz * vz,
            ],
        ]
        entries = [
            turn[3 * a] * matrix[0][b]
            + turn[3 * a + 1] * matrix[1][b]
            + turn[3 * a + 2] * matrix[2][b]
            for a in range(3)
            for b in range(3)
        ] + [
            turn[3 * a] * u[3] + turn[3 * a + 1] * u[4] + turn[3 * a + 2] * u[5] + shift[a]
            for a in range(3)
        ]
        fr = jnp.zeros((rows, LANE), F32)
        for k in range(12):
            fr = jnp.where((lane8 % 12 == k) & (lane8 < 36), entries[k], fr)
        return state, state_bf, fr

    last_copies = [
        pltpu.make_async_copy(src, dst, last_sem.at[k])
        for k, (src, dst) in enumerate(
            ((state_buf, out_state), (turn_buf, out_turn), (shift_buf, out_shift))
        )
    ]
    state = single[...].astype(F32)
    for layer in range(LAYERS):
        if layer == 0:
            exchange_across(2)
            exchange_across(3)
        with jax.named_scope(f"key_wait_{layer}"):
            pltpu.make_async_copy(
                kx.at[layer, 0 : g_count - 1], kx.at[layer, 0 : g_count - 1], kx_recv.at[layer]
            ).wait()
        if layer == 0:
            exchange_across(4)
        with jax.named_scope(f"key_{layer}"):
            key_phase(layer)
        with jax.named_scope(f"query_wait_{layer}"):
            pltpu.make_async_copy(
                qx.at[layer, 0 : nb - 1], qx.at[layer, 0 : nb - 1], qx_recv.at[layer]
            ).wait()
        with jax.named_scope(f"query_{layer}"):
            query_phase(layer)
        if layer == 0:
            exchange_across(5)
            with jax.named_scope(f"score_{layer}"):
                score_phase()
            exchange_across(6)
        with jax.named_scope(f"chunk_{layer}"):
            chunk_phase(layer)
        with jax.named_scope(f"combine_{layer}"):
            mixed, pairs = combine(layer)
        with jax.named_scope(f"update_{layer}"):
            state, state_bf, frames = update(layer, state, frames, mixed, pairs)
        if layer + 1 < LAYERS:
            with jax.named_scope(f"send_{layer}"):
                put_message(layer + 1, state_bf, frames)
                send_message(layer + 1)
    turn_buf[...] = frames[:, 0:9]
    pick = (iota((3, LANE), 1) == iota((3, LANE), 0) + 9).astype(F32)
    shift_buf[...] = lax.dot_general(
        pick, frames, (((1,), (1,)), ((), ())), precision=lax.Precision.HIGHEST,
        preferred_element_type=F32,
    )
    last_copies[1].start()
    last_copies[2].start()
    for layer in range(LAYERS):
        pltpu.make_async_copy(
            kx.at[layer, 0 : g_count - 1], kx.at[layer, 0 : g_count - 1], x_send.at[layer]
        ).wait()
        pltpu.make_async_copy(
            qx.at[layer, 0 : nb - 1], qx.at[layer, 0 : nb - 1], x_send.at[layer]
        ).wait()
        pltpu.make_async_copy(
            pr.at[layer, 0 : nb - 1], pr.at[layer, 0 : nb - 1], p_send.at[layer]
        ).wait()
    for offset in near:
        pltpu.make_async_copy(pair.at[0, :, 0, 0], pair.at[0, :, 0, 0], a2a_send).wait()
    for copy in last_copies:
        copy.wait()


def hand_over(a, b, c, a_out, b_out, c_out, sem):
    copies = [
        pltpu.make_async_copy(src, dst, sem.at[k])
        for k, (src, dst) in enumerate(((a, a_out), (b, b_out), (c, c_out)))
    ]
    for copy in copies:
        copy.start()
    for copy in copies:
        copy.wait()


def on_device(
    pair_cols,
    single,
    rotation,
    translation,
    residue_mask,
    chain_index,
    query_weight,
    key_weight,
    value_weight,
    qpoint_weight,
    kpoint_weight,
    vpoint_weight,
    pair_weight,
    head_weight,
    chain_weight,
    output_weight,
    gain_first,
    mlp_first,
    mlp_second,
    mlp_third,
    gain_second,
    frame_weight,
):
    nx = lax.axis_size("row_0")
    nz = lax.axis_size("row_1")
    cores = lax.axis_size("row_2")
    nb = nz // SPAN
    rows, chan = single.shape
    heads = head_weight.shape[0]
    hd = query_weight.shape[1]
    g_count = nx * SPAN * cores
    nk = g_count * rows
    nq = nb * rows
    width = chan + LANE
    pair = pair_cols.reshape(nx, nb, SPAN, cores, rows, *pair_cols.shape[1:])
    hbm = pl.BlockSpec(memory_space=pl.ANY)
    small = [
        single,
        jnp.transpose(rotation),
        translation,
        residue_mask.reshape(-1, LANE),
        chain_index.reshape(-1, LANE),
        pair_weight,
        head_weight.reshape(1, -1),
        chain_weight.reshape(1, -1),
        gain_first.reshape(-1, LANE),
        gain_second.reshape(-1, LANE),
        jnp.transpose(frame_weight),
    ]
    scratch = [pltpu.VMEM(v.shape, v.dtype) for v in small] + [
        pltpu.VMEM((nb, rows, nk, LANE), BF16),
        pltpu.VMEM((LAYERS, g_count, rows, width), BF16),
        pltpu.VMEM((LAYERS, nb, rows, width), BF16),
        pltpu.VMEM((LAYERS, rows, width), BF16),
        pltpu.VMEM((5 * LANE, chan), BF16),
        pltpu.VMEM((5 * LANE, chan), BF16),
        pltpu.VMEM((4 * LANE, chan), BF16),
        pltpu.VMEM((chan, 5 * LANE), BF16),
        pltpu.VMEM((chan, 5 * LANE), BF16),
        pltpu.VMEM((chan, 4 * LANE), BF16),
        pltpu.VMEM(((5 + heads) * LANE, chan), BF16),
        pltpu.VMEM(mlp_first.shape, BF16),
        pltpu.VMEM(mlp_second.shape, BF16),
        pltpu.VMEM(mlp_third.shape, BF16),
        pltpu.VMEM((LANE, 12 * LANE), BF16),
        pltpu.VMEM((LANE, 4 * LANE), BF16),
        pltpu.VMEM((nq, 8 * LANE), F32),
        pltpu.VMEM((nk, 8 * LANE), BF16),
        pltpu.VMEM((nk, 4 * LANE), BF16),
        pltpu.VMEM((nk, 3 * LANE), BF16),
        pltpu.VMEM((nq * HP, nk), F32),
        pltpu.VMEM((nq * HP, nk), F32),
        pltpu.VMEM((nq, nk), F32),
        pltpu.VMEM((HP, 8 * LANE), F32),
        pltpu.VMEM((HP, 4 * LANE), F32),
        pltpu.VMEM((rows * HP, LANE), F32),
        pltpu.VMEM((rows, 4 * LANE), F32),
        pltpu.VMEM((nq, 12 * LANE), F32),
        pltpu.VMEM((LAYERS, nb, heads + 4, rows, LANE), BF16),
        pltpu.VMEM((LAYERS, nb, heads + 4, rows, LANE), BF16),
        pltpu.VMEM((rows, chan), F32),
        pltpu.VMEM((rows, 9), F32),
        pltpu.VMEM((3, rows), F32),
        pltpu.SemaphoreType.DMA((3,)),
        pltpu.SemaphoreType.DMA((11,)),
        pltpu.SemaphoreType.DMA((23,)),
        pltpu.SemaphoreType.DMA((8,)),
        pltpu.SemaphoreType.DMA((nb,)),
        pltpu.SemaphoreType.DMA,
        pltpu.SemaphoreType.DMA((LAYERS,)),
        pltpu.SemaphoreType.DMA((LAYERS,)),
        pltpu.SemaphoreType.DMA((LAYERS,)),
        pltpu.SemaphoreType.DMA((LAYERS,)),
        pltpu.SemaphoreType.DMA((LAYERS, nb)),
    ]
    state, turned, moved = pl.pallas_call(
        functools.partial(kernel, (nx, nb, cores, rows, heads)),
        name="structure_layers",
        out_shape=(
            jax.ShapeDtypeStruct((rows, chan), F32),
            jax.ShapeDtypeStruct((rows, 9), F32),
            jax.ShapeDtypeStruct((3, rows), F32),
        ),
        in_specs=[hbm] * 22,
        out_specs=(hbm, hbm, hbm),
        scratch_shapes=scratch,
        compiler_params=pltpu.CompilerParams(
            collective_id=0, has_side_effects=True, vmem_limit_bytes=62 * 1024 * 1024
        ),
    )(
        pair,
        *small[:5],
        jnp.transpose(query_weight),
        jnp.transpose(key_weight),
        jnp.transpose(value_weight),
        jnp.transpose(qpoint_weight),
        jnp.transpose(kpoint_weight),
        jnp.transpose(vpoint_weight),
        *small[5:8],
        output_weight,
        small[8],
        mlp_first,
        mlp_second,
        mlp_third,
        small[9],
        small[10],
    )
    state, turned, moved = pl.pallas_call(
        hand_over,
        name="hand_over",
        out_shape=tuple(jax.ShapeDtypeStruct(v.shape, v.dtype) for v in (state, turned, moved)),
        in_specs=[hbm] * 3,
        out_specs=(hbm,) * 3,
        scratch_shapes=[pltpu.SemaphoreType.DMA((3,))],
        compiler_params=pltpu.CompilerParams(vmem_limit_bytes=62 * 1024 * 1024),
    )(state, turned, moved)
    return state, jnp.transpose(turned), moved


def solution(mesh):
    finer = Mesh(
        mesh.devices.reshape(mesh.shape["groups"], 4, 16, 2), ("groups", "row_0", "row_1", "row_2")
    )
    in_specs = (
        P(None, GROUPS_ROW, None),
        P(GROUPS_ROW, None),
        P(None, GROUPS_ROW),
        P(None, GROUPS_ROW),
        P("groups"),
        P("groups"),
    ) + (P(),) * 16
    out_specs = (P(GROUPS_ROW, None), P(None, GROUPS_ROW), P(None, GROUPS_ROW))
    return jax.shard_map(
        on_device, mesh=finer, in_specs=in_specs, out_specs=out_specs, check_vma=False
    )
```
